32 devices in a mesh: blk: 8 (over z, x), lane: 4 (over y, core).
Axes of the slice: x: 2, y: 2, z: 4, core: 2. Of those that a mesh axis runs over, the one named last changes fastest.
Arguments:
- left_factor: bfloat16 [4096, 512], P('blk'), may hold values from -6 to 6
- right_factor: bfloat16 [4, 4096, 512], P('lane', 'blk'), may hold values from -6 to 6
- observed: bfloat16 [4, 4, 512, 4096], P('lane', None, None, 'blk'), may hold values from -6 to 6
- row_codes: int32 [4096], P('blk'), may hold values from 0 to 1073741823
- shift_codes: int32 [4, 4, 4096], P('lane', None, 'blk'), may hold values from 0 to 29
Outputs:
- left_out: bfloat16 [4096, 512], P('blk')
- right_out: bfloat16 [4, 4096, 512], P('lane', 'blk')
The draws below stay inside these ranges and needn't reach their ends.
Inputs may be any that keep to these rules, and one draw needn't show every extreme that they name: `row_codes`: each row's word carries thirty independent sampling bits. `shift_codes`: A bit number for each lane, cycle step and visited tile entry column.
All inputs are finite; a program needn't handle non-finite values.
Results may differ from the reference program's by a relative error of at most 0.013.
Values may be sent and summed in bfloat16 or wider, within the bound.
A program may use at most 64 MiB of HBM per device.

```python
import math
import jax
import jax.numpy as jnp
from jax import lax

RANK = 512
TILE_COLS = 512
TILE_ROWS = 512
STEPS = 4
BLOCKS = 8
ROWS = 4096
COLUMNS = 4096
N_LANE = 4


def touch_ends(drawn, rng, low, high):
    longest = drawn.shape.index(max(drawn.shape))
    spots = []
    for shift in (0, 1):
        where = [jax.random.randint(jax.random.fold_in(rng, axis), (), 0, length) for axis, length in enumerate(drawn.shape)]
        where[longest] = (where[longest] + shift) % drawn.shape[longest]
        spots.append(tuple(where))
    return drawn.at[spots[0]].set(low).at[spots[1]].set(high)


def steps_of(rng, shape, pieces, smallest, high):
    gain = 1.0
    for axis_at, shards_of in pieces:
        steps = jax.random.uniform(jax.random.fold_in(jax.random.fold_in(rng, 6), axis_at), (shards_of,), jnp.float32, smallest / len(pieces), high / len(pieces))
        gain = gain * jnp.repeat(jnp.exp(steps), shape[axis_at] // shards_of).reshape((-1,) + (1,) * (len(shape) - 1 - axis_at))
    return gain


def normal_values(rng, dims, scale, reach, split=(), kind=jnp.bfloat16):
    drawn = jax.random.normal(rng, dims, jnp.float32) * scale
    if len(split) > 0:
        drawn = steps_of(rng, dims, split, -0.22, 0.18) * drawn
    return jnp.clip(drawn, min=-reach, max=reach).astype(kind)


def setup_inputs(seed: int = 0) -> dict:
    key_list = jax.random.split(jax.random.key(seed), 6)
    left_factor = normal_values(key_list[0], (ROWS, RANK), 1.0, 6.0, ((0, 8),))
    right_factor = normal_values(key_list[1], (N_LANE, COLUMNS, RANK), 1.0, 6.0, ((0, 4), (1, 8)))
    observed = normal_values(key_list[2], (N_LANE, STEPS, TILE_COLS, ROWS), 1.0, 6.0, ((0, 4), (3, 8)))
    row_codes = touch_ends(jax.random.randint(key_list[3], (ROWS,), 0, 1073741824), jax.random.fold_in(key_list[3], 1), 0, 1073741823).astype(jnp.int32)
    shift_codes = touch_ends(jax.random.randint(key_list[4], (N_LANE, STEPS, COLUMNS), 0, 30), jax.random.fold_in(key_list[4], 1), 0, 29).astype(jnp.int32)
    return {"left_factor": left_factor, "right_factor": right_factor, "observed": observed, "row_codes": row_codes, "shift_codes": shift_codes}


step_right = 0.25
step_left = 0.1

def reference(left_factor, right_factor, observed, row_codes, shift_codes):
    root_scale = 1.0 / math.sqrt(RANK)
    left_blocks = left_factor.reshape(BLOCKS, TILE_ROWS, RANK).astype(jnp.float32)
    row_blocks = row_codes.reshape(BLOCKS, TILE_ROWS)
    grad_total = jnp.zeros((BLOCKS, TILE_ROWS, RANK), jnp.float32)
    right_list = []
    for lane_index in range(N_LANE):
        right_now = right_factor[lane_index].reshape(BLOCKS, TILE_COLS, RANK)
        for cycle_step in range(STEPS):
            visited = jnp.roll(right_now, cycle_step, axis=0).astype(jnp.float32)
            predicted = jnp.einsum('nck,nrk->ncr', visited, left_blocks) * root_scale
            shifts = shift_codes[lane_index, cycle_step].reshape(BLOCKS, TILE_COLS)
            sample_bits = jnp.right_shift(row_blocks[:, None, :], shifts[:, :, None]) & 1
            target = observed[lane_index, cycle_step].reshape(TILE_COLS, BLOCKS, TILE_ROWS)
            target = jnp.transpose(target, (1, 0, 2)).astype(jnp.float32)
            error_tile = jnp.where(sample_bits == 1, predicted - target, 0.0).astype(jnp.bfloat16)
            error_tile = lax.optimization_barrier(error_tile).astype(jnp.float32)
            grad_right = jnp.einsum('ncr,nrk->nck', error_tile, left_blocks)
            grad_total = grad_total + jnp.einsum('ncr,nck->nrk', error_tile, visited)
            updated = (visited - step_right * root_scale * grad_right).astype(jnp.bfloat16)
            right_now = jnp.roll(updated, -cycle_step, axis=0)
        placed = jnp.roll(right_now, STEPS - 1, axis=0)
        right_list.append(placed.reshape(BLOCKS * TILE_COLS, RANK))
    left_out = (left_blocks - step_left * root_scale * grad_total).astype(jnp.bfloat16)
    return (left_out.reshape(BLOCKS * TILE_ROWS, RANK), jnp.stack(right_list))
```

```python
import functools
import math

import jax
import jax.numpy as jnp
from jax import lax
from jax.experimental import pallas as pl
from jax.experimental.pallas import tpu as pltpu
from jax.sharding import PartitionSpec as P

step_right = 0.25
step_left = 0.1

CHUNKS = 4
WIDTH = 128
PARTS = 2
PIECES = 4
SUBS = 2
GUEST = 1
MESH = pl.DeviceIdType.MESH


def kernel(
    blocks, lanes,
    left_hbm, right_hbm, obs_hbm, codes_hbm, shift_hbm,
    left_out, right_out,
    left, left_g, first, inner, hop_out, hop_in, turn_out, turn_in, final,
    obs, obs_g, codes, codes_g, shift, shift_g, turned, errs,
    grad, grad_g, back_out, back_in, ret_out, ret_in, pair_out, pair_in, peer_out, peer_in, result,
    load_sem, tile_send, tile_recv, table_send, table_recv, share_send, share_recv,
    peer_share_send, peer_share_recv, pair_share_send, pair_share_recv,
    hop_send, hop_recv, turn_send, turn_recv, back_send, back_recv, ret_send, ret_recv,
    swap_send, swap_recv, cross_send, cross_recv, last_send, last_recv, out_sem,
):
    steps, cols, rows = errs.shape
    rank = left.shape[1]
    scale = 1.0 / math.sqrt(rank)
    size = cols // CHUNKS
    half = rows // 2
    part = half // PIECES
    own = rows // lanes
    sub = own // SUBS
    width = turned.shape[2]
    others = lanes // 2 - 1
    blk = lax.axis_index("blk")
    lane = lax.axis_index("lane")
    odd = lax.rem(blk, 2)
    partner = blk + 1 - 2 * odd
    ahead = lax.rem(blk + 1, blocks)
    behind = lax.rem(blk + blocks - 1, blocks)
    ahead2 = lax.rem(blk + 2, blocks)
    behind2 = lax.rem(blk + blocks - 2, blocks)
    side = lax.rem(lane, 2)
    pair = lane + 1 - 2 * side
    peers = [lax.rem(lane + 2 * hop, lanes) for hop in range(1, lanes // 2)]
    sources = [lax.rem(lane + lanes - 2 * hop, lanes) for hop in range(1, lanes // 2)]
    mine = pl.multiple_of(side * half, half)
    other = pl.multiple_of((1 - side) * half, half)

    barrier = pltpu.get_barrier_semaphore()
    for target in (partner, behind, behind2):
        pl.semaphore_signal(barrier, inc=1, device_id={"blk": target}, device_id_type=MESH)
    for friend in [pair] + peers:
        pl.semaphore_signal(barrier, inc=1, device_id={"lane": friend}, device_id_type=MESH)

    def remote(source, target, send, recv, **place):
        return pltpu.make_async_remote_copy(
            src_ref=source, dst_ref=target, send_sem=send, recv_sem=recv,
            device_id=place, device_id_type=MESH,
        )

    def chunk(k):
        return pl.ds(pl.multiple_of(k * size, size), size)

    natural = [s for s in range(steps) if s != GUEST]
    loads = [
        pltpu.make_async_copy(shift_hbm, shift, load_sem.at[0]),
        pltpu.make_async_copy(codes_hbm, codes, load_sem.at[1]),
        pltpu.make_async_copy(right_hbm.at[0], first, load_sem.at[2]),
        pltpu.make_async_copy(left_hbm, left, load_sem.at[3]),
    ]
    for n, s in enumerate(natural):
        loads.append(pltpu.make_async_copy(obs_hbm.at[0, s], obs.at[n], load_sem.at[4 + n]))
    for copy in loads:
        copy.start()

    def piece(owner, u):
        return pl.ds(pl.multiple_of(owner * own + u * sub, sub), sub)

    def lend(u):
        span = piece(lane, u)
        return remote(left_hbm.at[span], left_g.at[span], share_send.at[u], share_recv.at[u], blk=partner)

    def lend_peer(m, u):
        span = piece(lane, u)
        return remote(left_g.at[span], left_g.at[span], peer_share_send.at[m, u], peer_share_recv.at[m, u], lane=peers[m])

    def lend_pair(m, u):
        span = piece(lane if m == 0 else sources[m - 1], u)
        return remote(left_g.at[span], left_g.at[span], pair_share_send.at[m, u], pair_share_recv.at[m, u], lane=pair)

    def give(k):
        span = chunk(k)
        return remote(obs_hbm.at[0, GUEST, span], obs_g.at[span], tile_send.at[k], tile_recv.at[k], blk=partner)

    tables = [
        remote(codes_hbm, codes_g, table_send.at[0], table_recv.at[0], blk=partner),
        remote(shift_hbm, shift_g, table_send.at[1], table_recv.at[1], blk=partner),
    ]

    def hop(k):
        span = chunk(k)
        return remote(hop_out.at[span], hop_in.at[span], hop_send.at[k], hop_recv.at[k], blk=ahead2)

    def cross_over(k):
        span = chunk(k)
        return remote(turn_out.at[span], turn_in.at[span], turn_send.at[k], turn_recv.at[k], blk=ahead)

    def turn(s, table):
        for start in range(0, cols, width):
            span = pl.ds(start, width)
            turned[s, span, :] = jnp.transpose(jnp.broadcast_to(table[0, pl.ds(s, 1), span], (width, width)))

    def error_of(k, s, block, factor, words, target):
        span = chunk(k)
        shifts = jnp.concatenate([turned[s, span, :]] * (rows // width), axis=1)
        seen = (jnp.right_shift(words[...], shifts) & 1) == 1
        predicted = lax.dot_general(
            block, factor[...], (((1,), (1,)), ((), ())), preferred_element_type=jnp.float32
        )
        error = predicted * scale - target[span, :].astype(jnp.float32)
        return jnp.where(seen, error, 0.0).astype(jnp.bfloat16)

    def stepped(error, block, factor):
        move = jnp.dot(error, factor[...], preferred_element_type=jnp.float32)
        return (block.astype(jnp.float32) - step_right * scale * move).astype(jnp.bfloat16)

    def tile(k, s, source, target, guest=False):
        span = chunk(k)
        block = source[span, :]
        if guest:
            factor, words, wanted = left_g, codes_g, obs_g
        else:
            factor, words, wanted = left, codes, obs.at[natural.index(s)]
        error = error_of(k, s, block, factor, words, wanted)
        errs[s, span, :] = error
        target[span, :] = stepped(error, block, factor)

    def outer(error, block):
        return lax.dot_general(error, block, (((0,), (0,)), ((), ())), preferred_element_type=jnp.float32)

    loads[0].wait()
    turn(0, shift)
    pl.semaphore_wait(barrier, 3 + 1 + len(peers))
    for u in range(SUBS):
        lend(u).start()
    for copy in tables:
        copy.start()
    for k in range(CHUNKS):
        give(k).start()
    for copy in loads[1:5]:
        copy.wait()

    def relay():
        for u in range(SUBS):
            lend(u).wait_recv()
            for m in range(others):
                lend_peer(m, u).start()
            lend_pair(0, u).start()

    def gather():
        for u in range(SUBS):
            for m in range(others):
                lend_peer(m, u).wait_recv()
                lend_pair(1 + m, u).start()
        for copy in tables:
            copy.wait_recv()
        turn(GUEST, shift_g)
        for m in range(1 + others):
            for u in range(SUBS):
                lend_pair(m, u).wait_recv()

    @pl.when(odd == 0)
    def _():
        pl.loop(0, CHUNKS)(lambda k: tile(k, 0, first, inner))
        relay()
        grad[...] = outer(errs[0], first[...])
        turn(2, shift)
        turn(3, shift)
        gather()

        @pl.loop(0, CHUNKS)
        def _(k):
            give(k).wait_recv()
            tile(k, 1, inner, hop_out, guest=True)
            hop(k).start()

        grad_g[...] = outer(errs[1], inner[...])
        loads[5].wait()

        @pl.loop(0, CHUNKS)
        def _(k):
            hop(k).wait_recv()
            tile(k, 2, hop_in, turn_out)
            cross_over(k).start()

        grad[...] += outer(errs[2], hop_in[...])

    @pl.when(odd == 1)
    def _():
        @pl.loop(0, CHUNKS)
        def _(k):
            tile(k, 0, first, hop_out)
            hop(k).start()

        relay()
        grad[...] = outer(errs[0], first[...])
        turn(2, shift)
        turn(3, shift)
        gather()
        loads[5].wait()

        @pl.loop(0, CHUNKS)
        def _(k):
            give(k).wait_recv()
            hop(k).wait_recv()
            tile(k, 1, hop_in, inner, guest=True)
            tile(k, 2, inner, turn_out)
            cross_over(k).start()

        grad_g[...] = outer(errs[1], hop_in[...])
        grad[...] += outer(errs[2], inner[...])

    back = remote(back_out, back_in, back_send.at[0], back_recv.at[0], lane=pair)
    back_out[...] = grad_g[pl.ds(other, half), :].astype(jnp.bfloat16)
    back.start()

    def give_back(q):
        span = pl.ds(q * part, part)
        return remote(ret_out.at[span], ret_in.at[span], ret_send.at[q], ret_recv.at[q], blk=partner)

    loads[6].wait()
    last = steps - 1

    @pl.loop(0, CHUNKS - 1)
    def _(k):
        cross_over(k).wait_recv()
        tile(k, last, turn_in, final)

    early = (CHUNKS - 1) * size
    grad[...] += outer(errs[last, pl.ds(0, early)], turn_in[pl.ds(0, early)])
    back.wait_recv()
    ret_out[...] = (grad_g[pl.ds(mine, half), :] + back_in[...].astype(jnp.float32)).astype(jnp.bfloat16)
    for q in range(PIECES):
        give_back(q).start()

    tail = pl.ds(early, size)
    cross_over(CHUNKS - 1).wait_recv()
    errs[last, tail, :] = error_of(CHUNKS - 1, last, turn_in[tail, :], left, codes, obs.at[natural.index(last)])

    def finish(start):
        span = pl.ds(start, half)
        return grad[span, :] + outer(errs[last, tail, span], turn_in[tail, :])

    def swap(q):
        span = pl.ds(q * part, part)
        return remote(pair_out.at[span], pair_in.at[span], swap_send.at[q], swap_recv.at[q], lane=pair)

    def cross(m, q):
        span = pl.ds(q * part, part)
        return remote(peer_out.at[span], peer_in.at[m, span], cross_send.at[m, q], cross_recv.at[m, q], lane=peers[m])

    def share(q):
        span = pl.ds(pl.multiple_of(mine + q * part, part), part)
        return remote(result.at[span], result.at[span], last_send.at[q], last_recv.at[q], lane=pair)

    pair_out[...] = finish(other).astype(jnp.bfloat16)
    for q in range(PIECES):
        swap(q).start()
    grad[pl.ds(mine, half), :] = finish(mine)
    for q in range(PIECES):
        span = pl.ds(q * part, part)
        swap(q).wait_recv()
        give_back(q).wait_recv()
        peer_out[span, :] = (
            grad[pl.ds(pl.multiple_of(mine + q * part, part), part), :]
            + pair_in[span, :].astype(jnp.float32)
            + ret_in[span, :].astype(jnp.float32)
        ).astype(jnp.bfloat16)
        for m in range(len(peers)):
            cross(m, q).start()

    final[tail, :] = stepped(errs[last, tail, :], turn_in[tail, :], left)

    outs = [
        pltpu.make_async_copy(final, right_out.at[0], out_sem.at[0]),
        pltpu.make_async_copy(result.at[pl.ds(mine, half)], left_out.at[pl.ds(mine, half)], out_sem.at[1]),
        pltpu.make_async_copy(result.at[pl.ds(other, half)], left_out.at[pl.ds(other, half)], out_sem.at[2]),
    ]
    outs[0].start()
    for u in range(SUBS):
        lend(u).wait_send()
        for m in range(others):
            lend_peer(m, u).wait_send()
        for m in range(1 + others):
            lend_pair(m, u).wait_send()
    for copy in tables:
        copy.wait_send()

    @pl.loop(0, CHUNKS)
    def _(k):
        give(k).wait_send()
        hop(k).wait_send()
        cross_over(k).wait_send()

    back.wait_send()

    for q in range(PIECES):
        span = pl.ds(q * part, part)
        here = pl.ds(pl.multiple_of(mine + q * part, part), part)
        total = peer_out[span, :].astype(jnp.float32)
        for m in range(len(peers)):
            cross(m, q).wait_recv()
            total = total + peer_in[m, span, :].astype(jnp.float32)
        result[here, :] = (left[here, :].astype(jnp.float32) - step_left * scale * total).astype(jnp.bfloat16)
        share(q).start()
    outs[1].start()
    for q in range(PIECES):
        share(q).wait_recv()
    outs[2].start()
    for q in range(PIECES):
        give_back(q).wait_send()
        swap(q).wait_send()
        for m in range(len(peers)):
            cross(m, q).wait_send()
        share(q).wait_send()
    for copy in outs:
        copy.wait()


def place(left_from, right_from, left_to, right_to, held, in_sem, out_sem):
    pairs = [(left_from, left_to), (right_from.at[0], right_to.at[0])]
    rows = left_from.shape[0] // PARTS
    moves = []
    for which, (source, target) in enumerate(pairs):
        for p in range(PARTS):
            span = pl.ds(p * rows, rows)
            moves.append((
                pltpu.make_async_copy(source.at[span], held.at[which, span], in_sem.at[which, p]),
                pltpu.make_async_copy(held.at[which, span], target.at[span], out_sem.at[which, p]),
            ))
    for inward, _ in moves:
        inward.start()
    for inward, outward in moves:
        inward.wait()
        outward.start()
    for _, outward in moves:
        outward.wait()


def solution(mesh):
    blocks = mesh.shape["blk"]
    lanes = mesh.shape["lane"]

    def local(left_factor, right_factor, observed, row_codes, shift_codes):
        rows, rank = left_factor.shape
        _, steps, cols, _ = observed.shape
        bf16, f32, i32 = jnp.bfloat16, jnp.float32, jnp.int32
        dma = pltpu.SemaphoreType.DMA
        vmem = pltpu.VMEM
        hbm = pl.BlockSpec(memory_space=pltpu.HBM)
        others = lanes // 2 - 1
        half = rows // 2
        shapes = (
            jax.ShapeDtypeStruct((rows, rank), bf16),
            jax.ShapeDtypeStruct((1, cols, rank), bf16),
        )
        results = pl.pallas_call(
            functools.partial(kernel, blocks, lanes),
            out_shape=shapes,
            in_specs=[hbm] * 5,
            out_specs=(hbm, hbm),
            scratch_shapes=[
                vmem((rows, rank), bf16),
                vmem((rows, rank), bf16),
                *[vmem((cols, rank), bf16)] * 7,
                vmem((steps - 1, cols, rows), bf16),
                vmem((cols, rows), bf16),
                vmem((1, rows), i32),
                vmem((1, rows), i32),
                vmem((1, steps, cols), i32),
                vmem((1, steps, cols), i32),
                vmem((steps, cols, WIDTH), i32),
                vmem((steps, cols, rows), bf16),
                vmem((rows, rank), f32),
                vmem((rows, rank), f32),
                *[vmem((half, rank), bf16)] * 7,
                vmem((others, half, rank), bf16),
                vmem((rows, rank), bf16),
                dma((4 + steps - 1,)),
                dma((CHUNKS,)), dma((CHUNKS,)),
                dma((2,)), dma((2,)),
                dma((SUBS,)), dma((SUBS,)),
                dma((others, SUBS)), dma((others, SUBS)),
                dma((1 + others, SUBS)), dma((1 + others, SUBS)),
                dma((CHUNKS,)), dma((CHUNKS,)),
                dma((CHUNKS,)), dma((CHUNKS,)),
                dma((1,)), dma((1,)),
                dma((PIECES,)), dma((PIECES,)),
                dma((PIECES,)), dma((PIECES,)),
                dma((others, PIECES)), dma((others, PIECES)),
                dma((PIECES,)), dma((PIECES,)),
                dma((3,)),
            ],
            compiler_params=pltpu.CompilerParams(
                collective_id=0, has_side_effects=True, vmem_limit_bytes=67043328
            ),
        )(
            left_factor, right_factor, observed,
            row_codes.reshape(1, rows), shift_codes,
        )
        return pl.pallas_call(
            place,
            out_shape=shapes,
            in_specs=[hbm] * 2,
            out_specs=(hbm, hbm),
            scratch_shapes=[pltpu.VMEM((2, max(rows, cols), rank), bf16), dma((2, PARTS)), dma((2, PARTS))],
            compiler_params=pltpu.CompilerParams(vmem_limit_bytes=67043328),
        )(*results)

    in_specs = (
        P("blk", None),
        P("lane", "blk", None),
        P("lane", None, None, "blk"),
        P("blk"),
        P("lane", None, "blk"),
    )
    out_specs = (P("blk", None), P("lane", "blk", None))
    return jax.shard_map(local, mesh=mesh, in_specs=in_specs, out_specs=out_specs, check_vma=False)
```

```python
import functools
import math

import jax
import jax.numpy as jnp
from jax import lax
from jax.experimental import pallas as pl
from jax.experimental.pallas import tpu as pltpu
from jax.sharding import PartitionSpec as P

step_right = 0.25
step_left = 0.1

CHUNKS = 8
LAG = 5
HOLD = 4
EARLY = 3
WIDTH = 128
PARTS = 2
PIECES = 4
SUBS = 2
GUEST = 1
MESH = pl.DeviceIdType.MESH


def kernel(
    blocks, lanes,
    left_hbm, right_hbm, obs_hbm, codes_hbm, shift_hbm,
    left_out, right_out,
    left, left_g, first, inner, hop_out, hop_in, turn_out, turn_in, final,
    obs, obs_g, codes, codes_g, shift, shift_g, turned, errs,
    grad, grad_g, back_out, back_in, ret_out, ret_in, pair_out, pair_in, peer_out, peer_in, result,
    load_sem, tile_send, tile_recv, table_send, table_recv, share_send, share_recv,
    peer_share_send, peer_share_recv, pair_share_send, pair_share_recv,
    hop_send, hop_recv, turn_send, turn_recv, back_send, back_recv, ret_send, ret_recv,
    swap_send, swap_recv, cross_send, cross_recv, last_send, last_recv, out_sem, clear_sem,
):
    steps, cols, rows = errs.shape
    rank = left.shape[1]
    scale = 1.0 / math.sqrt(rank)
    size = cols // CHUNKS
    half = rows // 2
    part = half // PIECES
    own = rows // lanes
    sub = own // SUBS
    width = turned.shape[2]
    others = lanes // 2 - 1
    blk = lax.axis_index("blk")
    lane = lax.axis_index("lane")
    odd = lax.rem(blk, 2)
    partner = blk + 1 - 2 * odd
    ahead = lax.rem(blk + 1, blocks)
    behind = lax.rem(blk + blocks - 1, blocks)
    ahead2 = lax.rem(blk + 2, blocks)
    behind2 = lax.rem(blk + blocks - 2, blocks)
    side = lax.rem(lane, 2)
    pair = lane + 1 - 2 * side
    peers = [lax.rem(lane + 2 * hop, lanes) for hop in range(1, lanes // 2)]
    sources = [lax.rem(lane + lanes - 2 * hop, lanes) for hop in range(1, lanes // 2)]
    mine = pl.multiple_of(side * half, half)
    other = pl.multiple_of((1 - side) * half, half)

    barrier = pltpu.get_barrier_semaphore()
    for target in (partner, behind, behind2):
        pl.semaphore_signal(barrier, inc=1, device_id={"blk": target}, device_id_type=MESH)
    for friend in [pair] + peers:
        pl.semaphore_signal(barrier, inc=1, device_id={"lane": friend}, device_id_type=MESH)
    pl.semaphore_signal(barrier, inc=1, device_id={"blk": ahead2, "lane": lane}, device_id_type=MESH)
    pl.semaphore_signal(barrier, inc=1, device_id={"blk": ahead2, "lane": pair}, device_id_type=MESH)

    def remote(source, target, send, recv, **place):
        return pltpu.make_async_remote_copy(
            src_ref=source, dst_ref=target, send_sem=send, recv_sem=recv,
            device_id=place, device_id_type=MESH,
        )

    def chunk(k):
        return pl.ds(pl.multiple_of(k * size, size), size)

    natural = [s for s in range(steps) if s != GUEST]
    loads = [
        pltpu.make_async_copy(shift_hbm, shift, load_sem.at[0]),
        pltpu.make_async_copy(codes_hbm, codes, load_sem.at[1]),
        pltpu.make_async_copy(right_hbm.at[0], first, load_sem.at[2]),
        pltpu.make_async_copy(left_hbm, left, load_sem.at[3]),
    ]
    for n, s in enumerate(natural):
        loads.append(pltpu.make_async_copy(obs_hbm.at[0, s], obs.at[n], load_sem.at[4 + n]))
    for copy in loads:
        copy.start()

    def piece(owner, u):
        return pl.ds(pl.multiple_of(owner * own + u * sub, sub), sub)

    def lend(u):
        span = piece(lane, u)
        return remote(left_hbm.at[span], left_g.at[span], share_send.at[u], share_recv.at[u], blk=partner)

    def lend_peer(m, u):
        span = piece(lane, u)
        return remote(left_g.at[span], left_g.at[span], peer_share_send.at[m, u], peer_share_recv.at[m, u], lane=peers[m])

    def lend_pair(m, u):
        span = piece(lane if m == 0 else sources[m - 1], u)
        return remote(left_g.at[span], left_g.at[span], pair_share_send.at[m, u], pair_share_recv.at[m, u], lane=pair)

    def give(k):
        span = chunk(k)
        return remote(obs_hbm.at[0, GUEST, span], obs_g.at[span], tile_send.at[k], tile_recv.at[k], blk=partner)

    tables = [
        remote(codes_hbm, codes_g, table_send.at[0], table_recv.at[0], blk=partner),
        remote(shift_hbm, shift_g, table_send.at[1], table_recv.at[1], blk=partner),
    ]

    def hop(k):
        span = chunk(k)
        return remote(hop_out.at[span], hop_in.at[span], hop_send.at[k], hop_recv.at[k], blk=ahead2)

    def cross_over(k):
        span = chunk(k)
        return remote(turn_out.at[span], turn_in.at[span], turn_send.at[k], turn_recv.at[k], blk=ahead)

    def turn(s, table):
        for start in range(0, cols, width):
            span = pl.ds(start, width)
            turned[s, span, :] = jnp.transpose(jnp.broadcast_to(table[0, pl.ds(s, 1), span], (width, width)))

    def error_of(k, s, block, factor, words, target):
        span = chunk(k)
        shifts = jnp.concatenate([turned[s, span, :]] * (rows // width), axis=1)
        seen = (jnp.right_shift(words[...], shifts) & 1) == 1
        predicted = lax.dot_general(
            block, factor[...], (((1,), (1,)), ((), ())), preferred_element_type=jnp.float32
        )
        error = predicted * scale - target[span, :].astype(jnp.float32)
        return jnp.where(seen, error, 0.0).astype(jnp.bfloat16)

    def stepped(error, block, factor):
        move = jnp.dot(error, factor[...], preferred_element_type=jnp.float32)
        return (block.astype(jnp.float32) - step_right * scale * move).astype(jnp.bfloat16)

    def tile(k, s, source, target, guest=False):
        span = chunk(k)
        block = source[span, :]
        if guest:
            factor, words, wanted = left_g, codes_g, obs_g
        else:
            factor, words, wanted = left, codes, obs.at[natural.index(s)]
        error = error_of(k, s, block, factor, words, wanted)
        errs[s, span, :] = error
        target[span, :] = stepped(error, block, factor)

    def outer(error, block):
        return lax.dot_general(error, block, (((0,), (0,)), ((), ())), preferred_element_type=jnp.float32)

    loads[0].wait()
    turn(0, shift)
    pl.semaphore_wait(barrier, 5 + 1 + len(peers))
    for u in range(SUBS):
        lend(u).start()
    for copy in tables:
        copy.start()
    for k in range(CHUNKS):
        give(k).start()
    for copy in loads[1:5]:
        copy.wait()

    def relay():
        for u in range(SUBS):
            lend(u).wait_recv()
            for m in range(others):
                lend_peer(m, u).start()
            lend_pair(0, u).start()

    def gather():
        for u in range(SUBS):
            for m in range(others):
                lend_peer(m, u).wait_recv()
                lend_pair(1 + m, u).start()
        for copy in tables:
            copy.wait_recv()
        turn(GUEST, shift_g)
        for m in range(1 + others):
            for u in range(SUBS):
                lend_pair(m, u).wait_recv()

    back = remote(back_out, back_in, back_send.at[0], back_recv.at[0], lane=pair)

    def send_back():
        back_out[...] = grad_g[pl.ds(other, half), :].astype(jnp.bfloat16)
        back.start()

    @pl.when(odd == 0)
    def _():
        pl.loop(0, CHUNKS)(lambda k: tile(k, 0, first, inner))
        relay()
        grad[...] = outer(errs[0], first[...])
        turn(2, shift)
        turn(3, shift)
        gather()

        def guest_visit(k):
            give(k).wait_recv()
            tile(k, GUEST, inner, hop_out, guest=True)
            hop(k).start()

        def home_visit(k):
            hop(k).wait_recv()
            tile(k, 2, hop_in, turn_out)
            cross_over(k).start()

        loads[5].wait()
        pl.loop(0, LAG)(guest_visit)
        pl.loop(0, CHUNKS)(lambda k: give(k).wait_send())
        pl.semaphore_signal(clear_sem, inc=1, device_id={"lane": pair}, device_id_type=MESH)
        pl.semaphore_wait(clear_sem, 1)

        @pl.loop(LAG, CHUNKS)
        def _(k):
            home_visit(k - LAG)
            guest_visit(k)

        grad_g[...] = outer(errs[GUEST], inner[...])
        send_back()
        pl.loop(CHUNKS - LAG, CHUNKS)(home_visit)
        grad[...] += outer(errs[2], hop_in[...])

    @pl.when(odd == 1)
    def _():
        @pl.loop(0, CHUNKS)
        def _(k):
            tile(k, 0, first, hop_out)
            hop(k).start()

        relay()
        grad[...] = outer(errs[0], first[...])
        turn(2, shift)
        turn(3, shift)
        gather()
        loads[5].wait()

        def visits(k):
            give(k).wait_recv()
            hop(k).wait_recv()
            tile(k, GUEST, hop_in, inner, guest=True)
            tile(k, 2, inner, turn_out)

        pl.loop(0, HOLD)(visits)
        pl.loop(0, CHUNKS - EARLY)(lambda k: give(k).wait_send())
        for place_lane in (lane, pair):
            pl.semaphore_signal(clear_sem, inc=1, device_id={"blk": behind2, "lane": place_lane}, device_id_type=MESH)
        pl.semaphore_wait(clear_sem, 2)
        pl.loop(0, HOLD)(lambda k: cross_over(k).start())

        @pl.loop(HOLD, CHUNKS)
        def _(k):
            visits(k)
            cross_over(k).start()

        grad_g[...] = outer(errs[GUEST], hop_in[...])
        send_back()
        grad[...] += outer(errs[2], inner[...])
        pl.loop(CHUNKS - EARLY, CHUNKS)(lambda k: give(k).wait_send())

    def give_back(q):
        span = pl.ds(q * part, part)
        return remote(ret_out.at[span], ret_in.at[span], ret_send.at[q], ret_recv.at[q], blk=partner)

    back.wait_recv()
    ret_out[...] = (grad_g[pl.ds(mine, half), :] + back_in[...].astype(jnp.float32)).astype(jnp.bfloat16)
    for q in range(PIECES):
        give_back(q).start()

    loads[6].wait()
    last = steps - 1

    @pl.loop(0, CHUNKS - 1)
    def _(k):
        cross_over(k).wait_recv()
        tile(k, last, turn_in, final)

    early = (CHUNKS - 1) * size
    grad[...] += outer(errs[last, pl.ds(0, early)], turn_in[pl.ds(0, early)])
    tail = pl.ds(early, size)
    cross_over(CHUNKS - 1).wait_recv()
    errs[last, tail, :] = error_of(CHUNKS - 1, last, turn_in[tail, :], left, codes, obs.at[natural.index(last)])

    def finish(start):
        span = pl.ds(start, half)
        return grad[span, :] + outer(errs[last, tail, span], turn_in[tail, :])

    def swap(q):
        span = pl.ds(q * part, part)
        return remote(pair_out.at[span], pair_in.at[span], swap_send.at[q], swap_recv.at[q], lane=pair)

    def cross(m, q):
        span = pl.ds(q * part, part)
        return remote(peer_out.at[span], peer_in.at[m, span], cross_send.at[m, q], cross_recv.at[m, q], lane=peers[m])

    def share(q):
        span = pl.ds(pl.multiple_of(mine + q * part, part), part)
        return remote(result.at[span], result.at[span], last_send.at[q], last_recv.at[q], lane=pair)

    pair_out[...] = finish(other).astype(jnp.bfloat16)
    for q in range(PIECES):
        swap(q).start()
    grad[pl.ds(mine, half), :] = finish(mine)
    for q in range(PIECES):
        span = pl.ds(q * part, part)
        swap(q).wait_recv()
        give_back(q).wait_recv()
        peer_out[span, :] = (
            grad[pl.ds(pl.multiple_of(mine + q * part, part), part), :]
            + pair_in[span, :].astype(jnp.float32)
            + ret_in[span, :].astype(jnp.float32)
        ).astype(jnp.bfloat16)
        for m in range(len(peers)):
            cross(m, q).start()

    final[tail, :] = stepped(errs[last, tail, :], turn_in[tail, :], left)

    outs = [
        pltpu.make_async_copy(final, right_out.at[0], out_sem.at[0]),
        pltpu.make_async_copy(result.at[pl.ds(mine, half)], left_out.at[pl.ds(mine, half)], out_sem.at[1]),
        pltpu.make_async_copy(result.at[pl.ds(other, half)], left_out.at[pl.ds(other, half)], out_sem.at[2]),
    ]
    outs[0].start()
    for u in range(SUBS):
        lend(u).wait_send()
        for m in range(others):
            lend_peer(m, u).wait_send()
        for m in range(1 + others):
            lend_pair(m, u).wait_send()
    for copy in tables:
        copy.wait_send()

    @pl.loop(0, CHUNKS)
    def _(k):
        hop(k).wait_send()
        cross_over(k).wait_send()

    back.wait_send()

    for q in range(PIECES):
        span = pl.ds(q * part, part)
        here = pl.ds(pl.multiple_of(mine + q * part, part), part)
        total = peer_out[span, :].astype(jnp.float32)
        for m in range(len(peers)):
            cross(m, q).wait_recv()
            total = total + peer_in[m, span, :].astype(jnp.float32)
        result[here, :] = (left[here, :].astype(jnp.float32) - step_left * scale * total).astype(jnp.bfloat16)
        share(q).start()
    outs[1].start()
    for q in range(PIECES):
        share(q).wait_recv()
    outs[2].start()
    for q in range(PIECES):
        give_back(q).wait_send()
        swap(q).wait_send()
        for m in range(len(peers)):
            cross(m, q).wait_send()
        share(q).wait_send()
    for copy in outs:
        copy.wait()


def place(left_from, right_from, left_to, right_to, held, in_sem, out_sem):
    pairs = [(left_from, left_to), (right_from.at[0], right_to.at[0])]
    rows = left_from.shape[0] // PARTS
    moves = []
    for which, (source, target) in enumerate(pairs):
        for p in range(PARTS):
            span = pl.ds(p * rows, rows)
            moves.append((
                pltpu.make_async_copy(source.at[span], held.at[which, span], in_sem.at[which, p]),
                pltpu.make_async_copy(held.at[which, span], target.at[span], out_sem.at[which, p]),
            ))
    for inward, _ in moves:
        inward.start()
    for inward, outward in moves:
        inward.wait()
        outward.start()
    for _, outward in moves:
        outward.wait()


def solution(mesh):
    blocks = mesh.shape["blk"]
    lanes = mesh.shape["lane"]

    def local(left_factor, right_factor, observed, row_codes, shift_codes):
        rows, rank = left_factor.shape
        _, steps, cols, _ = observed.shape
        bf16, f32, i32 = jnp.bfloat16, jnp.float32, jnp.int32
        dma = pltpu.SemaphoreType.DMA
        vmem = pltpu.VMEM
        hbm = pl.BlockSpec(memory_space=pltpu.HBM)
        others = lanes // 2 - 1
        half = rows // 2
        shapes = (
            jax.ShapeDtypeStruct((rows, rank), bf16),
            jax.ShapeDtypeStruct((1, cols, rank), bf16),
        )
        results = pl.pallas_call(
            functools.partial(kernel, blocks, lanes),
            out_shape=shapes,
            in_specs=[hbm] * 5,
            out_specs=(hbm, hbm),
            scratch_shapes=[
                vmem((rows, rank), bf16),
                vmem((rows, rank), bf16),
                *[vmem((cols, rank), bf16)] * 7,
                vmem((steps - 1, cols, rows), bf16),
                vmem((cols, rows), bf16),
                vmem((1, rows), i32),
                vmem((1, rows), i32),
                vmem((1, steps, cols), i32),
                vmem((1, steps, cols), i32),
                vmem((steps, cols, WIDTH), i32),
                vmem((steps, cols, rows), bf16),
                vmem((rows, rank), f32),
                vmem((rows, rank), f32),
                *[vmem((half, rank), bf16)] * 7,
                vmem((others, half, rank), bf16),
                vmem((rows, rank), bf16),
                dma((4 + steps - 1,)),
                dma((CHUNKS,)), dma((CHUNKS,)),
                dma((2,)), dma((2,)),
                dma((SUBS,)), dma((SUBS,)),
                dma((others, SUBS)), dma((others, SUBS)),
                dma((1 + others, SUBS)), dma((1 + others, SUBS)),
                dma((CHUNKS,)), dma((CHUNKS,)),
                dma((CHUNKS,)), dma((CHUNKS,)),
                dma((1,)), dma((1,)),
                dma((PIECES,)), dma((PIECES,)),
                dma((PIECES,)), dma((PIECES,)),
                dma((others, PIECES)), dma((others, PIECES)),
                dma((PIECES,)), dma((PIECES,)),
                dma((3,)),
                pltpu.SemaphoreType.REGULAR,
            ],
            compiler_params=pltpu.CompilerParams(
                collective_id=0, has_side_effects=True, vmem_limit_bytes=67043328
            ),
        )(
            left_factor, right_factor, observed,
            row_codes.reshape(1, rows), shift_codes,
        )
        return pl.pallas_call(
            place,
            out_shape=shapes,
            in_specs=[hbm] * 2,
            out_specs=(hbm, hbm),
            scratch_shapes=[pltpu.VMEM((2, max(rows, cols), rank), bf16), dma((2, PARTS)), dma((2, PARTS))],
            compiler_params=pltpu.CompilerParams(vmem_limit_bytes=67043328),
        )(*results)

    in_specs = (
        P("blk", None),
        P("lane", "blk", None),
        P("lane", None, None, "blk"),
        P("blk"),
        P("lane", None, "blk"),
    )
    out_specs = (P("blk", None), P("lane", "blk", None))
    return jax.shard_map(local, mesh=mesh, in_specs=in_specs, out_specs=out_specs, check_vma=False)
```

```python
import functools
import math

import jax
import jax.numpy as jnp
from jax import lax
from jax.experimental import pallas as pl
from jax.experimental.pallas import tpu as pltpu
from jax.sharding import PartitionSpec as P

step_right = 0.25
step_left = 0.1

CHUNKS = 8
LAG = 5
HOLD = 4
EARLY = 2
WIDTH = 128
PARTS = 2
PIECES = 4
SUBS = 2
GUEST = 1
MESH = pl.DeviceIdType.MESH


def kernel(
    blocks, lanes,
    left_hbm, right_hbm, obs_hbm, codes_hbm, shift_hbm,
    left_out, right_out,
    left, left_g, first, inner, hop_out, hop_in, turn_out, turn_in, final,
    obs, obs_g, codes, codes_g, shift, shift_g, turned, errs,
    grad, grad_g, back_out, back_in, ret_out, ret_in, pair_out, pair_in, peer_out, peer_in, result,
    load_sem, tile_send, tile_recv, table_send, table_recv, share_send, share_recv,
    peer_share_send, peer_share_recv, pair_share_send, pair_share_recv,
    hop_send, hop_recv, turn_send, turn_recv, back_send, back_recv, ret_send, ret_recv,
    swap_send, swap_recv, cross_send, cross_recv, last_send, last_recv, out_sem, clear_sem,
):
    steps, cols, rows = errs.shape
    rank = left.shape[1]
    scale = 1.0 / math.sqrt(rank)
    size = cols // CHUNKS
    half = rows // 2
    part = half // PIECES
    own = rows // lanes
    sub = own // SUBS
    width = turned.shape[2]
    others = lanes // 2 - 1
    blk = lax.axis_index("blk")
    lane = lax.axis_index("lane")
    odd = lax.rem(blk, 2)
    partner = blk + 1 - 2 * odd
    ahead = lax.rem(blk + 1, blocks)
    behind = lax.rem(blk + blocks - 1, blocks)
    ahead2 = lax.rem(blk + 2, blocks)
    behind2 = lax.rem(blk + blocks - 2, blocks)
    side = lax.rem(lane, 2)
    pair = lane + 1 - 2 * side
    peers = [lax.rem(lane + 2 * hop, lanes) for hop in range(1, lanes // 2)]
    sources = [lax.rem(lane + lanes - 2 * hop, lanes) for hop in range(1, lanes // 2)]
    mine = pl.multiple_of(side * half, half)
    other = pl.multiple_of((1 - side) * half, half)

    barrier = pltpu.get_barrier_semaphore()
    for target in (partner, behind, behind2):
        pl.semaphore_signal(barrier, inc=1, device_id={"blk": target}, device_id_type=MESH)
    for friend in [pair] + peers:
        pl.semaphore_signal(barrier, inc=1, device_id={"lane": friend}, device_id_type=MESH)
    pl.semaphore_signal(barrier, inc=1, device_id={"blk": ahead2, "lane": lane}, device_id_type=MESH)
    pl.semaphore_signal(barrier, inc=1, device_id={"blk": ahead2, "lane": pair}, device_id_type=MESH)

    def remote(source, target, send, recv, **place):
        return pltpu.make_async_remote_copy(
            src_ref=source, dst_ref=target, send_sem=send, recv_sem=recv,
            device_id=place, device_id_type=MESH,
        )

    def chunk(k):
        return pl.ds(pl.multiple_of(k * size, size), size)

    natural = [s for s in range(steps) if s != GUEST]
    loads = [
        pltpu.make_async_copy(shift_hbm, shift, load_sem.at[0]),
        pltpu.make_async_copy(codes_hbm, codes, load_sem.at[1]),
        pltpu.make_async_copy(right_hbm.at[0], first, load_sem.at[2]),
        pltpu.make_async_copy(left_hbm, left, load_sem.at[3]),
    ]
    for n, s in enumerate(natural):
        loads.append(pltpu.make_async_copy(obs_hbm.at[0, s], obs.at[n], load_sem.at[4 + n]))
    for copy in loads:
        copy.start()

    def piece(owner, u):
        return pl.ds(pl.multiple_of(owner * own + u * sub, sub), sub)

    def lend(u):
        span = piece(lane, u)
        return remote(left_hbm.at[span], left_g.at[span], share_send.at[u], share_recv.at[u], blk=partner)

    def lend_peer(m, u):
        span = piece(lane, u)
        return remote(left_g.at[span], left_g.at[span], peer_share_send.at[m, u], peer_share_recv.at[m, u], lane=peers[m])

    def lend_pair(m, u):
        span = piece(lane if m == 0 else sources[m - 1], u)
        return remote(left_g.at[span], left_g.at[span], pair_share_send.at[m, u], pair_share_recv.at[m, u], lane=pair)

    def give(k):
        span = chunk(k)
        return remote(obs_hbm.at[0, GUEST, span], obs_g.at[span], tile_send.at[k], tile_recv.at[k], blk=partner)

    tables = [
        remote(codes_hbm, codes_g, table_send.at[0], table_recv.at[0], blk=partner),
        remote(shift_hbm, shift_g, table_send.at[1], table_recv.at[1], blk=partner),
    ]

    def hop(k):
        span = chunk(k)
        return remote(hop_out.at[span], hop_in.at[span], hop_send.at[k], hop_recv.at[k], blk=ahead2)

    def cross_over(k):
        span = chunk(k)
        return remote(turn_out.at[span], turn_in.at[span], turn_send.at[k], turn_recv.at[k], blk=ahead)

    def turn(s, table):
        for start in range(0, cols, width):
            span = pl.ds(start, width)
            turned[s, span, :] = jnp.transpose(jnp.broadcast_to(table[0, pl.ds(s, 1), span], (width, width)))

    def error_of(k, s, block, factor, words, target):
        span = chunk(k)
        shifts = jnp.concatenate([turned[s, span, :]] * (rows // width), axis=1)
        seen = (jnp.right_shift(words[...], shifts) & 1) == 1
        predicted = lax.dot_general(
            block, factor[...], (((1,), (1,)), ((), ())), preferred_element_type=jnp.float32
        )
        error = predicted * scale - target[span, :].astype(jnp.float32)
        return jnp.where(seen, error, 0.0).astype(jnp.bfloat16)

    def stepped(error, block, factor):
        move = jnp.dot(error, factor[...], preferred_element_type=jnp.float32)
        return (block.astype(jnp.float32) - step_right * scale * move).astype(jnp.bfloat16)

    def tile(k, s, source, target, guest=False):
        span = chunk(k)
        block = source[span, :]
        if guest:
            factor, words, wanted = left_g, codes_g, obs_g
        else:
            factor, words, wanted = left, codes, obs.at[natural.index(s)]
        error = error_of(k, s, block, factor, words, wanted)
        errs[s, span, :] = error
        target[span, :] = stepped(error, block, factor)

    def outer(error, block):
        return lax.dot_general(error, block, (((0,), (0,)), ((), ())), preferred_element_type=jnp.float32)

    loads[0].wait()
    turn(0, shift)
    pl.semaphore_wait(barrier, 5 + 1 + len(peers))
    for u in range(SUBS):
        lend(u).start()
    for copy in tables:
        copy.start()
    for k in range(CHUNKS):
        give(k).start()
    for copy in loads[1:5]:
        copy.wait()

    def relay():
        for u in range(SUBS):
            lend(u).wait_recv()
            for m in range(others):
                lend_peer(m, u).start()
            lend_pair(0, u).start()

    def gather():
        for u in range(SUBS):
            for m in range(others):
                lend_peer(m, u).wait_recv()
                lend_pair(1 + m, u).start()
        for copy in tables:
            copy.wait_recv()
        turn(GUEST, shift_g)
        for m in range(1 + others):
            for u in range(SUBS):
                lend_pair(m, u).wait_recv()

    back = remote(back_out, back_in, back_send.at[0], back_recv.at[0], lane=pair)

    def send_back():
        back_out[...] = grad_g[pl.ds(other, half), :].astype(jnp.bfloat16)
        back.start()

    @pl.when(odd == 0)
    def _():
        pl.loop(0, CHUNKS)(lambda k: tile(k, 0, first, inner))
        relay()
        grad[...] = outer(errs[0], first[...])
        turn(2, shift)
        turn(3, shift)
        gather()

        def guest_visit(k):
            give(k).wait_recv()
            tile(k, GUEST, inner, hop_out, guest=True)
            hop(k).start()

        def home_visit(k):
            hop(k).wait_recv()
            tile(k, 2, hop_in, turn_out)
            cross_over(k).start()

        loads[5].wait()
        pl.loop(0, LAG)(guest_visit)
        pl.loop(0, CHUNKS)(lambda k: give(k).wait_send())
        pl.semaphore_signal(clear_sem, inc=1, device_id={"lane": pair}, device_id_type=MESH)
        pl.semaphore_wait(clear_sem, 1)

        @pl.loop(LAG, CHUNKS)
        def _(k):
            home_visit(k - LAG)
            guest_visit(k)

        grad_g[...] = outer(errs[GUEST], inner[...])
        send_back()
        pl.loop(CHUNKS - LAG, CHUNKS)(home_visit)
        grad[...] += outer(errs[2], hop_in[...])

    @pl.when(odd == 1)
    def _():
        @pl.loop(0, CHUNKS)
        def _(k):
            tile(k, 0, first, hop_out)
            hop(k).start()

        relay()
        grad[...] = outer(errs[0], first[...])
        turn(2, shift)
        turn(3, shift)
        gather()
        loads[5].wait()

        def visits(k):
            give(k).wait_recv()
            hop(k).wait_recv()
            tile(k, GUEST, hop_in, inner, guest=True)
            tile(k, 2, inner, turn_out)

        pl.loop(0, HOLD)(visits)
        pl.loop(0, CHUNKS - EARLY)(lambda k: give(k).wait_send())
        for place_lane in (lane, pair):
            pl.semaphore_signal(clear_sem, inc=1, device_id={"blk": behind2, "lane": place_lane}, device_id_type=MESH)
        pl.semaphore_wait(clear_sem, 2)
        pl.loop(0, HOLD)(lambda k: cross_over(k).start())

        @pl.loop(HOLD, CHUNKS)
        def _(k):
            visits(k)
            cross_over(k).start()

        grad_g[...] = outer(errs[GUEST], hop_in[...])
        send_back()
        grad[...] += outer(errs[2], inner[...])
        pl.loop(CHUNKS - EARLY, CHUNKS)(lambda k: give(k).wait_send())

    def give_back(q):
        span = pl.ds(q * part, part)
        return remote(ret_out.at[span], ret_in.at[span], ret_send.at[q], ret_recv.at[q], blk=partner)

    back.wait_recv()
    ret_out[...] = (grad_g[pl.ds(mine, half), :] + back_in[...].astype(jnp.float32)).astype(jnp.bfloat16)
    for q in range(PIECES):
        give_back(q).start()

    loads[6].wait()
    last = steps - 1

    @pl.loop(0, CHUNKS - 1)
    def _(k):
        cross_over(k).wait_recv()
        tile(k, last, turn_in, final)

    early = (CHUNKS - 1) * size
    grad[...] += outer(errs[last, pl.ds(0, early)], turn_in[pl.ds(0, early)])
    tail = pl.ds(early, size)
    cross_over(CHUNKS - 1).wait_recv()
    errs[last, tail, :] = error_of(CHUNKS - 1, last, turn_in[tail, :], left, codes, obs.at[natural.index(last)])

    def finish(start):
        span = pl.ds(start, half)
        return grad[span, :] + outer(errs[last, tail, span], turn_in[tail, :])

    def swap(q):
        span = pl.ds(q * part, part)
        return remote(pair_out.at[span], pair_in.at[span], swap_send.at[q], swap_recv.at[q], lane=pair)

    def cross(m, q):
        span = pl.ds(q * part, part)
        return remote(peer_out.at[span], peer_in.at[m, span], cross_send.at[m, q], cross_recv.at[m, q], lane=peers[m])

    def share(q):
        span = pl.ds(pl.multiple_of(mine + q * part, part), part)
        return remote(result.at[span], result.at[span], last_send.at[q], last_recv.at[q], lane=pair)

    pair_out[...] = finish(other).astype(jnp.bfloat16)
    for q in range(PIECES):
        swap(q).start()
    grad[pl.ds(mine, half), :] = finish(mine)
    for q in range(PIECES):
        span = pl.ds(q * part, part)
        swap(q).wait_recv()
        give_back(q).wait_recv()
        peer_out[span, :] = (
            grad[pl.ds(pl.multiple_of(mine + q * part, part), part), :]
            + pair_in[span, :].astype(jnp.float32)
            + ret_in[span, :].astype(jnp.float32)
        ).astype(jnp.bfloat16)
        for m in range(len(peers)):
            cross(m, q).start()

    final[tail, :] = stepped(errs[last, tail, :], turn_in[tail, :], left)

    outs = [
        pltpu.make_async_copy(final, right_out.at[0], out_sem.at[0]),
        pltpu.make_async_copy(result.at[pl.ds(mine, half)], left_out.at[pl.ds(mine, half)], out_sem.at[1]),
        pltpu.make_async_copy(result.at[pl.ds(other, half)], left_out.at[pl.ds(other, half)], out_sem.at[2]),
    ]
    outs[0].start()
    for u in range(SUBS):
        lend(u).wait_send()
        for m in range(others):
            lend_peer(m, u).wait_send()
        for m in range(1 + others):
            lend_pair(m, u).wait_send()
    for copy in tables:
        copy.wait_send()

    @pl.loop(0, CHUNKS)
    def _(k):
        hop(k).wait_send()
        cross_over(k).wait_send()

    back.wait_send()

    for q in range(PIECES):
        span = pl.ds(q * part, part)
        here = pl.ds(pl.multiple_of(mine + q * part, part), part)
        total = peer_out[span, :].astype(jnp.float32)
        for m in range(len(peers)):
            cross(m, q).wait_recv()
            total = total + peer_in[m, span, :].astype(jnp.float32)
        result[here, :] = (left[here, :].astype(jnp.float32) - step_left * scale * total).astype(jnp.bfloat16)
        share(q).start()
    outs[1].start()
    for q in range(PIECES):
        share(q).wait_recv()
    outs[2].start()
    for q in range(PIECES):
        give_back(q).wait_send()
        swap(q).wait_send()
        for m in range(len(peers)):
            cross(m, q).wait_send()
        share(q).wait_send()
    for copy in outs:
        copy.wait()


def place(left_from, right_from, left_to, right_to, held, in_sem, out_sem):
    pairs = [(left_from, left_to), (right_from.at[0], right_to.at[0])]
    rows = left_from.shape[0] // PARTS
    moves = []
    for which, (source, target) in enumerate(pairs):
        for p in range(PARTS):
            span = pl.ds(p * rows, rows)
            moves.append((
                pltpu.make_async_copy(source.at[span], held.at[which, span], in_sem.at[which, p]),
                pltpu.make_async_copy(held.at[which, span], target.at[span], out_sem.at[which, p]),
            ))
    for inward, _ in moves:
        inward.start()
    for inward, outward in moves:
        inward.wait()
        outward.start()
    for _, outward in moves:
        outward.wait()


def solution(mesh):
    blocks = mesh.shape["blk"]
    lanes = mesh.shape["lane"]

    def local(left_factor, right_factor, observed, row_codes, shift_codes):
        rows, rank = left_factor.shape
        _, steps, cols, _ = observed.shape
        bf16, f32, i32 = jnp.bfloat16, jnp.float32, jnp.int32
        dma = pltpu.SemaphoreType.DMA
        vmem = pltpu.VMEM
        hbm = pl.BlockSpec(memory_space=pltpu.HBM)
        others = lanes // 2 - 1
        half = rows // 2
        shapes = (
            jax.ShapeDtypeStruct((rows, rank), bf16),
            jax.ShapeDtypeStruct((1, cols, rank), bf16),
        )
        results = pl.pallas_call(
            functools.partial(kernel, blocks, lanes),
            out_shape=shapes,
            in_specs=[hbm] * 5,
            out_specs=(hbm, hbm),
            scratch_shapes=[
                vmem((rows, rank), bf16),
                vmem((rows, rank), bf16),
                *[vmem((cols, rank), bf16)] * 7,
                vmem((steps - 1, cols, rows), bf16),
                vmem((cols, rows), bf16),
                vmem((1, rows), i32),
                vmem((1, rows), i32),
                vmem((1, steps, cols), i32),
                vmem((1, steps, cols), i32),
                vmem((steps, cols, WIDTH), i32),
                vmem((steps, cols, rows), bf16),
                vmem((rows, rank), f32),
                vmem((rows, rank), f32),
                *[vmem((half, rank), bf16)] * 7,
                vmem((others, half, rank), bf16),
                vmem((rows, rank), bf16),
                dma((4 + steps - 1,)),
                dma((CHUNKS,)), dma((CHUNKS,)),
                dma((2,)), dma((2,)),
                dma((SUBS,)), dma((SUBS,)),
                dma((others, SUBS)), dma((others, SUBS)),
                dma((1 + others, SUBS)), dma((1 + others, SUBS)),
                dma((CHUNKS,)), dma((CHUNKS,)),
                dma((CHUNKS,)), dma((CHUNKS,)),
                dma((1,)), dma((1,)),
                dma((PIECES,)), dma((PIECES,)),
                dma((PIECES,)), dma((PIECES,)),
                dma((others, PIECES)), dma((others, PIECES)),
                dma((PIECES,)), dma((PIECES,)),
                dma((3,)),
                pltpu.SemaphoreType.REGULAR,
            ],
            compiler_params=pltpu.CompilerParams(
                collective_id=0, has_side_effects=True, vmem_limit_bytes=67043328
            ),
        )(
            left_factor, right_factor, observed,
            row_codes.reshape(1, rows), shift_codes,
        )
        return pl.pallas_call(
            place,
            out_shape=shapes,
            in_specs=[hbm] * 2,
            out_specs=(hbm, hbm),
            scratch_shapes=[pltpu.VMEM((2, max(rows, cols), rank), bf16), dma((2, PARTS)), dma((2, PARTS))],
            compiler_params=pltpu.CompilerParams(vmem_limit_bytes=67043328),
        )(*results)

    in_specs = (
        P("blk", None),
        P("lane", "blk", None),
        P("lane", None, None, "blk"),
        P("blk"),
        P("lane", None, "blk"),
    )
    out_specs = (P("blk", None), P("lane", "blk", None))
    return jax.shard_map(local, mesh=mesh, in_specs=in_specs, out_specs=out_specs, check_vma=False)
```

```python
import functools
import math

import jax
import jax.numpy as jnp
from jax import lax
from jax.experimental import pallas as pl
from jax.experimental.pallas import tpu as pltpu
from jax.sharding import PartitionSpec as P

step_right = 0.25
step_left = 0.1

CHUNKS = 8
LAG = 5
HOLD = 4
EARLY = 2
WIDTH = 128
PIECES = 4
SUBS = 2
GUEST = 1
VMEM_BYTES = 67043328
MESH = pl.DeviceIdType.MESH


def kernel(
    blocks, lanes,
    left_hbm, right_hbm, obs_hbm, codes_hbm, shift_hbm,
    result, final_out,
    left, left_g, first, inner, hop_out, hop_in, turn_out, turn_in,
    obs, obs_g, codes, codes_g, shift, shift_g, turned, errs,
    grad, grad_g, back_out, back_in, ret_out, ret_in, pair_out, pair_in, peer_out, peer_in,
    load_sem, tile_send, tile_recv, table_send, table_recv, share_send, share_recv,
    peer_share_send, peer_share_recv, pair_share_send, pair_share_recv,
    hop_send, hop_recv, turn_send, turn_recv, back_send, back_recv, ret_send, ret_recv,
    swap_send, swap_recv, cross_send, cross_recv, last_send, last_recv, clear_sem,
):
    steps, cols, rows = errs.shape
    final = final_out.at[0]
    rank = left.shape[1]
    scale = 1.0 / math.sqrt(rank)
    size = cols // CHUNKS
    half = rows // 2
    part = half // PIECES
    own = rows // lanes
    sub = own // SUBS
    width = turned.shape[2]
    others = lanes // 2 - 1
    blk = lax.axis_index("blk")
    lane = lax.axis_index("lane")
    odd = lax.rem(blk, 2)
    partner = blk + 1 - 2 * odd
    ahead = lax.rem(blk + 1, blocks)
    behind = lax.rem(blk + blocks - 1, blocks)
    ahead2 = lax.rem(blk + 2, blocks)
    behind2 = lax.rem(blk + blocks - 2, blocks)
    side = lax.rem(lane, 2)
    pair = lane + 1 - 2 * side
    peers = [lax.rem(lane + 2 * hop, lanes) for hop in range(1, lanes // 2)]
    sources = [lax.rem(lane + lanes - 2 * hop, lanes) for hop in range(1, lanes // 2)]
    mine = pl.multiple_of(side * half, half)
    other = pl.multiple_of((1 - side) * half, half)

    barrier = pltpu.get_barrier_semaphore()
    for target in (partner, behind, behind2):
        pl.semaphore_signal(barrier, inc=1, device_id={"blk": target}, device_id_type=MESH)
    for friend in [pair] + peers:
        pl.semaphore_signal(barrier, inc=1, device_id={"lane": friend}, device_id_type=MESH)
    pl.semaphore_signal(barrier, inc=1, device_id={"blk": ahead2, "lane": lane}, device_id_type=MESH)
    pl.semaphore_signal(barrier, inc=1, device_id={"blk": ahead2, "lane": pair}, device_id_type=MESH)

    def remote(source, target, send, recv, **place):
        return pltpu.make_async_remote_copy(
            src_ref=source, dst_ref=target, send_sem=send, recv_sem=recv,
            device_id=place, device_id_type=MESH,
        )

    def chunk(k):
        return pl.ds(pl.multiple_of(k * size, size), size)

    natural = [s for s in range(steps) if s != GUEST]
    loads = [
        pltpu.make_async_copy(shift_hbm, shift, load_sem.at[0]),
        pltpu.make_async_copy(codes_hbm, codes, load_sem.at[1]),
        pltpu.make_async_copy(right_hbm.at[0], first, load_sem.at[2]),
        pltpu.make_async_copy(left_hbm, left, load_sem.at[3]),
    ]
    for n, s in enumerate(natural):
        loads.append(pltpu.make_async_copy(obs_hbm.at[0, s], obs.at[n], load_sem.at[4 + n]))
    for copy in loads:
        copy.start()

    def piece(owner, u):
        return pl.ds(pl.multiple_of(owner * own + u * sub, sub), sub)

    def lend(u):
        span = piece(lane, u)
        return remote(left_hbm.at[span], left_g.at[span], share_send.at[u], share_recv.at[u], blk=partner)

    def lend_peer(m, u):
        span = piece(lane, u)
        return remote(left_g.at[span], left_g.at[span], peer_share_send.at[m, u], peer_share_recv.at[m, u], lane=peers[m])

    def lend_pair(m, u):
        span = piece(lane if m == 0 else sources[m - 1], u)
        return remote(left_g.at[span], left_g.at[span], pair_share_send.at[m, u], pair_share_recv.at[m, u], lane=pair)

    def give(k):
        span = chunk(k)
        return remote(obs_hbm.at[0, GUEST, span], obs_g.at[span], tile_send.at[k], tile_recv.at[k], blk=partner)

    tables = [
        remote(codes_hbm, codes_g, table_send.at[0], table_recv.at[0], blk=partner),
        remote(shift_hbm, shift_g, table_send.at[1], table_recv.at[1], blk=partner),
    ]

    def hop(k):
        span = chunk(k)
        return remote(hop_out.at[span], hop_in.at[span], hop_send.at[k], hop_recv.at[k], blk=ahead2)

    def cross_over(k):
        span = chunk(k)
        return remote(turn_out.at[span], turn_in.at[span], turn_send.at[k], turn_recv.at[k], blk=ahead)

    def turn(s, table):
        for start in range(0, cols, width):
            span = pl.ds(start, width)
            turned[s, span, :] = jnp.transpose(jnp.broadcast_to(table[0, pl.ds(s, 1), span], (width, width)))

    def error_of(k, s, block, factor, words, target):
        span = chunk(k)
        shifts = jnp.concatenate([turned[s, span, :]] * (rows // width), axis=1)
        seen = (jnp.right_shift(words[...], shifts) & 1) == 1
        predicted = lax.dot_general(
            block, factor[...], (((1,), (1,)), ((), ())), preferred_element_type=jnp.float32
        )
        error = predicted * scale - target[span, :].astype(jnp.float32)
        return jnp.where(seen, error, 0.0).astype(jnp.bfloat16)

    def stepped(error, block, factor):
        move = jnp.dot(error, factor[...], preferred_element_type=jnp.float32)
        return (block.astype(jnp.float32) - step_right * scale * move).astype(jnp.bfloat16)

    def tile(k, s, source, target, guest=False):
        span = chunk(k)
        block = source[span, :]
        if guest:
            factor, words, wanted = left_g, codes_g, obs_g
        else:
            factor, words, wanted = left, codes, obs.at[natural.index(s)]
        error = error_of(k, s, block, factor, words, wanted)
        errs[s, span, :] = error
        target[span, :] = stepped(error, block, factor)

    def outer(error, block):
        return lax.dot_general(error, block, (((0,), (0,)), ((), ())), preferred_element_type=jnp.float32)

    loads[0].wait()
    turn(0, shift)
    pl.semaphore_wait(barrier, 5 + 1 + len(peers))
    for u in range(SUBS):
        lend(u).start()
    for copy in tables:
        copy.start()
    for k in range(CHUNKS):
        give(k).start()
    for copy in loads[1:5]:
        copy.wait()

    def relay():
        for u in range(SUBS):
            lend(u).wait_recv()
            for m in range(others):
                lend_peer(m, u).start()
            lend_pair(0, u).start()

    def gather():
        for u in range(SUBS):
            for m in range(others):
                lend_peer(m, u).wait_recv()
                lend_pair(1 + m, u).start()
        for copy in tables:
            copy.wait_recv()
        turn(GUEST, shift_g)
        for m in range(1 + others):
            for u in range(SUBS):
                lend_pair(m, u).wait_recv()

    back = remote(back_out, back_in, back_send.at[0], back_recv.at[0], lane=pair)

    def send_back():
        back_out[...] = grad_g[pl.ds(other, half), :].astype(jnp.bfloat16)
        back.start()

    @pl.when(odd == 0)
    def _():
        pl.loop(0, CHUNKS)(lambda k: tile(k, 0, first, inner))
        relay()
        grad[...] = outer(errs[0], first[...])
        turn(2, shift)
        turn(3, shift)
        gather()

        def guest_visit(k):
            give(k).wait_recv()
            tile(k, GUEST, inner, hop_out, guest=True)
            hop(k).start()

        def home_visit(k):
            hop(k).wait_recv()
            tile(k, 2, hop_in, turn_out)
            cross_over(k).start()

        loads[5].wait()
        pl.loop(0, LAG)(guest_visit)
        pl.loop(0, CHUNKS)(lambda k: give(k).wait_send())
        pl.semaphore_signal(clear_sem, inc=1, device_id={"lane": pair}, device_id_type=MESH)
        pl.semaphore_wait(clear_sem, 1)

        @pl.loop(LAG, CHUNKS)
        def _(k):
            home_visit(k - LAG)
            guest_visit(k)

        grad_g[...] = outer(errs[GUEST], inner[...])
        send_back()
        pl.loop(CHUNKS - LAG, CHUNKS)(home_visit)
        grad[...] += outer(errs[2], hop_in[...])

    @pl.when(odd == 1)
    def _():
        @pl.loop(0, CHUNKS)
        def _(k):
            tile(k, 0, first, hop_out)
            hop(k).start()

        relay()
        grad[...] = outer(errs[0], first[...])
        turn(2, shift)
        turn(3, shift)
        gather()
        loads[5].wait()

        def visits(k):
            give(k).wait_recv()
            hop(k).wait_recv()
            tile(k, GUEST, hop_in, inner, guest=True)
            tile(k, 2, inner, turn_out)

        pl.loop(0, HOLD)(visits)
        pl.loop(0, CHUNKS - EARLY)(lambda k: give(k).wait_send())
        for place_lane in (lane, pair):
            pl.semaphore_signal(clear_sem, inc=1, device_id={"blk": behind2, "lane": place_lane}, device_id_type=MESH)
        pl.semaphore_wait(clear_sem, 2)
        pl.loop(0, HOLD)(lambda k: cross_over(k).start())

        @pl.loop(HOLD, CHUNKS)
        def _(k):
            visits(k)
            cross_over(k).start()

        grad_g[...] = outer(errs[GUEST], hop_in[...])
        send_back()
        grad[...] += outer(errs[2], inner[...])
        pl.loop(CHUNKS - EARLY, CHUNKS)(lambda k: give(k).wait_send())

    def give_back(q):
        span = pl.ds(q * part, part)
        return remote(ret_out.at[span], ret_in.at[span], ret_send.at[q], ret_recv.at[q], blk=partner)

    back.wait_recv()
    ret_out[...] = (grad_g[pl.ds(mine, half), :] + back_in[...].astype(jnp.float32)).astype(jnp.bfloat16)
    for q in range(PIECES):
        give_back(q).start()

    loads[6].wait()
    last = steps - 1

    @pl.loop(0, CHUNKS - 1)
    def _(k):
        cross_over(k).wait_recv()
        tile(k, last, turn_in, final)

    early = (CHUNKS - 1) * size
    grad[...] += outer(errs[last, pl.ds(0, early)], turn_in[pl.ds(0, early)])
    tail = pl.ds(early, size)
    cross_over(CHUNKS - 1).wait_recv()
    errs[last, tail, :] = error_of(CHUNKS - 1, last, turn_in[tail, :], left, codes, obs.at[natural.index(last)])

    def finish(start):
        span = pl.ds(start, half)
        return grad[span, :] + outer(errs[last, tail, span], turn_in[tail, :])

    def swap(q):
        span = pl.ds(q * part, part)
        return remote(pair_out.at[span], pair_in.at[span], swap_send.at[q], swap_recv.at[q], lane=pair)

    def cross(m, q):
        span = pl.ds(q * part, part)
        return remote(peer_out.at[span], peer_in.at[m, span], cross_send.at[m, q], cross_recv.at[m, q], lane=peers[m])

    def share(q):
        span = pl.ds(pl.multiple_of(mine + q * part, part), part)
        return remote(result.at[span], result.at[span], last_send.at[q], last_recv.at[q], lane=pair)

    pair_out[...] = finish(other).astype(jnp.bfloat16)
    for q in range(PIECES):
        swap(q).start()
    grad[pl.ds(mine, half), :] = finish(mine)
    for q in range(PIECES):
        span = pl.ds(q * part, part)
        swap(q).wait_recv()
        give_back(q).wait_recv()
        peer_out[span, :] = (
            grad[pl.ds(pl.multiple_of(mine + q * part, part), part), :]
            + pair_in[span, :].astype(jnp.float32)
            + ret_in[span, :].astype(jnp.float32)
        ).astype(jnp.bfloat16)
        for m in range(len(peers)):
            cross(m, q).start()

    final[tail, :] = stepped(errs[last, tail, :], turn_in[tail, :], left)

    for u in range(SUBS):
        lend(u).wait_send()
        for m in range(others):
            lend_peer(m, u).wait_send()
        for m in range(1 + others):
            lend_pair(m, u).wait_send()
    for copy in tables:
        copy.wait_send()

    @pl.loop(0, CHUNKS)
    def _(k):
        hop(k).wait_send()
        cross_over(k).wait_send()

    back.wait_send()

    for q in range(PIECES):
        span = pl.ds(q * part, part)
        here = pl.ds(pl.multiple_of(mine + q * part, part), part)
        total = peer_out[span, :].astype(jnp.float32)
        for m in range(len(peers)):
            cross(m, q).wait_recv()
            total = total + peer_in[m, span, :].astype(jnp.float32)
        result[here, :] = (left[here, :].astype(jnp.float32) - step_left * scale * total).astype(jnp.bfloat16)
        share(q).start()
    for q in range(PIECES):
        share(q).wait_recv()
    for q in range(PIECES):
        give_back(q).wait_send()
        swap(q).wait_send()
        for m in range(len(peers)):
            cross(m, q).wait_send()
        share(q).wait_send()


def place(left_from, right_from, left_to, right_to, sem):
    moves = [
        pltpu.make_async_copy(left_from, left_to, sem.at[0]),
        pltpu.make_async_copy(right_from, right_to, sem.at[1]),
    ]
    for move in moves:
        move.start()
    for move in moves:
        move.wait()


def solution(mesh):
    blocks = mesh.shape["blk"]
    lanes = mesh.shape["lane"]

    def local(left_factor, right_factor, observed, row_codes, shift_codes):
        rows, rank = left_factor.shape
        _, steps, cols, _ = observed.shape
        bf16, f32, i32 = jnp.bfloat16, jnp.float32, jnp.int32
        dma = pltpu.SemaphoreType.DMA
        vmem = pltpu.VMEM
        hbm = pl.BlockSpec(memory_space=pltpu.HBM)
        here = pl.BlockSpec(memory_space=pltpu.VMEM)
        room = VMEM_BYTES - 2 * (rows + cols) * rank
        others = lanes // 2 - 1
        half = rows // 2
        shapes = (
            jax.ShapeDtypeStruct((rows, rank), bf16),
            jax.ShapeDtypeStruct((1, cols, rank), bf16),
        )
        results = pl.pallas_call(
            functools.partial(kernel, blocks, lanes),
            out_shape=(vmem((rows, rank), bf16), vmem((1, cols, rank), bf16)),
            in_specs=[hbm] * 5,
            out_specs=(here, here),
            scratch_shapes=[
                vmem((rows, rank), bf16),
                vmem((rows, rank), bf16),
                *[vmem((cols, rank), bf16)] * 6,
                vmem((steps - 1, cols, rows), bf16),
                vmem((cols, rows), bf16),
                vmem((1, rows), i32),
                vmem((1, rows), i32),
                vmem((1, steps, cols), i32),
                vmem((1, steps, cols), i32),
                vmem((steps, cols, WIDTH), i32),
                vmem((steps, cols, rows), bf16),
                vmem((rows, rank), f32),
                vmem((rows, rank), f32),
                *[vmem((half, rank), bf16)] * 7,
                vmem((others, half, rank), bf16),
                dma((4 + steps - 1,)),
                dma((CHUNKS,)), dma((CHUNKS,)),
                dma((2,)), dma((2,)),
                dma((SUBS,)), dma((SUBS,)),
                dma((others, SUBS)), dma((others, SUBS)),
                dma((1 + others, SUBS)), dma((1 + others, SUBS)),
                dma((CHUNKS,)), dma((CHUNKS,)),
                dma((CHUNKS,)), dma((CHUNKS,)),
                dma((1,)), dma((1,)),
                dma((PIECES,)), dma((PIECES,)),
                dma((PIECES,)), dma((PIECES,)),
                dma((others, PIECES)), dma((others, PIECES)),
                dma((PIECES,)), dma((PIECES,)),
                pltpu.SemaphoreType.REGULAR,
            ],
            compiler_params=pltpu.CompilerParams(
                collective_id=0, has_side_effects=True, vmem_limit_bytes=room
            ),
        )(
            left_factor, right_factor, observed,
            row_codes.reshape(1, rows), shift_codes,
        )
        return pl.pallas_call(
            place,
            out_shape=shapes,
            in_specs=[here] * 2,
            out_specs=(hbm, hbm),
            scratch_shapes=[dma((2,))],
            compiler_params=pltpu.CompilerParams(vmem_limit_bytes=room),
        )(*[pltpu.with_memory_space_constraint(value, pltpu.VMEM) for value in results])

    in_specs = (
        P("blk", None),
        P("lane", "blk", None),
        P("lane", None, None, "blk"),
        P("blk"),
        P("lane", None, "blk"),
    )
    out_specs = (P("blk", None), P("lane", "blk", None))
    return jax.shard_map(local, mesh=mesh, in_specs=in_specs, out_specs=out_specs, check_vma=False)
```

```python
import functools
import math

import jax
import jax.numpy as jnp
from jax import lax
from jax.experimental import pallas as pl
from jax.experimental.pallas import tpu as pltpu
from jax.sharding import PartitionSpec as P

step_right = 0.25
step_left = 0.1

CHUNKS = 8
LAG = 5
HOLD = 4
EARLY = 2
WIDTH = 128
PIECES = 8
SUBS = 2
GUEST = 1
VMEM_BYTES = 67043328
MESH = pl.DeviceIdType.MESH


def kernel(
    blocks, lanes,
    left_hbm, right_hbm, obs_hbm, codes_hbm, shift_hbm,
    result, final_out,
    left, left_g, first, inner, hop_out, hop_in, turn_out, turn_in,
    obs, obs_g, codes, codes_g, shift, shift_g, turned, errs,
    grad, grad_g, back_out, back_in, ret_out, ret_in, pair_out, pair_in, peer_out, peer_in,
    load_sem, tile_send, tile_recv, table_send, table_recv, share_send, share_recv,
    peer_share_send, peer_share_recv, pair_share_send, pair_share_recv,
    hop_send, hop_recv, turn_send, turn_recv, back_send, back_recv, ret_send, ret_recv,
    swap_send, swap_recv, cross_send, cross_recv, last_send, last_recv, clear_sem, go_sem,
):
    steps, cols, rows = errs.shape
    final = final_out.at[0]
    rank = left.shape[1]
    scale = 1.0 / math.sqrt(rank)
    size = cols // CHUNKS
    half = rows // 2
    part = half // PIECES
    own = rows // lanes
    sub = own // SUBS
    width = turned.shape[2]
    others = lanes // 2 - 1
    blk = lax.axis_index("blk")
    lane = lax.axis_index("lane")
    odd = lax.rem(blk, 2)
    partner = blk + 1 - 2 * odd
    ahead = lax.rem(blk + 1, blocks)
    behind = lax.rem(blk + blocks - 1, blocks)
    ahead2 = lax.rem(blk + 2, blocks)
    behind2 = lax.rem(blk + blocks - 2, blocks)
    side = lax.rem(lane, 2)
    pair = lane + 1 - 2 * side
    peers = [lax.rem(lane + 2 * hop, lanes) for hop in range(1, lanes // 2)]
    sources = [lax.rem(lane + lanes - 2 * hop, lanes) for hop in range(1, lanes // 2)]
    mine = pl.multiple_of(side * half, half)
    other = pl.multiple_of((1 - side) * half, half)

    barrier = pltpu.get_barrier_semaphore()
    for target in (partner, behind, behind2):
        pl.semaphore_signal(barrier, inc=1, device_id={"blk": target}, device_id_type=MESH)
    for friend in [pair] + peers:
        pl.semaphore_signal(barrier, inc=1, device_id={"lane": friend}, device_id_type=MESH)

    def remote(source, target, send, recv, **place):
        return pltpu.make_async_remote_copy(
            src_ref=source, dst_ref=target, send_sem=send, recv_sem=recv,
            device_id=place, device_id_type=MESH,
        )

    def chunk(k):
        return pl.ds(pl.multiple_of(k * size, size), size)

    natural = [s for s in range(steps) if s != GUEST]
    loads = [
        pltpu.make_async_copy(shift_hbm, shift, load_sem.at[0]),
        pltpu.make_async_copy(codes_hbm, codes, load_sem.at[1]),
        pltpu.make_async_copy(right_hbm.at[0], first, load_sem.at[2]),
        pltpu.make_async_copy(left_hbm, left, load_sem.at[3]),
    ]
    for n, s in enumerate(natural):
        loads.append(pltpu.make_async_copy(obs_hbm.at[0, s], obs.at[n], load_sem.at[4 + n]))
    for copy in loads:
        copy.start()

    def piece(owner, u):
        return pl.ds(pl.multiple_of(owner * own + u * sub, sub), sub)

    def lend(u):
        span = piece(lane, u)
        return remote(left_hbm.at[span], left_g.at[span], share_send.at[u], share_recv.at[u], blk=partner)

    def lend_peer(m, u):
        span = piece(lane, u)
        return remote(left_g.at[span], left_g.at[span], peer_share_send.at[m, u], peer_share_recv.at[m, u], lane=peers[m])

    def lend_pair(m, u):
        span = piece(lane if m == 0 else sources[m - 1], u)
        return remote(left_g.at[span], left_g.at[span], pair_share_send.at[m, u], pair_share_recv.at[m, u], lane=pair)

    def give(k):
        span = chunk(k)
        return remote(obs_hbm.at[0, GUEST, span], obs_g.at[span], tile_send.at[k], tile_recv.at[k], blk=partner)

    tables = [
        remote(codes_hbm, codes_g, table_send.at[0], table_recv.at[0], blk=partner),
        remote(shift_hbm, shift_g, table_send.at[1], table_recv.at[1], blk=partner),
    ]

    def hop(k):
        span = chunk(k)
        return remote(hop_out.at[span], hop_in.at[span], hop_send.at[k], hop_recv.at[k], blk=ahead2)

    def cross_over(k):
        span = chunk(k)
        return remote(turn_out.at[span], turn_in.at[span], turn_send.at[k], turn_recv.at[k], blk=ahead)

    def turn(s, table):
        for start in range(0, cols, width):
            span = pl.ds(start, width)
            turned[s, span, :] = jnp.transpose(jnp.broadcast_to(table[0, pl.ds(s, 1), span], (width, width)))

    def error_of(k, s, block, factor, words, target):
        span = chunk(k)
        shifts = jnp.concatenate([turned[s, span, :]] * (rows // width), axis=1)
        seen = (jnp.right_shift(words[...], shifts) & 1) == 1
        predicted = lax.dot_general(
            block, factor[...], (((1,), (1,)), ((), ())), preferred_element_type=jnp.float32
        )
        error = predicted * scale - target[span, :].astype(jnp.float32)
        return jnp.where(seen, error, 0.0).astype(jnp.bfloat16)

    def stepped(error, block, factor):
        move = jnp.dot(error, factor[...], preferred_element_type=jnp.float32)
        return (block.astype(jnp.float32) - step_right * scale * move).astype(jnp.bfloat16)

    def tile(k, s, source, target, guest=False):
        span = chunk(k)
        block = source[span, :]
        if guest:
            factor, words, wanted = left_g, codes_g, obs_g
        else:
            factor, words, wanted = left, codes, obs.at[natural.index(s)]
        error = error_of(k, s, block, factor, words, wanted)
        errs[s, span, :] = error
        target[span, :] = stepped(error, block, factor)

    def outer(error, block):
        return lax.dot_general(error, block, (((0,), (0,)), ((), ())), preferred_element_type=jnp.float32)

    loads[0].wait()
    turn(0, shift)
    pl.semaphore_wait(barrier, 3 + 1 + len(peers))
    for u in range(SUBS):
        lend(u).start()
    for copy in tables:
        copy.start()
    for k in range(CHUNKS):
        give(k).start()
    for copy in loads[1:5]:
        copy.wait()

    def relay():
        for u in range(SUBS):
            lend(u).wait_recv()
            for m in range(others):
                lend_peer(m, u).start()
            lend_pair(0, u).start()

    def gather():
        for u in range(SUBS):
            for m in range(others):
                lend_peer(m, u).wait_recv()
                lend_pair(1 + m, u).start()
        for copy in tables:
            copy.wait_recv()
        turn(GUEST, shift_g)
        for m in range(1 + others):
            for u in range(SUBS):
                lend_pair(m, u).wait_recv()

    back = remote(back_out, back_in, back_send.at[0], back_recv.at[0], lane=pair)

    def send_back():
        back_out[...] = grad_g[pl.ds(other, half), :].astype(jnp.bfloat16)
        back.start()

    @pl.when(odd == 0)
    def _():
        pl.loop(0, CHUNKS)(lambda k: tile(k, 0, first, inner))
        relay()
        grad[...] = outer(errs[0], first[...])
        turn(2, shift)
        turn(3, shift)
        gather()

        def guest_visit(k):
            give(k).wait_recv()
            tile(k, GUEST, inner, hop_out, guest=True)
            hop(k).start()

        def home_visit(k):
            hop(k).wait_recv()
            tile(k, 2, hop_in, turn_out)
            cross_over(k).start()

        loads[5].wait()
        pl.loop(0, LAG)(guest_visit)
        pl.loop(0, CHUNKS)(lambda k: give(k).wait_send())
        pl.semaphore_signal(clear_sem, inc=1, device_id={"lane": pair}, device_id_type=MESH)
        pl.semaphore_wait(clear_sem, 1)

        @pl.loop(LAG, CHUNKS)
        def _(k):
            home_visit(k - LAG)
            guest_visit(k)

        grad_g[...] = outer(errs[GUEST], inner[...])
        send_back()
        pl.loop(CHUNKS - LAG, CHUNKS)(home_visit)
        grad[...] += outer(errs[2], hop_in[...])

    @pl.when(odd == 1)
    def _():
        @pl.loop(0, CHUNKS)
        def _(k):
            tile(k, 0, first, hop_out)
            hop(k).start()

        relay()
        grad[...] = outer(errs[0], first[...])
        turn(2, shift)
        turn(3, shift)
        gather()
        loads[5].wait()

        def visits(k):
            give(k).wait_recv()
            hop(k).wait_recv()
            tile(k, GUEST, hop_in, inner, guest=True)
            tile(k, 2, inner, turn_out)

        pl.loop(0, HOLD)(visits)
        pl.loop(0, CHUNKS - EARLY)(lambda k: give(k).wait_send())
        pl.semaphore_signal(clear_sem, inc=1, device_id={"lane": pair}, device_id_type=MESH)
        pl.semaphore_wait(clear_sem, 1)
        pl.semaphore_signal(go_sem, inc=1, device_id={"blk": behind2}, device_id_type=MESH)
        pl.semaphore_wait(go_sem, 1)
        pl.loop(0, HOLD)(lambda k: cross_over(k).start())

        @pl.loop(HOLD, CHUNKS)
        def _(k):
            visits(k)
            cross_over(k).start()

        grad_g[...] = outer(errs[GUEST], hop_in[...])
        send_back()
        grad[...] += outer(errs[2], inner[...])
        pl.loop(CHUNKS - EARLY, CHUNKS)(lambda k: give(k).wait_send())

    def give_back(q):
        span = pl.ds(q * part, part)
        return remote(ret_out.at[span], ret_in.at[span], ret_send.at[q], ret_recv.at[q], blk=partner)

    back.wait_recv()
    ret_out[...] = (grad_g[pl.ds(mine, half), :] + back_in[...].astype(jnp.float32)).astype(jnp.bfloat16)
    for q in range(PIECES):
        give_back(q).start()

    loads[6].wait()
    last = steps - 1

    @pl.loop(0, CHUNKS - 1)
    def _(k):
        cross_over(k).wait_recv()
        tile(k, last, turn_in, final)

    early = (CHUNKS - 1) * size
    grad[...] += outer(errs[last, pl.ds(0, early)], turn_in[pl.ds(0, early)])
    tail = pl.ds(early, size)
    cross_over(CHUNKS - 1).wait_recv()
    errs[last, tail, :] = error_of(CHUNKS - 1, last, turn_in[tail, :], left, codes, obs.at[natural.index(last)])

    def finish(start):
        span = pl.ds(pl.multiple_of(start, width), width)
        return grad[span, :] + outer(errs[last, tail, span], turn_in[tail, :])

    def swap(q):
        span = pl.ds(q * part, part)
        return remote(pair_out.at[span], pair_in.at[span], swap_send.at[q], swap_recv.at[q], lane=pair)

    def cross(m, q):
        span = pl.ds(q * part, part)
        return remote(peer_out.at[span], peer_in.at[m, span], cross_send.at[m, q], cross_recv.at[m, q], lane=peers[m])

    def share(q):
        span = pl.ds(pl.multiple_of(mine + q * part, part), part)
        return remote(result.at[span], result.at[span], last_send.at[q], last_recv.at[q], lane=pair)

    for start in range(0, half, width):
        pair_out[pl.ds(start, width), :] = finish(other + start).astype(jnp.bfloat16)
        for q in range(start // part, (start + width) // part):
            swap(q).start()
    for start in range(0, half, width):
        grad[pl.ds(pl.multiple_of(mine + start, width), width), :] = finish(mine + start)
    for q in range(PIECES):
        span = pl.ds(q * part, part)
        swap(q).wait_recv()
        give_back(q).wait_recv()
        peer_out[span, :] = (
            grad[pl.ds(pl.multiple_of(mine + q * part, part), part), :]
            + pair_in[span, :].astype(jnp.float32)
            + ret_in[span, :].astype(jnp.float32)
        ).astype(jnp.bfloat16)
        for m in range(len(peers)):
            cross(m, q).start()

    final[tail, :] = stepped(errs[last, tail, :], turn_in[tail, :], left)

    for u in range(SUBS):
        lend(u).wait_send()
        for m in range(others):
            lend_peer(m, u).wait_send()
        for m in range(1 + others):
            lend_pair(m, u).wait_send()
    for copy in tables:
        copy.wait_send()

    @pl.loop(0, CHUNKS)
    def _(k):
        hop(k).wait_send()
        cross_over(k).wait_send()

    back.wait_send()

    for q in range(PIECES):
        span = pl.ds(q * part, part)
        here = pl.ds(pl.multiple_of(mine + q * part, part), part)
        total = peer_out[span, :].astype(jnp.float32)
        for m in range(len(peers)):
            cross(m, q).wait_recv()
            total = total + peer_in[m, span, :].astype(jnp.float32)
        result[here, :] = (left[here, :].astype(jnp.float32) - step_left * scale * total).astype(jnp.bfloat16)
        share(q).start()
    for q in range(PIECES):
        share(q).wait_recv()
    for q in range(PIECES):
        give_back(q).wait_send()
        swap(q).wait_send()
        for m in range(len(peers)):
            cross(m, q).wait_send()
        share(q).wait_send()


def place(left_from, right_from, left_to, right_to, sem):
    moves = [
        pltpu.make_async_copy(left_from, left_to, sem.at[0]),
        pltpu.make_async_copy(right_from, right_to, sem.at[1]),
    ]
    for move in moves:
        move.start()
    for move in moves:
        move.wait()


def solution(mesh):
    blocks = mesh.shape["blk"]
    lanes = mesh.shape["lane"]

    def local(left_factor, right_factor, observed, row_codes, shift_codes):
        rows, rank = left_factor.shape
        _, steps, cols, _ = observed.shape
        bf16, f32, i32 = jnp.bfloat16, jnp.float32, jnp.int32
        dma = pltpu.SemaphoreType.DMA
        vmem = pltpu.VMEM
        hbm = pl.BlockSpec(memory_space=pltpu.HBM)
        here = pl.BlockSpec(memory_space=pltpu.VMEM)
        room = VMEM_BYTES - 2 * (rows + cols) * rank
        others = lanes // 2 - 1
        half = rows // 2
        shapes = (
            jax.ShapeDtypeStruct((rows, rank), bf16),
            jax.ShapeDtypeStruct((1, cols, rank), bf16),
        )
        results = pl.pallas_call(
            functools.partial(kernel, blocks, lanes),
            out_shape=(vmem((rows, rank), bf16), vmem((1, cols, rank), bf16)),
            in_specs=[hbm] * 5,
            out_specs=(here, here),
            scratch_shapes=[
                vmem((rows, rank), bf16),
                vmem((rows, rank), bf16),
                *[vmem((cols, rank), bf16)] * 6,
                vmem((steps - 1, cols, rows), bf16),
                vmem((cols, rows), bf16),
                vmem((1, rows), i32),
                vmem((1, rows), i32),
                vmem((1, steps, cols), i32),
                vmem((1, steps, cols), i32),
                vmem((steps, cols, WIDTH), i32),
                vmem((steps, cols, rows), bf16),
                vmem((rows, rank), f32),
                vmem((rows, rank), f32),
                *[vmem((half, rank), bf16)] * 7,
                vmem((others, half, rank), bf16),
                dma((4 + steps - 1,)),
                dma((CHUNKS,)), dma((CHUNKS,)),
                dma((2,)), dma((2,)),
                dma((SUBS,)), dma((SUBS,)),
                dma((others, SUBS)), dma((others, SUBS)),
                dma((1 + others, SUBS)), dma((1 + others, SUBS)),
                dma((CHUNKS,)), dma((CHUNKS,)),
                dma((CHUNKS,)), dma((CHUNKS,)),
                dma((1,)), dma((1,)),
                dma((PIECES,)), dma((PIECES,)),
                dma((PIECES,)), dma((PIECES,)),
                dma((others, PIECES)), dma((others, PIECES)),
                dma((PIECES,)), dma((PIECES,)),
                pltpu.SemaphoreType.REGULAR,
                pltpu.SemaphoreType.REGULAR,
            ],
            compiler_params=pltpu.CompilerParams(
                collective_id=0, has_side_effects=True, vmem_limit_bytes=room
            ),
        )(
            left_factor, right_factor, observed,
            row_codes.reshape(1, rows), shift_codes,
        )
        return pl.pallas_call(
            place,
            out_shape=shapes,
            in_specs=[here] * 2,
            out_specs=(hbm, hbm),
            scratch_shapes=[dma((2,))],
            compiler_params=pltpu.CompilerParams(vmem_limit_bytes=room),
        )(*[pltpu.with_memory_space_constraint(value, pltpu.VMEM) for value in results])

    in_specs = (
        P("blk", None),
        P("lane", "blk", None),
        P("lane", None, None, "blk"),
        P("blk"),
        P("lane", None, "blk"),
    )
    out_specs = (P("blk", None), P("lane", "blk", None))
    return jax.shard_map(local, mesh=mesh, in_specs=in_specs, out_specs=out_specs, check_vma=False)
```

```python
import functools
import math

import jax
import jax.numpy as jnp
from jax import lax
from jax.experimental import pallas as pl
from jax.experimental.pallas import tpu as pltpu
from jax.sharding import PartitionSpec as P

step_right = 0.25
step_left = 0.1

CHUNKS = 8
LAG = 5
HOLD = 1
EARLY = 2
RETURN = 5
WIDTH = 128
PIECES = 8
SUBS = 2
GUEST = 1
VMEM_BYTES = 67043328
MESH = pl.DeviceIdType.MESH


def kernel(
    blocks, lanes,
    left_hbm, right_hbm, obs_hbm, codes_hbm, shift_hbm,
    result, final_out,
    left, left_g, first, inner, hop_out, hop_in, turn_out, turn_in,
    obs, obs_g, codes, codes_g, shift, shift_g, turned, errs,
    grad, grad_g, back_out, back_in, ret_sum, ret_part, ret_out, ret_in, pair_out, pair_in, peer_out, peer_in,
    load_sem, tile_send, tile_recv, table_send, table_recv, share_send, share_recv,
    peer_share_send, peer_share_recv, pair_share_send, pair_share_recv,
    hop_send, hop_recv, turn_send, turn_recv, back_send, back_recv, fold_send, fold_recv, ret_send, ret_recv,
    swap_send, swap_recv, cross_send, cross_recv, last_send, last_recv, clear_sem, go_sem, ready_sem,
):
    steps, cols, rows = errs.shape
    final = final_out.at[0]
    rank = left.shape[1]
    scale = 1.0 / math.sqrt(rank)
    size = cols // CHUNKS
    ready = cols - EARLY * size
    half = rows // 2
    part = half // PIECES
    own = rows // lanes
    sub = own // SUBS
    width = turned.shape[2]
    others = lanes // 2 - 1
    quota = own // part
    blk = lax.axis_index("blk")
    lane = lax.axis_index("lane")
    odd = lax.rem(blk, 2)
    partner = blk + 1 - 2 * odd
    ahead = lax.rem(blk + 1, blocks)
    behind = lax.rem(blk + blocks - 1, blocks)
    ahead2 = lax.rem(blk + 2, blocks)
    behind2 = lax.rem(blk + blocks - 2, blocks)
    side = lax.rem(lane, 2)
    chip = lane // 2
    pair = lane + 1 - 2 * side
    peers = [lax.rem(lane + 2 * hop, lanes) for hop in range(1, lanes // 2)]
    sources = [lax.rem(lane + lanes - 2 * hop, lanes) for hop in range(1, lanes // 2)]
    mine = pl.multiple_of(side * half, half)
    other = pl.multiple_of((1 - side) * half, half)

    barrier = pltpu.get_barrier_semaphore()

    def greet(**place):
        pl.semaphore_signal(barrier, inc=1, device_id=place, device_id_type=MESH)

    def answer(which, **place):
        pl.semaphore_signal(ready_sem.at[which], inc=1, device_id=place, device_id_type=MESH)

    def await_answer(which):
        pl.semaphore_wait(ready_sem.at[which], 1)

    inner_blk = blk >= 2
    wraps = blk >= blocks - 2
    ends = blk == blocks - 1
    greet(lane=pair)
    pl.when(odd == 0)(lambda: greet(blk=partner))
    pl.when((odd == 1) & ~ends)(lambda: greet(blk=ahead))
    pl.when(~wraps)(lambda: greet(blk=ahead2))
    pl.when(~inner_blk)(lambda: greet(blk=behind2))
    pl.when(blk == 0)(lambda: greet(blk=behind))
    greeters = 1 + odd + ((odd == 0) & inner_blk).astype(jnp.int32) + inner_blk.astype(jnp.int32)
    greeters += wraps.astype(jnp.int32) + ends.astype(jnp.int32)
    for peer in peers:
        pl.when(peer > lane)(functools.partial(greet, lane=peer))
        greeters += (peer < lane).astype(jnp.int32)

    def remote(source, target, send, recv, **place):
        return pltpu.make_async_remote_copy(
            src_ref=source, dst_ref=target, send_sem=send, recv_sem=recv,
            device_id=place, device_id_type=MESH,
        )

    def chunk(k):
        return pl.ds(pl.multiple_of(k * size, size), size)

    natural = [s for s in range(steps) if s != GUEST]
    loads = [
        pltpu.make_async_copy(shift_hbm, shift, load_sem.at[0]),
        pltpu.make_async_copy(codes_hbm, codes, load_sem.at[1]),
        pltpu.make_async_copy(right_hbm.at[0], first, load_sem.at[2]),
        pltpu.make_async_copy(left_hbm, left, load_sem.at[3]),
    ]
    for n, s in enumerate(natural):
        loads.append(pltpu.make_async_copy(obs_hbm.at[0, s], obs.at[n], load_sem.at[4 + n]))
    for copy in loads:
        copy.start()

    def piece(owner, u):
        return pl.ds(pl.multiple_of(owner * own + u * sub, sub), sub)

    def lend(u):
        span = piece(lane, u)
        return remote(left_hbm.at[span], left_g.at[span], share_send.at[0], share_recv.at[u], blk=partner)

    def lend_peer(m, u):
        span = piece(lane, u)
        return remote(left_g.at[span], left_g.at[span], peer_share_send.at[m], peer_share_recv.at[m, u], lane=peers[m])

    def lend_pair(m, u):
        span = piece(lane if m == 0 else sources[m - 1], u)
        return remote(left_g.at[span], left_g.at[span], pair_share_send.at[m], pair_share_recv.at[m, u], lane=pair)

    def given(k):
        span = chunk(k)
        return remote(obs_hbm.at[0, GUEST, span], obs_g.at[span], tile_send.at[0], tile_recv.at[k], blk=partner)

    def give_sent(late):
        span = pl.ds(ready, cols - ready) if late else pl.ds(0, ready)
        return remote(obs_hbm.at[0, GUEST, span], obs_g.at[span], tile_send.at[late], tile_recv.at[0], blk=partner)

    def give(k):
        span = chunk(k)
        return remote(
            obs_hbm.at[0, GUEST, span], obs_g.at[span], tile_send.at[int(k >= CHUNKS - EARLY)], tile_recv.at[k], blk=partner
        )

    tables = [
        remote(codes_hbm, codes_g, table_send.at[0], table_recv.at[0], blk=partner),
        remote(shift_hbm, shift_g, table_send.at[1], table_recv.at[1], blk=partner),
    ]

    def hop(k):
        span = chunk(k)
        return remote(hop_out.at[span], hop_in.at[span], hop_send.at[0], hop_recv.at[k], blk=ahead2)

    def cross_over(k):
        span = chunk(k)
        return remote(turn_out.at[span], turn_in.at[span], turn_send.at[0], turn_recv.at[k], blk=ahead)

    def turn(s, table):
        for start in range(0, cols, width):
            span = pl.ds(start, width)
            turned[s, span, :] = jnp.transpose(jnp.broadcast_to(table[0, pl.ds(s, 1), span], (width, width)))

    def error_of(k, s, block, factor, words, target):
        span = chunk(k)
        shifts = jnp.concatenate([turned[s, span, :]] * (rows // width), axis=1)
        seen = (jnp.right_shift(words[...], shifts) & 1) == 1
        predicted = lax.dot_general(
            block, factor[...], (((1,), (1,)), ((), ())), preferred_element_type=jnp.float32
        )
        error = predicted * scale - target[span, :].astype(jnp.float32)
        return jnp.where(seen, error, 0.0).astype(jnp.bfloat16)

    def stepped(error, block, factor):
        move = jnp.dot(error, factor[...], preferred_element_type=jnp.float32)
        return (block.astype(jnp.float32) - step_right * scale * move).astype(jnp.bfloat16)

    def tile(k, s, source, target, guest=False):
        span = chunk(k)
        block = source[span, :]
        if guest:
            factor, words, wanted = left_g, codes_g, obs_g
        else:
            factor, words, wanted = left, codes, obs.at[natural.index(s)]
        error = error_of(k, s, block, factor, words, wanted)
        errs[s, span, :] = error
        target[span, :] = stepped(error, block, factor)

    last = steps - 1

    def last_visit(k):
        cross_over(k).wait_recv()
        tile(k, last, turn_in, final)

    def outer(error, block):
        return lax.dot_general(error, block, (((0,), (0,)), ((), ())), preferred_element_type=jnp.float32)

    loads[0].wait()
    turn(0, shift)
    pl.semaphore_wait(barrier, greeters)
    pl.when(odd == 1)(lambda: answer(0, blk=partner))
    pl.when((odd == 0) & inner_blk)(lambda: answer(1, blk=behind))
    pl.when(inner_blk)(lambda: answer(2, blk=behind2))
    for m, peer in enumerate(peers):
        pl.when(peer < lane)(functools.partial(answer, 3 + others - 1 - m, lane=peer))
    pl.when(odd == 0)(lambda: await_answer(0))
    for u in range(SUBS):
        lend(u).start()
    for copy in tables:
        copy.start()
    for k in range(CHUNKS):
        give(k).start()
    for copy in loads[1:5]:
        copy.wait()

    def relay():
        for m, peer in enumerate(peers):
            pl.when(peer > lane)(functools.partial(await_answer, 3 + m))
        for u in range(SUBS):
            lend(u).wait_recv()
            for m in range(others):
                lend_peer(m, u).start()
            lend_pair(0, u).start()

    def gather():
        for u in range(SUBS):
            for m in range(others):
                lend_peer(m, u).wait_recv()
                lend_pair(1 + m, u).start()
        for copy in tables:
            copy.wait_recv()
        turn(GUEST, shift_g)
        for m in range(1 + others):
            for u in range(SUBS):
                lend_pair(m, u).wait_recv()

    back = remote(back_out, back_in, back_send.at[0], back_recv.at[0], lane=pair)

    def send_back():
        back_out[...] = grad_g[pl.ds(other, half), :].astype(jnp.bfloat16)
        back.start()

    def fold(m):
        span = pl.ds(pl.multiple_of((peers[m] // 2) * own, own), own)
        return remote(ret_sum.at[span], ret_part.at[m], fold_send.at[m], fold_recv.at[m], lane=peers[m])

    def give_back(q):
        span = pl.ds(q * part, part)
        return remote(ret_out.at[span], ret_in.at[span], ret_send.at[0], ret_recv.at[q], blk=partner)

    def send_fold():
        back.wait_recv()
        ret_sum[...] = (grad_g[pl.ds(mine, half), :] + back_in[...].astype(jnp.float32)).astype(jnp.bfloat16)
        for m in range(others):
            fold(m).start()

    def send_return():
        total = ret_sum[pl.ds(pl.multiple_of(chip * own, own), own), :].astype(jnp.float32)
        for m in range(others):
            fold(m).wait_recv()
            total = total + ret_part[m].astype(jnp.float32)
        ret_out[...] = total.astype(jnp.bfloat16)
        for q in range(quota):
            give_back(q).start()

    @pl.when(odd == 0)
    def _():
        pl.loop(0, CHUNKS)(lambda k: tile(k, 0, first, inner))
        relay()
        grad[...] = outer(errs[0], first[...])
        turn(2, shift)
        turn(3, shift)
        gather()

        pl.when(~wraps)(lambda: await_answer(2))

        def guest_visit(k):
            given(k).wait_recv()
            tile(k, GUEST, inner, hop_out, guest=True)
            hop(k).start()

        def home_visit(k):
            hop(k).wait_recv()
            tile(k, 2, hop_in, turn_out)
            cross_over(k).start()

        loads[5].wait()
        loads[6].wait()
        pl.loop(0, LAG)(guest_visit)
        give_sent(0).wait_send()
        give_sent(1).wait_send()
        pl.semaphore_signal(clear_sem, inc=1, device_id={"lane": pair}, device_id_type=MESH)
        pl.semaphore_wait(clear_sem, 1)

        @pl.loop(LAG, CHUNKS)
        def _(k):
            home_visit(k - LAG)
            guest_visit(k)

        grad_g[...] = outer(errs[GUEST], inner[...])
        send_back()
        pl.loop(CHUNKS - LAG, CHUNKS - LAG + 2)(home_visit)
        send_fold()

        @pl.loop(CHUNKS - LAG + 2, CHUNKS)
        def _(k):
            home_visit(k)
            last_visit(k - (CHUNKS - LAG + 2))

        grad[...] += outer(errs[2], hop_in[...])

    @pl.when(odd == 1)
    def _():
        tile(0, 0, first, hop_out)
        pl.when(~wraps)(lambda: await_answer(2))
        hop(0).start()

        @pl.loop(1, CHUNKS)
        def _(k):
            tile(k, 0, first, hop_out)
            hop(k).start()

        relay()
        grad[...] = outer(errs[0], first[...])
        turn(2, shift)
        turn(3, shift)
        gather()
        loads[5].wait()
        loads[6].wait()

        def visits(k):
            given(k).wait_recv()
            hop(k).wait_recv()
            tile(k, GUEST, hop_in, inner, guest=True)
            tile(k, 2, inner, turn_out)

        pl.loop(0, HOLD)(visits)
        give_sent(0).wait_send()
        pl.semaphore_signal(clear_sem, inc=1, device_id={"lane": pair}, device_id_type=MESH)
        pl.semaphore_wait(clear_sem, 1)
        pl.semaphore_signal(go_sem, inc=1, device_id={"blk": behind2}, device_id_type=MESH)
        pl.semaphore_wait(go_sem, 1)
        pl.when(~ends)(lambda: await_answer(1))
        pl.loop(0, HOLD)(lambda k: cross_over(k).start())

        @pl.loop(HOLD, CHUNKS)
        def _(k):
            visits(k)
            cross_over(k).start()

        grad_g[...] = outer(errs[GUEST], hop_in[...])
        send_back()
        grad[...] += outer(errs[2], inner[...])
        give_sent(1).wait_send()
        send_fold()

    pl.loop(lax.select(odd == 0, LAG - 2, 0), RETURN)(last_visit)
    send_return()
    pl.loop(RETURN, CHUNKS - 1)(last_visit)

    early = (CHUNKS - 1) * size
    grad[...] += outer(errs[last, pl.ds(0, early)], turn_in[pl.ds(0, early)])
    tail = pl.ds(early, size)
    cross_over(CHUNKS - 1).wait_recv()
    errs[last, tail, :] = error_of(CHUNKS - 1, last, turn_in[tail, :], left, codes, obs.at[natural.index(last)])

    def finish(start):
        span = pl.ds(pl.multiple_of(start, width), width)
        return grad[span, :] + outer(errs[last, tail, span], turn_in[tail, :])

    def swap(q):
        span = pl.ds(pl.multiple_of(q * part, part), part)
        return remote(pair_out.at[span], pair_in.at[span], swap_send.at[0], swap_recv.at[q], lane=pair)

    def cross(m, n):
        span = pl.ds(pl.multiple_of(n * part, part), part)
        return remote(peer_out.at[span], peer_in.at[m, span], cross_send.at[m], cross_recv.at[m, n], lane=peers[m])

    def share(n):
        span = pl.ds(pl.multiple_of(mine + n * part, part), part)
        return remote(result.at[span], result.at[span], last_send.at[0], last_recv.at[0], lane=pair)

    for start in range(0, half, width):
        pair_out[pl.ds(start, width), :] = finish(other + start).astype(jnp.bfloat16)
        for q in range(start // part, (start + width) // part):
            swap(q).start()
    for start in range(0, half, width):
        grad[pl.ds(pl.multiple_of(mine + start, width), width), :] = finish(mine + start)
    for q in range(PIECES):
        n = lax.rem((chip + 1) * quota + q, PIECES)
        span = pl.ds(pl.multiple_of(n * part, part), part)
        swap(n).wait_recv()
        total = (
            grad[pl.ds(pl.multiple_of(mine + n * part, part), part), :]
            + pair_in[span, :].astype(jnp.float32)
        )
        if q >= PIECES - quota:
            r = q - (PIECES - quota)
            give_back(r).wait_recv()
            total = total + ret_in[pl.ds(r * part, part), :].astype(jnp.float32)
        peer_out[span, :] = total.astype(jnp.bfloat16)
        for m in range(len(peers)):
            cross(m, n).start()

    final[tail, :] = stepped(errs[last, tail, :], turn_in[tail, :], left)

    lent = pl.ds(pl.multiple_of(lane * own, own), own)
    remote(left_hbm.at[lent], left_g.at[lent], share_send.at[0], share_recv.at[0], blk=partner).wait_send()
    for m in range(others):
        remote(left_g.at[lent], left_g.at[lent], peer_share_send.at[m], peer_share_recv.at[m, 0], lane=peers[m]).wait_send()
    for m in range(1 + others):
        remote(left_g.at[lent], left_g.at[lent], pair_share_send.at[m], pair_share_recv.at[m, 0], lane=pair).wait_send()
    for copy in tables:
        copy.wait_send()
    remote(hop_out, hop_in, hop_send.at[0], hop_recv.at[0], blk=ahead2).wait_send()
    remote(turn_out, turn_in, turn_send.at[0], turn_recv.at[0], blk=ahead).wait_send()
    back.wait_send()
    for m in range(others):
        fold(m).wait_send()

    for q in range(PIECES):
        n = lax.rem(chip * quota + q, PIECES)
        span = pl.ds(pl.multiple_of(n * part, part), part)
        here = pl.ds(pl.multiple_of(mine + n * part, part), part)
        total = peer_out[span, :].astype(jnp.float32)
        for m in range(len(peers)):
            cross(m, n).wait_recv()
            total = total + peer_in[m, span, :].astype(jnp.float32)
        result[here, :] = (left[here, :].astype(jnp.float32) - step_left * scale * total).astype(jnp.bfloat16)
        share(n).start()
    shared = result.at[pl.ds(mine, half)]
    remote(shared, shared, last_send.at[0], last_recv.at[0], lane=pair).wait_recv()
    remote(ret_out, ret_in, ret_send.at[0], ret_recv.at[0], blk=partner).wait_send()
    remote(pair_out, pair_in, swap_send.at[0], swap_recv.at[0], lane=pair).wait_send()
    for m in range(len(peers)):
        remote(peer_out, peer_in.at[m], cross_send.at[m], cross_recv.at[m, 0], lane=peers[m]).wait_send()
    remote(shared, shared, last_send.at[0], last_recv.at[0], lane=pair).wait_send()


def place(left_from, right_from, left_to, right_to, sem):
    moves = [
        pltpu.make_async_copy(left_from, left_to, sem.at[0]),
        pltpu.make_async_copy(right_from, right_to, sem.at[1]),
    ]
    for move in moves:
        move.start()
    for move in moves:
        move.wait()


def solution(mesh):
    blocks = mesh.shape["blk"]
    lanes = mesh.shape["lane"]

    def local(left_factor, right_factor, observed, row_codes, shift_codes):
        rows, rank = left_factor.shape
        _, steps, cols, _ = observed.shape
        bf16, f32, i32 = jnp.bfloat16, jnp.float32, jnp.int32
        dma = pltpu.SemaphoreType.DMA
        vmem = pltpu.VMEM
        hbm = pl.BlockSpec(memory_space=pltpu.HBM)
        here = pl.BlockSpec(memory_space=pltpu.VMEM)
        room = VMEM_BYTES - 2 * (rows + cols) * rank
        others = lanes // 2 - 1
        half = rows // 2
        shapes = (
            jax.ShapeDtypeStruct((rows, rank), bf16),
            jax.ShapeDtypeStruct((1, cols, rank), bf16),
        )
        results = pl.pallas_call(
            functools.partial(kernel, blocks, lanes),
            out_shape=(vmem((rows, rank), bf16), vmem((1, cols, rank), bf16)),
            in_specs=[hbm] * 5,
            out_specs=(here, here),
            scratch_shapes=[
                vmem((rows, rank), bf16),
                vmem((rows, rank), bf16),
                *[vmem((cols, rank), bf16)] * 6,
                vmem((steps - 1, cols, rows), bf16),
                vmem((cols, rows), bf16),
                vmem((1, rows), i32),
                vmem((1, rows), i32),
                vmem((1, steps, cols), i32),
                vmem((1, steps, cols), i32),
                vmem((steps, cols, WIDTH), i32),
                vmem((steps, cols, rows), bf16),
                vmem((rows, rank), f32),
                vmem((rows, rank), f32),
                *[vmem((half, rank), bf16)] * 3,
                vmem((others, rows // lanes, rank), bf16),
                *[vmem((rows // lanes, rank), bf16)] * 2,
                *[vmem((half, rank), bf16)] * 3,
                vmem((others, half, rank), bf16),
                dma((4 + steps - 1,)),
                dma((2,)), dma((CHUNKS,)),
                dma((2,)), dma((2,)),
                dma((1,)), dma((SUBS,)),
                dma((others,)), dma((others, SUBS)),
                dma((1 + others,)), dma((1 + others, SUBS)),
                dma((1,)), dma((CHUNKS,)),
                dma((1,)), dma((CHUNKS,)),
                dma((1,)), dma((1,)),
                dma((others,)), dma((others,)),
                dma((1,)), dma((PIECES,)),
                dma((1,)), dma((PIECES,)),
                dma((others,)), dma((others, PIECES)),
                dma((1,)), dma((1,)),
                pltpu.SemaphoreType.REGULAR,
                pltpu.SemaphoreType.REGULAR,
                pltpu.SemaphoreType.REGULAR((3 + others,)),
            ],
            compiler_params=pltpu.CompilerParams(
                collective_id=0, has_side_effects=True, vmem_limit_bytes=room
            ),
        )(
            left_factor, right_factor, observed,
            row_codes.reshape(1, rows), shift_codes,
        )
        return pl.pallas_call(
            place,
            out_shape=shapes,
            in_specs=[here] * 2,
            out_specs=(hbm, hbm),
            scratch_shapes=[dma((2,))],
            compiler_params=pltpu.CompilerParams(vmem_limit_bytes=room),
        )(*[pltpu.with_memory_space_constraint(value, pltpu.VMEM) for value in results])

    in_specs = (
        P("blk", None),
        P("lane", "blk", None),
        P("lane", None, None, "blk"),
        P("blk"),
        P("lane", None, "blk"),
    )
    out_specs = (P("blk", None), P("lane", "blk", None))
    return jax.shard_map(local, mesh=mesh, in_specs=in_specs, out_specs=out_specs, check_vma=False)
```

```python
import functools
import math

import jax
import jax.numpy as jnp
from jax import lax
from jax.experimental import pallas as pl
from jax.experimental.pallas import tpu as pltpu
from jax.sharding import PartitionSpec as P

step_right = 0.25
step_left = 0.1

CHUNKS = 8
PAIRS = CHUNKS // 2
WIDTH = 128
PIECES = 8
SUBS = 2
GUEST = 1
VMEM_BYTES = 67043328
MESH = pl.DeviceIdType.MESH


def kernel(
    blocks, lanes,
    left_hbm, right_hbm, obs_hbm, codes_hbm, shift_hbm,
    result, final_out,
    left, left_g, first, inner, hop_out, hop_in, turn_out, turn_in,
    obs, obs_g, codes, codes_g, shift, shift_g, turned, errs,
    grad, grad_g, back_out, back_in, ret_sum, ret_part, ret_out, ret_in, pair_out, pair_in, peer_out, peer_in,
    load_sem, tile_send, tile_recv, table_send, table_recv, share_send, share_recv,
    peer_share_send, peer_share_recv, pair_share_send, pair_share_recv,
    hop_send, hop_recv, turn_send, turn_recv, back_send, back_recv, fold_send, fold_recv, ret_send, ret_recv,
    swap_send, swap_recv, cross_send, cross_recv, last_send, last_recv, clear_sem, go_sem, ready_sem,
):
    steps, cols, rows = errs.shape
    final = final_out.at[0]
    rank = left.shape[1]
    scale = 1.0 / math.sqrt(rank)
    size = cols // CHUNKS
    early = cols - size
    half = rows // 2
    part = half // PIECES
    own = rows // lanes
    sub = own // SUBS
    width = turned.shape[2]
    others = lanes // 2 - 1
    quota = own // part
    blk = lax.axis_index("blk")
    lane = lax.axis_index("lane")
    odd = lax.rem(blk, 2)
    partner = blk + 1 - 2 * odd
    ahead = lax.rem(blk + 1, blocks)
    behind = lax.rem(blk + blocks - 1, blocks)
    ahead2 = lax.rem(blk + 2, blocks)
    behind2 = lax.rem(blk + blocks - 2, blocks)
    side = lax.rem(lane, 2)
    chip = lane // 2
    pair = lane + 1 - 2 * side
    peers = [lax.rem(lane + 2 * hop, lanes) for hop in range(1, lanes // 2)]
    sources = [lax.rem(lane + lanes - 2 * hop, lanes) for hop in range(1, lanes // 2)]
    mine = pl.multiple_of(side * half, half)
    other = pl.multiple_of((1 - side) * half, half)

    barrier = pltpu.get_barrier_semaphore()

    def greet(**place):
        pl.semaphore_signal(barrier, inc=1, device_id=place, device_id_type=MESH)

    def answer(which, **place):
        pl.semaphore_signal(ready_sem.at[which], inc=1, device_id=place, device_id_type=MESH)

    def await_answer(which):
        pl.semaphore_wait(ready_sem.at[which], 1)

    inner_blk = blk >= 2
    wraps = blk >= blocks - 2
    ends = blk == blocks - 1
    greet(lane=pair)
    pl.when(odd == 0)(lambda: greet(blk=partner))
    pl.when((odd == 1) & ~ends)(lambda: greet(blk=ahead))
    pl.when(~wraps)(lambda: greet(blk=ahead2))
    pl.when(~inner_blk)(lambda: greet(blk=behind2))
    pl.when(blk == 0)(lambda: greet(blk=behind))
    greeters = 1 + odd + ((odd == 0) & inner_blk).astype(jnp.int32) + inner_blk.astype(jnp.int32)
    greeters += wraps.astype(jnp.int32) + ends.astype(jnp.int32)
    for peer in peers:
        pl.when(peer > lane)(functools.partial(greet, lane=peer))
        greeters += (peer < lane).astype(jnp.int32)

    def remote(source, target, send, recv, **place):
        return pltpu.make_async_remote_copy(
            src_ref=source, dst_ref=target, send_sem=send, recv_sem=recv,
            device_id=place, device_id_type=MESH,
        )

    def chunk(k, count=1):
        return pl.ds(pl.multiple_of(k * size, size), count * size)

    natural = [s for s in range(steps) if s != GUEST]
    loads = [
        pltpu.make_async_copy(shift_hbm, shift, load_sem.at[0]),
        pltpu.make_async_copy(codes_hbm, codes, load_sem.at[1]),
        pltpu.make_async_copy(right_hbm.at[0], first, load_sem.at[2]),
        pltpu.make_async_copy(left_hbm, left, load_sem.at[3]),
    ]
    for n, s in enumerate(natural):
        loads.append(pltpu.make_async_copy(obs_hbm.at[0, s], obs.at[n], load_sem.at[4 + n]))
    for copy in loads:
        copy.start()

    def piece(owner, u):
        return pl.ds(pl.multiple_of(owner * own + u * sub, sub), sub)

    def lend(u):
        span = piece(lane, u)
        return remote(left_hbm.at[span], left_g.at[span], share_send.at[0], share_recv.at[u], blk=partner)

    def lend_peer(m, u):
        span = piece(lane, u)
        return remote(left_g.at[span], left_g.at[span], peer_share_send.at[m], peer_share_recv.at[m, u], lane=peers[m])

    def lend_pair(m, u):
        span = piece(lane if m == 0 else sources[m - 1], u)
        return remote(left_g.at[span], left_g.at[span], pair_share_send.at[m], pair_share_recv.at[m, u], lane=pair)

    def give(p, group=0):
        span = chunk(2 * p, 2)
        return remote(obs_hbm.at[0, GUEST, span], obs_g.at[span], tile_send.at[group], tile_recv.at[p], blk=partner)

    def give_sent(group):
        first_col = (0, cols - 4 * size, cols - 2 * size)[group]
        span = pl.ds(first_col, cols - 4 * size if group == 0 else 2 * size)
        return remote(obs_hbm.at[0, GUEST, span], obs_g.at[span], tile_send.at[group], tile_recv.at[0], blk=partner)

    tables = [
        remote(codes_hbm, codes_g, table_send.at[0], table_recv.at[0], blk=partner),
        remote(shift_hbm, shift_g, table_send.at[1], table_recv.at[1], blk=partner),
    ]

    def hop(k):
        span = chunk(k)
        return remote(hop_out.at[span], hop_in.at[span], hop_send.at[0], hop_recv.at[k], blk=ahead2)

    def cross_over(k):
        span = chunk(k)
        return remote(turn_out.at[span], turn_in.at[span], turn_send.at[0], turn_recv.at[k], blk=ahead)

    def turn(s, table):
        for start in range(0, cols, width):
            span = pl.ds(start, width)
            turned[s, span, :] = jnp.transpose(jnp.broadcast_to(table[0, pl.ds(s, 1), span], (width, width)))

    def error_of(span, s, block, factor, words, target):
        shifts = jnp.concatenate([turned[s, span, :]] * (rows // width), axis=1)
        seen = (jnp.right_shift(words[...], shifts) & 1) == 1
        predicted = lax.dot_general(
            block, factor[...], (((1,), (1,)), ((), ())), preferred_element_type=jnp.float32
        )
        error = predicted * scale - target[span, :].astype(jnp.float32)
        return jnp.where(seen, error, 0.0).astype(jnp.bfloat16)

    def stepped(error, block, factor):
        move = jnp.dot(error, factor[...], preferred_element_type=jnp.float32)
        return (block.astype(jnp.float32) - step_right * scale * move).astype(jnp.bfloat16)

    def tile(k, s, source, target, guest=False, count=1):
        span = chunk(k, count)
        block = source[span, :]
        if guest:
            factor, words, wanted = left_g, codes_g, obs_g
        else:
            factor, words, wanted = left, codes, obs.at[natural.index(s)]
        error = error_of(span, s, block, factor, words, wanted)
        errs[s, span, :] = error
        target[span, :] = stepped(error, block, factor)

    last = steps - 1

    def last_visit(k, count=1):
        for step in range(count):
            cross_over(k + step).wait_recv()
        tile(k, last, turn_in, final, count=count)

    def last_pair(p):
        last_visit(2 * p, 2)

    def outer(error, block):
        return lax.dot_general(error, block, (((0,), (0,)), ((), ())), preferred_element_type=jnp.float32)

    def open_table():
        loads[0].wait()
        turn(0, shift)

    pl.semaphore_wait(barrier, greeters)
    pl.when(odd == 1)(lambda: answer(0, blk=partner))
    pl.when((odd == 0) & inner_blk)(lambda: answer(1, blk=behind))
    pl.when(inner_blk)(lambda: answer(2, blk=behind2))
    for m, peer in enumerate(peers):
        pl.when(peer < lane)(functools.partial(answer, 3 + others - 1 - m, lane=peer))

    @pl.when(odd == 0)
    def _():
        open_table()
        await_answer(0)

    for u in range(SUBS):
        lend(u).start()
    for copy in tables:
        copy.start()
    for p in range(PAIRS):
        give(p, max(0, p + 3 - PAIRS)).start()
    pl.when(odd == 1)(open_table)
    for copy in loads[1:5]:
        copy.wait()

    def relay():
        for m, peer in enumerate(peers):
            pl.when(peer > lane)(functools.partial(await_answer, 3 + m))
        for u in range(SUBS):
            lend(u).wait_recv()
            for m in range(others):
                lend_peer(m, u).start()
            lend_pair(0, u).start()

    def gather():
        for u in range(SUBS):
            for m in range(others):
                lend_peer(m, u).wait_recv()
                lend_pair(1 + m, u).start()
        for copy in tables:
            copy.wait_recv()
        turn(GUEST, shift_g)
        for m in range(1 + others):
            for u in range(SUBS):
                lend_pair(m, u).wait_recv()

    back = remote(back_out, back_in, back_send.at[0], back_recv.at[0], lane=pair)

    def send_back():
        back_out[...] = grad_g[pl.ds(other, half), :].astype(jnp.bfloat16)
        back.start()

    def fold(m):
        span = pl.ds(pl.multiple_of((peers[m] // 2) * own, own), own)
        return remote(ret_sum.at[span], ret_part.at[m], fold_send.at[m], fold_recv.at[m], lane=peers[m])

    def give_back(q):
        span = pl.ds(q * part, part)
        return remote(ret_out.at[span], ret_in.at[span], ret_send.at[0], ret_recv.at[q], blk=partner)

    def send_fold():
        back.wait_recv()
        ret_sum[...] = (grad_g[pl.ds(mine, half), :] + back_in[...].astype(jnp.float32)).astype(jnp.bfloat16)
        for m in range(others):
            fold(m).start()

    def send_return():
        total = ret_sum[pl.ds(pl.multiple_of(chip * own, own), own), :].astype(jnp.float32)
        for m in range(others):
            fold(m).wait_recv()
            total = total + ret_part[m].astype(jnp.float32)
        ret_out[...] = total.astype(jnp.bfloat16)
        for q in range(quota):
            give_back(q).start()

    @pl.when(odd == 0)
    def _():
        pl.loop(0, CHUNKS)(lambda k: tile(k, 0, first, inner))
        relay()
        grad[...] = outer(errs[0], first[...])
        turn(2, shift)
        turn(3, shift)
        gather()

        pl.when(~wraps)(lambda: await_answer(2))

        def guest_pair(p):
            give(p).wait_recv()
            tile(2 * p, GUEST, inner, hop_out, guest=True, count=2)
            for step in range(2):
                hop(2 * p + step).start()

        def home_visit(k):
            hop(k).wait_recv()
            tile(k, 2, hop_in, turn_out)
            cross_over(k).start()

        loads[5].wait()
        loads[6].wait()
        pl.loop(0, PAIRS - 1)(guest_pair)
        give_sent(0).wait_send()
        give_sent(1).wait_send()
        pl.semaphore_signal(clear_sem, inc=1, device_id={"lane": pair}, device_id_type=MESH)
        pl.semaphore_wait(clear_sem, 1)
        pl.loop(0, PAIRS - 1)(home_visit)
        guest_pair(PAIRS - 1)
        grad_g[...] = outer(errs[GUEST], inner[...])
        send_back()
        pl.loop(PAIRS - 1, PAIRS + 1)(home_visit)
        send_fold()

        pl.loop(PAIRS + 1, CHUNKS - 1)(home_visit)
        last_pair(0)
        before, after = pl.ds(0, early), pl.ds(early, size)
        grad[...] += outer(errs[2, before], hop_in[before])
        home_visit(CHUNKS - 1)
        last_pair(1)
        grad[...] += outer(errs[2, after], hop_in[after])
        give_sent(2).wait_send()

    @pl.when(odd == 1)
    def _():
        tile(0, 0, first, hop_out)
        pl.when(~wraps)(lambda: await_answer(2))
        hop(0).start()

        @pl.loop(1, CHUNKS)
        def _(k):
            tile(k, 0, first, hop_out)
            hop(k).start()

        relay()
        grad[...] = outer(errs[0], first[...])
        turn(2, shift)
        turn(3, shift)
        gather()
        loads[5].wait()
        loads[6].wait()

        def visit_pair(p):
            give(p).wait_recv()
            for step in range(2):
                hop(2 * p + step).wait_recv()
            tile(2 * p, GUEST, hop_in, inner, guest=True, count=2)
            tile(2 * p, 2, inner, turn_out, count=2)

        def send_pair(p):
            for step in range(2):
                cross_over(2 * p + step).start()

        def release(*groups):
            for group in groups:
                give_sent(group).wait_send()
            pl.semaphore_signal(clear_sem, inc=1, device_id={"lane": pair}, device_id_type=MESH)
            pl.semaphore_wait(clear_sem, 1)
            pl.semaphore_signal(go_sem, inc=1, device_id={"blk": behind2}, device_id_type=MESH)

        def go():
            pl.semaphore_wait(go_sem, 1)
            pl.when(~ends)(lambda: await_answer(1))
            send_pair(0)

        visit_pair(0)

        @pl.when(blk == 1)
        def _():
            release(0)
            go()
            give_sent(1).wait_send()

        @pl.when((blk > 1) & ~wraps)
        def _():
            release(0, 1)
            go()

        @pl.when((blk > 1) & wraps)
        def _():
            go()
            release(0, 1)

        @pl.loop(1, PAIRS)
        def _(p):
            visit_pair(p)
            send_pair(p)

        grad_g[...] = outer(errs[GUEST], hop_in[...])
        send_back()
        grad[...] += outer(errs[2], inner[...])
        give_sent(2).wait_send()
        send_fold()

    pl.loop(2 - 2 * odd, CHUNKS // 2 - 1)(last_pair)
    send_return()
    last_visit(CHUNKS - 2)

    grad[...] += outer(errs[last, pl.ds(0, early)], turn_in[pl.ds(0, early)])
    tail = pl.ds(early, size)
    cross_over(CHUNKS - 1).wait_recv()
    errs[last, tail, :] = error_of(tail, last, turn_in[tail, :], left, codes, obs.at[natural.index(last)])

    def finish(start):
        span = pl.ds(pl.multiple_of(start, width), width)
        return grad[span, :] + outer(errs[last, tail, span], turn_in[tail, :])

    def swap(start):
        span = pl.ds(pl.multiple_of(start, width), width)
        return remote(pair_out.at[span], pair_in.at[span], swap_send.at[0], swap_recv.at[start // width], lane=pair)

    def cross(m, n):
        span = pl.ds(pl.multiple_of(n * part, part), part)
        return remote(peer_out.at[span], peer_in.at[m, span], cross_send.at[m], cross_recv.at[m, n], lane=peers[m])

    def share(n):
        span = pl.ds(pl.multiple_of(mine + n * part, part), part)
        return remote(result.at[span], result.at[span], last_send.at[0], last_recv.at[0], lane=pair)

    starts = [lax.rem((chip + 1) * own + step, half) for step in range(0, half, width)]
    for start in starts:
        pair_out[pl.ds(pl.multiple_of(start, width), width), :] = finish(other + start).astype(jnp.bfloat16)
        swap(start).start()
    for start in starts:
        grad[pl.ds(pl.multiple_of(mine + start, width), width), :] = finish(mine + start)
    for q in range(PIECES):
        n = lax.rem((chip + 1) * quota + q, PIECES)
        span = pl.ds(pl.multiple_of(n * part, part), part)
        if q % (width // part) == 0:
            swap(n * part).wait_recv()
        total = (
            grad[pl.ds(pl.multiple_of(mine + n * part, part), part), :]
            + pair_in[span, :].astype(jnp.float32)
        )
        if q >= PIECES - quota:
            r = q - (PIECES - quota)
            give_back(r).wait_recv()
            total = total + ret_in[pl.ds(r * part, part), :].astype(jnp.float32)
        peer_out[span, :] = total.astype(jnp.bfloat16)
        for m in range(len(peers)):
            cross(m, n).start()

    final[tail, :] = stepped(errs[last, tail, :], turn_in[tail, :], left)

    lent = pl.ds(pl.multiple_of(lane * own, own), own)
    remote(left_hbm.at[lent], left_g.at[lent], share_send.at[0], share_recv.at[0], blk=partner).wait_send()
    for m in range(others):
        remote(left_g.at[lent], left_g.at[lent], peer_share_send.at[m], peer_share_recv.at[m, 0], lane=peers[m]).wait_send()
    for m in range(1 + others):
        remote(left_g.at[lent], left_g.at[lent], pair_share_send.at[m], pair_share_recv.at[m, 0], lane=pair).wait_send()
    for copy in tables:
        copy.wait_send()
    remote(hop_out, hop_in, hop_send.at[0], hop_recv.at[0], blk=ahead2).wait_send()
    remote(turn_out, turn_in, turn_send.at[0], turn_recv.at[0], blk=ahead).wait_send()
    back.wait_send()
    for m in range(others):
        fold(m).wait_send()

    for q in range(PIECES):
        n = lax.rem(chip * quota + q, PIECES)
        span = pl.ds(pl.multiple_of(n * part, part), part)
        here = pl.ds(pl.multiple_of(mine + n * part, part), part)
        total = peer_out[span, :].astype(jnp.float32)
        for m in range(len(peers)):
            cross(m, n).wait_recv()
            total = total + peer_in[m, span, :].astype(jnp.float32)
        result[here, :] = (left[here, :].astype(jnp.float32) - step_left * scale * total).astype(jnp.bfloat16)
        share(n).start()
    shared = result.at[pl.ds(mine, half)]
    remote(shared, shared, last_send.at[0], last_recv.at[0], lane=pair).wait_recv()
    remote(ret_out, ret_in, ret_send.at[0], ret_recv.at[0], blk=partner).wait_send()
    remote(pair_out, pair_in, swap_send.at[0], swap_recv.at[0], lane=pair).wait_send()
    for m in range(len(peers)):
        remote(peer_out, peer_in.at[m], cross_send.at[m], cross_recv.at[m, 0], lane=peers[m]).wait_send()
    remote(shared, shared, last_send.at[0], last_recv.at[0], lane=pair).wait_send()


def place(left_from, right_from, left_to, right_to, sem):
    moves = [
        pltpu.make_async_copy(left_from, left_to, sem.at[0]),
        pltpu.make_async_copy(right_from, right_to, sem.at[1]),
    ]
    for move in moves:
        move.start()
    for move in moves:
        move.wait()


def solution(mesh):
    blocks = mesh.shape["blk"]
    lanes = mesh.shape["lane"]

    def local(left_factor, right_factor, observed, row_codes, shift_codes):
        rows, rank = left_factor.shape
        _, steps, cols, _ = observed.shape
        bf16, f32, i32 = jnp.bfloat16, jnp.float32, jnp.int32
        dma = pltpu.SemaphoreType.DMA
        vmem = pltpu.VMEM
        hbm = pl.BlockSpec(memory_space=pltpu.HBM)
        here = pl.BlockSpec(memory_space=pltpu.VMEM)
        room = VMEM_BYTES - 2 * (rows + cols) * rank
        others = lanes // 2 - 1
        half = rows // 2
        shapes = (
            jax.ShapeDtypeStruct((rows, rank), bf16),
            jax.ShapeDtypeStruct((1, cols, rank), bf16),
        )
        results = pl.pallas_call(
            functools.partial(kernel, blocks, lanes),
            out_shape=(vmem((rows, rank), bf16), vmem((1, cols, rank), bf16)),
            in_specs=[hbm] * 5,
            out_specs=(here, here),
            scratch_shapes=[
                vmem((rows, rank), bf16),
                vmem((rows, rank), bf16),
                *[vmem((cols, rank), bf16)] * 6,
                vmem((steps - 1, cols, rows), bf16),
                vmem((cols, rows), bf16),
                vmem((1, rows), i32),
                vmem((1, rows), i32),
                vmem((1, steps, cols), i32),
                vmem((1, steps, cols), i32),
                vmem((steps, cols, WIDTH), i32),
                vmem((steps, cols, rows), bf16),
                vmem((rows, rank), f32),
                vmem((rows, rank), f32),
                *[vmem((half, rank), bf16)] * 3,
                vmem((others, rows // lanes, rank), bf16),
                *[vmem((rows // lanes, rank), bf16)] * 2,
                *[vmem((half, rank), bf16)] * 3,
                vmem((others, half, rank), bf16),
                dma((4 + steps - 1,)),
                dma((3,)), dma((PAIRS,)),
                dma((2,)), dma((2,)),
                dma((1,)), dma((SUBS,)),
                dma((others,)), dma((others, SUBS)),
                dma((1 + others,)), dma((1 + others, SUBS)),
                dma((1,)), dma((CHUNKS,)),
                dma((1,)), dma((CHUNKS,)),
                dma((1,)), dma((1,)),
                dma((others,)), dma((others,)),
                dma((1,)), dma((PIECES * 2 // lanes,)),
                dma((1,)), dma((half // WIDTH,)),
                dma((others,)), dma((others, PIECES)),
                dma((1,)), dma((1,)),
                pltpu.SemaphoreType.REGULAR,
                pltpu.SemaphoreType.REGULAR,
                pltpu.SemaphoreType.REGULAR((3 + others,)),
            ],
            compiler_params=pltpu.CompilerParams(
                collective_id=0, has_side_effects=True, vmem_limit_bytes=room
            ),
        )(
            left_factor, right_factor, observed,
            row_codes.reshape(1, rows), shift_codes,
        )
        return pl.pallas_call(
            place,
            out_shape=shapes,
            in_specs=[here] * 2,
            out_specs=(hbm, hbm),
            scratch_shapes=[dma((2,))],
            compiler_params=pltpu.CompilerParams(vmem_limit_bytes=room),
        )(*[pltpu.with_memory_space_constraint(value, pltpu.VMEM) for value in results])

    in_specs = (
        P("blk", None),
        P("lane", "blk", None),
        P("lane", None, None, "blk"),
        P("blk"),
        P("lane", None, "blk"),
    )
    out_specs = (P("blk", None), P("lane", "blk", None))
    return jax.shard_map(local, mesh=mesh, in_specs=in_specs, out_specs=out_specs, check_vma=False)
```

```python
import functools
import math

import jax
import jax.numpy as jnp
from jax import lax
from jax.experimental import pallas as pl
from jax.experimental.pallas import tpu as pltpu
from jax.sharding import PartitionSpec as P

step_right = 0.25
step_left = 0.1

CHUNKS = 8
PAIRS = CHUNKS // 2
WIDTH = 128
PIECES = 4
SUBS = 2
GUEST = 1
VMEM_BYTES = 67043328
MESH = pl.DeviceIdType.MESH


def kernel(
    blocks, lanes,
    left_hbm, right_hbm, obs_hbm, codes_hbm, shift_hbm,
    result, final_out,
    left, left_g, first, inner, hop_out, hop_in, turn_out, turn_in,
    obs, obs_g, codes, codes_g, shift, shift_g, turned, errs,
    grad, grad_g, back_out, back_in, ret_sum, ret_part, ret_out, ret_in, pair_out, pair_in, peer_out, peer_in,
    load_sem, tile_send, tile_recv, table_send, table_recv, share_send, share_recv,
    peer_share_send, peer_share_recv, pair_share_send, pair_share_recv,
    hop_send, hop_recv, turn_send, turn_recv, back_send, back_recv, fold_send, fold_recv, ret_send, ret_recv,
    swap_send, swap_recv, cross_send, cross_recv, last_send, last_recv, clear_sem, go_sem, ready_sem,
):
    steps, cols, rows = errs.shape
    final = final_out.at[0]
    rank = left.shape[1]
    scale = 1.0 / math.sqrt(rank)
    size = cols // CHUNKS
    early = cols - size
    half = rows // 2
    part = half // PIECES
    own = rows // lanes
    sub = own // SUBS
    width = turned.shape[2]
    others = lanes // 2 - 1
    quota = own // part
    blk = lax.axis_index("blk")
    lane = lax.axis_index("lane")
    odd = lax.rem(blk, 2)
    partner = blk + 1 - 2 * odd
    ahead = lax.rem(blk + 1, blocks)
    behind = lax.rem(blk + blocks - 1, blocks)
    ahead2 = lax.rem(blk + 2, blocks)
    behind2 = lax.rem(blk + blocks - 2, blocks)
    side = lax.rem(lane, 2)
    chip = lane // 2
    pair = lane + 1 - 2 * side
    peers = [lax.rem(lane + 2 * hop, lanes) for hop in range(1, lanes // 2)]
    sources = [lax.rem(lane + lanes - 2 * hop, lanes) for hop in range(1, lanes // 2)]
    mine = pl.multiple_of(side * half, half)
    other = pl.multiple_of((1 - side) * half, half)

    barrier = pltpu.get_barrier_semaphore()

    def greet(**place):
        pl.semaphore_signal(barrier, inc=1, device_id=place, device_id_type=MESH)

    def answer(which, **place):
        pl.semaphore_signal(ready_sem.at[which], inc=1, device_id=place, device_id_type=MESH)

    def await_answer(which):
        pl.semaphore_wait(ready_sem.at[which], 1)

    inner_blk = blk >= 2
    wraps = blk >= blocks - 2
    ends = blk == blocks - 1
    greet(lane=pair)
    pl.when(odd == 0)(lambda: greet(blk=partner))
    pl.when((odd == 1) & ~ends)(lambda: greet(blk=ahead))
    pl.when(~wraps)(lambda: greet(blk=ahead2))
    pl.when(~inner_blk)(lambda: greet(blk=behind2))
    pl.when(blk == 0)(lambda: greet(blk=behind))
    greeters = 1 + odd + ((odd == 0) & inner_blk).astype(jnp.int32) + inner_blk.astype(jnp.int32)
    greeters += wraps.astype(jnp.int32) + ends.astype(jnp.int32)
    for peer in peers:
        pl.when(peer > lane)(functools.partial(greet, lane=peer))
        greeters += (peer < lane).astype(jnp.int32)

    def remote(source, target, send, recv, **place):
        return pltpu.make_async_remote_copy(
            src_ref=source, dst_ref=target, send_sem=send, recv_sem=recv,
            device_id=place, device_id_type=MESH,
        )

    def chunk(k, count=1):
        return pl.ds(pl.multiple_of(k * size, size), count * size)

    natural = [s for s in range(steps) if s != GUEST]
    loads = [
        pltpu.make_async_copy(shift_hbm, shift, load_sem.at[0]),
        pltpu.make_async_copy(codes_hbm, codes, load_sem.at[1]),
        pltpu.make_async_copy(right_hbm.at[0], first, load_sem.at[2]),
        pltpu.make_async_copy(left_hbm, left, load_sem.at[3]),
    ]
    later = pl.ds(GUEST + 1, steps - 1 - GUEST)
    loads.append(pltpu.make_async_copy(obs_hbm.at[0, 0], obs.at[0], load_sem.at[4]))
    loads.append(pltpu.make_async_copy(obs_hbm.at[0, later], obs.at[pl.ds(1, steps - 2)], load_sem.at[5]))
    for copy in loads[:5]:
        copy.start()

    def piece(owner, u):
        return pl.ds(pl.multiple_of(owner * own + u * sub, sub), sub)

    def lend(u):
        span = piece(lane, u)
        return remote(left_hbm.at[span], left_g.at[span], share_send.at[0], share_recv.at[u], blk=partner)

    def lend_peer(m, u):
        span = piece(lane, u)
        return remote(left_g.at[span], left_g.at[span], peer_share_send.at[m], peer_share_recv.at[m, u], lane=peers[m])

    def lend_pair(m, u):
        span = piece(lane if m == 0 else sources[m - 1], u)
        return remote(left_g.at[span], left_g.at[span], pair_share_send.at[m], pair_share_recv.at[m, u], lane=pair)

    def give(p, group=0):
        span = chunk(2 * p, 2)
        return remote(obs_hbm.at[0, GUEST, span], obs_g.at[span], tile_send.at[group], tile_recv.at[p], blk=partner)

    def give_sent(group):
        first_col = (0, cols - 4 * size, cols - 2 * size)[group]
        span = pl.ds(first_col, cols - 4 * size if group == 0 else 2 * size)
        return remote(obs_hbm.at[0, GUEST, span], obs_g.at[span], tile_send.at[group], tile_recv.at[0], blk=partner)

    tables = [
        remote(codes_hbm, codes_g, table_send.at[0], table_recv.at[0], blk=partner),
        remote(shift_hbm, shift_g, table_send.at[1], table_recv.at[1], blk=partner),
    ]

    def hop(k):
        span = chunk(k)
        return remote(hop_out.at[span], hop_in.at[span], hop_send.at[0], hop_recv.at[k], blk=ahead2)

    def cross_over(k, count=1):
        span = chunk(k, count)
        return remote(turn_out.at[span], turn_in.at[span], turn_send.at[0], turn_recv.at[k // 2 + k // (CHUNKS - 1)], blk=ahead)

    def turn(s, table):
        for start in range(0, cols, width):
            span = pl.ds(start, width)
            turned[s, span, :] = jnp.transpose(jnp.broadcast_to(table[0, pl.ds(s, 1), span], (width, width)))

    def error_of(span, s, block, factor, words, target):
        shifts = jnp.concatenate([turned[s, span, :]] * (rows // width), axis=1)
        seen = (jnp.right_shift(words[...], shifts) & 1) == 1
        predicted = lax.dot_general(
            block, factor[...], (((1,), (1,)), ((), ())), preferred_element_type=jnp.float32
        )
        error = predicted * scale - target[span, :].astype(jnp.float32)
        return jnp.where(seen, error, 0.0).astype(jnp.bfloat16)

    def stepped(error, block, factor):
        move = jnp.dot(error, factor[...], preferred_element_type=jnp.float32)
        return (block.astype(jnp.float32) - step_right * scale * move).astype(jnp.bfloat16)

    def tile(k, s, source, target, guest=False, count=1):
        span = chunk(k, count)
        block = source[span, :]
        if guest:
            factor, words, wanted = left_g, codes_g, obs_g
        else:
            factor, words, wanted = left, codes, obs.at[natural.index(s)]
        error = error_of(span, s, block, factor, words, wanted)
        errs[s, span, :] = error
        target[span, :] = stepped(error, block, factor)

    last = steps - 1

    def last_visit(k, count=1):
        cross_over(k, count).wait_recv()
        tile(k, last, turn_in, final, count=count)

    def last_pair(p):
        last_visit(2 * p, 2)

    def outer(error, block):
        return lax.dot_general(error, block, (((0,), (0,)), ((), ())), preferred_element_type=jnp.float32)

    def open_table():
        loads[0].wait()
        turn(0, shift)

    pl.semaphore_wait(barrier, greeters)
    pl.when(odd == 1)(lambda: answer(0, blk=partner))
    pl.when((odd == 0) & inner_blk)(lambda: answer(1, blk=behind))
    pl.when(inner_blk)(lambda: answer(2, blk=behind2))
    for m, peer in enumerate(peers):
        pl.when(peer < lane)(functools.partial(answer, 3 + others - 1 - m, lane=peer))

    @pl.when(odd == 0)
    def _():
        open_table()
        await_answer(0)

    for u in range(SUBS):
        lend(u).start()
    for copy in tables:
        copy.start()
    for p in range(PAIRS):
        give(p, max(0, p + 3 - PAIRS)).start()
    pl.when(odd == 1)(open_table)
    for copy in loads[1:5]:
        copy.wait()
    for copy in loads[5:]:
        copy.start()

    def relay():
        for m, peer in enumerate(peers):
            pl.when(peer > lane)(functools.partial(await_answer, 3 + m))
        for u in range(SUBS):
            lend(u).wait_recv()
            for m in range(others):
                lend_peer(m, u).start()
            lend_pair(0, u).start()

    def gather():
        for u in range(SUBS):
            for m in range(others):
                lend_peer(m, u).wait_recv()
                lend_pair(1 + m, u).start()
        for copy in tables:
            copy.wait_recv()
        turn(GUEST, shift_g)
        for m in range(1 + others):
            for u in range(SUBS):
                lend_pair(m, u).wait_recv()

    back = remote(back_out, back_in, back_send.at[0], back_recv.at[0], lane=pair)

    def send_back():
        back_out[...] = grad_g[pl.ds(other, half), :].astype(jnp.bfloat16)
        back.start()

    def fold(m):
        span = pl.ds(pl.multiple_of((peers[m] // 2) * own, own), own)
        return remote(ret_sum.at[span], ret_part.at[m], fold_send.at[m], fold_recv.at[m], lane=peers[m])

    def give_back(q):
        span = pl.ds(q * part, part)
        return remote(ret_out.at[span], ret_in.at[span], ret_send.at[0], ret_recv.at[q], blk=partner)

    def send_fold():
        back.wait_recv()
        ret_sum[...] = (grad_g[pl.ds(mine, half), :] + back_in[...].astype(jnp.float32)).astype(jnp.bfloat16)
        for m in range(others):
            fold(m).start()

    def send_return():
        total = ret_sum[pl.ds(pl.multiple_of(chip * own, own), own), :].astype(jnp.float32)
        for m in range(others):
            fold(m).wait_recv()
            total = total + ret_part[m].astype(jnp.float32)
        ret_out[...] = total.astype(jnp.bfloat16)
        for q in range(quota):
            give_back(q).start()

    @pl.when(odd == 0)
    def _():
        pl.loop(0, PAIRS)(lambda p: tile(2 * p, 0, first, inner, count=2))
        relay()
        grad[...] = outer(errs[0], first[...])
        turn(2, shift)
        turn(3, shift)
        gather()

        pl.when(~wraps)(lambda: await_answer(2))

        def guest_pair(p):
            give(p).wait_recv()
            tile(2 * p, GUEST, inner, hop_out, guest=True, count=2)
            for step in range(2):
                hop(2 * p + step).start()

        def home_visit(k):
            hop(k).wait_recv()
            tile(k, 2, hop_in, turn_out)
            cross_over(k).start()

        loads[5].wait()
        pl.loop(0, PAIRS - 1)(guest_pair)
        give_sent(0).wait_send()
        give_sent(1).wait_send()
        pl.semaphore_signal(clear_sem, inc=1, device_id={"lane": pair}, device_id_type=MESH)
        pl.semaphore_wait(clear_sem, 1)
        pl.loop(0, PAIRS - 1)(home_visit)
        guest_pair(PAIRS - 1)
        grad_g[...] = outer(errs[GUEST], inner[...])
        send_back()
        pl.loop(PAIRS - 1, PAIRS + 1)(home_visit)
        send_fold()

        pl.loop(PAIRS + 1, CHUNKS - 2)(home_visit)
        last_pair(0)
        home_visit(CHUNKS - 2)
        last_pair(1)
        home_visit(CHUNKS - 1)
        grad[...] += outer(errs[2], hop_in[...])
        give_sent(2).wait_send()

    @pl.when(odd == 1)
    def _():
        def start_pair(p):
            tile(2 * p, 0, first, hop_out, count=2)

        def hop_pair(p):
            for step in range(2):
                hop(2 * p + step).start()

        start_pair(0)
        pl.when(~wraps)(lambda: await_answer(2))
        hop_pair(0)

        @pl.loop(1, PAIRS)
        def _(p):
            start_pair(p)
            hop_pair(p)

        relay()
        grad[...] = outer(errs[0], first[...])
        turn(2, shift)
        turn(3, shift)
        gather()
        loads[5].wait()

        def visit_pair(p):
            give(p).wait_recv()
            for step in range(2):
                hop(2 * p + step).wait_recv()
            tile(2 * p, GUEST, hop_in, inner, guest=True, count=2)
            tile(2 * p, 2, inner, turn_out, count=2)

        def send_pair(p):
            for step in range(2):
                cross_over(2 * p + step).start()

        def release(*groups):
            for group in groups:
                give_sent(group).wait_send()
            pl.semaphore_signal(clear_sem, inc=1, device_id={"lane": pair}, device_id_type=MESH)
            pl.semaphore_wait(clear_sem, 1)
            pl.semaphore_signal(go_sem, inc=1, device_id={"blk": behind2}, device_id_type=MESH)

        def go():
            pl.semaphore_wait(go_sem, 1)
            pl.when(~ends)(lambda: await_answer(1))
            send_pair(0)

        visit_pair(0)

        @pl.when(blk == 1)
        def _():
            release(0)
            go()
            give_sent(1).wait_send()

        @pl.when((blk > 1) & ~wraps)
        def _():
            release(0, 1)
            go()

        @pl.when((blk > 1) & wraps)
        def _():
            go()
            release(0, 1)

        @pl.loop(1, PAIRS)
        def _(p):
            visit_pair(p)
            send_pair(p)

        grad_g[...] = outer(errs[GUEST], hop_in[...])
        send_back()
        grad[...] += outer(errs[2], inner[...])
        give_sent(2).wait_send()
        send_fold()

    pl.loop(2 - 2 * odd, CHUNKS // 2 - 1)(last_pair)
    send_return()
    grad[...] += outer(errs[last, pl.ds(0, cols - 4 * size)], turn_in[pl.ds(0, cols - 4 * size)])
    last_visit(CHUNKS - 2)

    rest = pl.ds(cols - 4 * size, 3 * size)
    grad[...] += outer(errs[last, rest], turn_in[rest])
    tail = pl.ds(early, size)
    cross_over(CHUNKS - 1).wait_recv()
    errs[last, tail, :] = error_of(tail, last, turn_in[tail, :], left, codes, obs.at[natural.index(last)])

    def finish(start):
        span = pl.ds(pl.multiple_of(start, width), width)
        return grad[span, :] + outer(errs[last, tail, span], turn_in[tail, :])

    def swap(start):
        span = pl.ds(pl.multiple_of(start, width), width)
        return remote(pair_out.at[span], pair_in.at[span], swap_send.at[0], swap_recv.at[start // width], lane=pair)

    def cross(m, n):
        span = pl.ds(pl.multiple_of(n * part, part), part)
        return remote(peer_out.at[span], peer_in.at[m, span], cross_send.at[m], cross_recv.at[m, n], lane=peers[m])

    def share(n):
        span = pl.ds(pl.multiple_of(mine + n * part, part), part)
        return remote(result.at[span], result.at[span], last_send.at[0], last_recv.at[0], lane=pair)

    starts = [lax.rem((chip + 1) * own + step, half) for step in range(0, half, width)]
    for start in starts:
        pair_out[pl.ds(pl.multiple_of(start, width), width), :] = finish(other + start).astype(jnp.bfloat16)
        swap(start).start()
    for start in starts:
        grad[pl.ds(pl.multiple_of(mine + start, width), width), :] = finish(mine + start)
    for q in range(PIECES):
        n = lax.rem((chip + 1) * quota + q, PIECES)
        span = pl.ds(pl.multiple_of(n * part, part), part)
        if q % (width // part) == 0:
            swap(n * part).wait_recv()
        total = (
            grad[pl.ds(pl.multiple_of(mine + n * part, part), part), :]
            + pair_in[span, :].astype(jnp.float32)
        )
        if q >= PIECES - quota:
            r = q - (PIECES - quota)
            give_back(r).wait_recv()
            total = total + ret_in[pl.ds(r * part, part), :].astype(jnp.float32)
        peer_out[span, :] = total.astype(jnp.bfloat16)
        for m in range(len(peers)):
            cross(m, n).start()

    final[tail, :] = stepped(errs[last, tail, :], turn_in[tail, :], left)

    lent = pl.ds(pl.multiple_of(lane * own, own), own)
    remote(left_hbm.at[lent], left_g.at[lent], share_send.at[0], share_recv.at[0], blk=partner).wait_send()
    for m in range(others):
        remote(left_g.at[lent], left_g.at[lent], peer_share_send.at[m], peer_share_recv.at[m, 0], lane=peers[m]).wait_send()
    for m in range(1 + others):
        remote(left_g.at[lent], left_g.at[lent], pair_share_send.at[m], pair_share_recv.at[m, 0], lane=pair).wait_send()
    for copy in tables:
        copy.wait_send()
    remote(hop_out, hop_in, hop_send.at[0], hop_recv.at[0], blk=ahead2).wait_send()
    remote(turn_out, turn_in, turn_send.at[0], turn_recv.at[0], blk=ahead).wait_send()
    back.wait_send()
    for m in range(others):
        fold(m).wait_send()

    for q in range(PIECES):
        n = lax.rem(chip * quota + q, PIECES)
        span = pl.ds(pl.multiple_of(n * part, part), part)
        here = pl.ds(pl.multiple_of(mine + n * part, part), part)
        total = peer_out[span, :].astype(jnp.float32)
        for m in range(len(peers)):
            cross(m, n).wait_recv()
            total = total + peer_in[m, span, :].astype(jnp.float32)
        result[here, :] = (left[here, :].astype(jnp.float32) - step_left * scale * total).astype(jnp.bfloat16)
        share(n).start()
    shared = result.at[pl.ds(mine, half)]
    remote(shared, shared, last_send.at[0], last_recv.at[0], lane=pair).wait_recv()
    remote(ret_out, ret_in, ret_send.at[0], ret_recv.at[0], blk=partner).wait_send()
    remote(pair_out, pair_in, swap_send.at[0], swap_recv.at[0], lane=pair).wait_send()
    for m in range(len(peers)):
        remote(peer_out, peer_in.at[m], cross_send.at[m], cross_recv.at[m, 0], lane=peers[m]).wait_send()
    remote(shared, shared, last_send.at[0], last_recv.at[0], lane=pair).wait_send()


def place(left_from, right_from, left_to, right_to, sem):
    moves = [
        pltpu.make_async_copy(left_from, left_to, sem.at[0]),
        pltpu.make_async_copy(right_from, right_to, sem.at[1]),
    ]
    for move in moves:
        move.start()
    for move in moves:
        move.wait()


def solution(mesh):
    blocks = mesh.shape["blk"]
    lanes = mesh.shape["lane"]

    def local(left_factor, right_factor, observed, row_codes, shift_codes):
        rows, rank = left_factor.shape
        _, steps, cols, _ = observed.shape
        bf16, f32, i32 = jnp.bfloat16, jnp.float32, jnp.int32
        dma = pltpu.SemaphoreType.DMA
        vmem = pltpu.VMEM
        hbm = pl.BlockSpec(memory_space=pltpu.HBM)
        here = pl.BlockSpec(memory_space=pltpu.VMEM)
        room = VMEM_BYTES - 2 * (rows + cols) * rank
        others = lanes // 2 - 1
        half = rows // 2
        shapes = (
            jax.ShapeDtypeStruct((rows, rank), bf16),
            jax.ShapeDtypeStruct((1, cols, rank), bf16),
        )
        results = pl.pallas_call(
            functools.partial(kernel, blocks, lanes),
            out_shape=(vmem((rows, rank), bf16), vmem((1, cols, rank), bf16)),
            in_specs=[hbm] * 5,
            out_specs=(here, here),
            scratch_shapes=[
                vmem((rows, rank), bf16),
                vmem((rows, rank), bf16),
                *[vmem((cols, rank), bf16)] * 6,
                vmem((steps - 1, cols, rows), bf16),
                vmem((cols, rows), bf16),
                vmem((1, rows), i32),
                vmem((1, rows), i32),
                vmem((1, steps, cols), i32),
                vmem((1, steps, cols), i32),
                vmem((steps, cols, WIDTH), i32),
                vmem((steps, cols, rows), bf16),
                vmem((rows, rank), f32),
                vmem((rows, rank), f32),
                *[vmem((half, rank), bf16)] * 3,
                vmem((others, rows // lanes, rank), bf16),
                *[vmem((rows // lanes, rank), bf16)] * 2,
                *[vmem((half, rank), bf16)] * 3,
                vmem((others, half, rank), bf16),
                dma((6,)),
                dma((3,)), dma((PAIRS,)),
                dma((2,)), dma((2,)),
                dma((1,)), dma((SUBS,)),
                dma((others,)), dma((others, SUBS)),
                dma((1 + others,)), dma((1 + others, SUBS)),
                dma((1,)), dma((CHUNKS,)),
                dma((1,)), dma((PAIRS + 1,)),
                dma((1,)), dma((1,)),
                dma((others,)), dma((others,)),
                dma((1,)), dma((PIECES * 2 // lanes,)),
                dma((1,)), dma((half // WIDTH,)),
                dma((others,)), dma((others, PIECES)),
                dma((1,)), dma((1,)),
                pltpu.SemaphoreType.REGULAR,
                pltpu.SemaphoreType.REGULAR,
                pltpu.SemaphoreType.REGULAR((3 + others,)),
            ],
            compiler_params=pltpu.CompilerParams(
                collective_id=0, has_side_effects=True, vmem_limit_bytes=room
            ),
        )(
            left_factor, right_factor, observed,
            row_codes.reshape(1, rows), shift_codes,
        )
        return pl.pallas_call(
            place,
            out_shape=shapes,
            in_specs=[here] * 2,
            out_specs=(hbm, hbm),
            scratch_shapes=[dma((2,))],
            compiler_params=pltpu.CompilerParams(vmem_limit_bytes=room),
        )(*[pltpu.with_memory_space_constraint(value, pltpu.VMEM) for value in results])

    in_specs = (
        P("blk", None),
        P("lane", "blk", None),
        P("lane", None, None, "blk"),
        P("blk"),
        P("lane", None, "blk"),
    )
    out_specs = (P("blk", None), P("lane", "blk", None))
    return jax.shard_map(local, mesh=mesh, in_specs=in_specs, out_specs=out_specs, check_vma=False)
```

```python
import functools
import math

import jax
import jax.numpy as jnp
from jax import lax
from jax.experimental import pallas as pl
from jax.experimental.pallas import tpu as pltpu
from jax.sharding import PartitionSpec as P

step_right = 0.25
step_left = 0.1

CHUNKS = 8
PAIRS = CHUNKS // 2
WIDTH = 128
PIECES = 4
SUBS = 2
GUEST = 1
VMEM_BYTES = 67043328
MESH = pl.DeviceIdType.MESH


def kernel(
    blocks, lanes,
    left_hbm, right_hbm, obs_hbm, codes_hbm, shift_hbm,
    result, final_out,
    left, left_g, first, inner, hop_out, hop_in, turn_out, turn_in,
    obs, obs_g, codes, codes_g, shift, shift_g, turned, errs,
    grad, grad_g, back_out, back_in, ret_sum, ret_part, ret_out, ret_in, pair_out, pair_in, peer_out, peer_in,
    load_sem, tile_send, tile_recv, table_send, table_recv, share_send, share_recv,
    peer_share_send, peer_share_recv, pair_share_send, pair_share_recv,
    hop_send, hop_recv, turn_send, turn_recv, back_send, back_recv, fold_send, fold_recv, ret_send, ret_recv,
    swap_send, swap_recv, cross_send, cross_recv, last_send, last_recv, clear_sem, go_sem, ready_sem,
):
    steps, cols, rows = errs.shape
    final = final_out.at[0]
    rank = left.shape[1]
    scale = 1.0 / math.sqrt(rank)
    size = cols // CHUNKS
    early = cols - size
    half = rows // 2
    part = half // PIECES
    own = rows // lanes
    sub = own // SUBS
    width = turned.shape[2]
    others = lanes // 2 - 1
    quota = own // part
    blk = lax.axis_index("blk")
    lane = lax.axis_index("lane")
    odd = lax.rem(blk, 2)
    partner = blk + 1 - 2 * odd
    ahead = lax.rem(blk + 1, blocks)
    behind = lax.rem(blk + blocks - 1, blocks)
    ahead2 = lax.rem(blk + 2, blocks)
    behind2 = lax.rem(blk + blocks - 2, blocks)
    side = lax.rem(lane, 2)
    chip = lane // 2
    pair = lane + 1 - 2 * side
    peers = [lax.rem(lane + 2 * hop, lanes) for hop in range(1, lanes // 2)]
    sources = [lax.rem(lane + lanes - 2 * hop, lanes) for hop in range(1, lanes // 2)]
    mine = pl.multiple_of(side * half, half)
    other = pl.multiple_of((1 - side) * half, half)

    barrier = pltpu.get_barrier_semaphore()

    def greet(**place):
        pl.semaphore_signal(barrier, inc=1, device_id=place, device_id_type=MESH)

    def answer(which, **place):
        pl.semaphore_signal(ready_sem.at[which], inc=1, device_id=place, device_id_type=MESH)

    def await_answer(which):
        pl.semaphore_wait(ready_sem.at[which], 1)

    inner_blk = blk >= 2
    wraps = blk >= blocks - 2
    ends = blk == blocks - 1
    greet(lane=pair)
    pl.when(odd == 0)(lambda: greet(blk=partner))
    pl.when((odd == 1) & ~ends)(lambda: greet(blk=ahead))
    pl.when(~wraps)(lambda: greet(blk=ahead2))
    pl.when(~inner_blk)(lambda: greet(blk=behind2))
    pl.when(blk == 0)(lambda: greet(blk=behind))
    greeters = 1 + odd + ((odd == 0) & inner_blk).astype(jnp.int32) + inner_blk.astype(jnp.int32)
    greeters += wraps.astype(jnp.int32) + ends.astype(jnp.int32)
    for peer in peers:
        pl.when(peer > lane)(functools.partial(greet, lane=peer))
        greeters += (peer < lane).astype(jnp.int32)

    def remote(source, target, send, recv, **place):
        return pltpu.make_async_remote_copy(
            src_ref=source, dst_ref=target, send_sem=send, recv_sem=recv,
            device_id=place, device_id_type=MESH,
        )

    def chunk(k, count=1):
        return pl.ds(pl.multiple_of(k * size, size), count * size)

    natural = [s for s in range(steps) if s != GUEST]
    loads = [
        pltpu.make_async_copy(shift_hbm, shift, load_sem.at[0]),
        pltpu.make_async_copy(codes_hbm, codes, load_sem.at[1]),
        pltpu.make_async_copy(right_hbm.at[0], first, load_sem.at[2]),
        pltpu.make_async_copy(left_hbm, left, load_sem.at[3]),
    ]
    later = pl.ds(GUEST + 1, steps - 1 - GUEST)
    loads.append(pltpu.make_async_copy(obs_hbm.at[0, 0], obs.at[0], load_sem.at[4]))
    loads.append(pltpu.make_async_copy(obs_hbm.at[0, later], obs.at[pl.ds(1, steps - 2)], load_sem.at[5]))
    for copy in loads[:5]:
        copy.start()

    def piece(owner, u):
        return pl.ds(pl.multiple_of(owner * own + u * sub, sub), sub)

    def lend(u):
        span = piece(lane, u)
        return remote(left_hbm.at[span], left_g.at[span], share_send.at[0], share_recv.at[u], blk=partner)

    def lend_peer(m, u):
        span = piece(lane, u)
        return remote(left_g.at[span], left_g.at[span], peer_share_send.at[m], peer_share_recv.at[m, u], lane=peers[m])

    def lend_pair(m, u):
        span = piece(lane if m == 0 else sources[m - 1], u)
        return remote(left_g.at[span], left_g.at[span], pair_share_send.at[m], pair_share_recv.at[m, u], lane=pair)

    def give(p, group=0):
        span = chunk(2 * p, 2)
        return remote(obs_hbm.at[0, GUEST, span], obs_g.at[span], tile_send.at[group], tile_recv.at[p], blk=partner)

    def give_sent(group):
        first_col = (0, cols - 4 * size, cols - 2 * size)[group]
        span = pl.ds(first_col, cols - 4 * size if group == 0 else 2 * size)
        return remote(obs_hbm.at[0, GUEST, span], obs_g.at[span], tile_send.at[group], tile_recv.at[0], blk=partner)

    tables = [
        remote(codes_hbm, codes_g, table_send.at[0], table_recv.at[0], blk=partner),
        remote(shift_hbm, shift_g, table_send.at[1], table_recv.at[1], blk=partner),
    ]

    def hop(k):
        span = chunk(k)
        return remote(hop_out.at[span], hop_in.at[span], hop_send.at[0], hop_recv.at[k], blk=ahead2)

    def cross_over(k, count=1):
        span = chunk(k, count)
        return remote(turn_out.at[span], turn_in.at[span], turn_send.at[0], turn_recv.at[k // 2 + k // (CHUNKS - 1)], blk=ahead)

    def turn(s, table):
        for start in range(0, cols, width):
            span = pl.ds(start, width)
            turned[s, span, :] = jnp.transpose(jnp.broadcast_to(table[0, pl.ds(s, 1), span], (width, width)))

    def error_of(span, s, block, factor, words, target):
        shifts = jnp.concatenate([turned[s, span, :]] * (rows // width), axis=1)
        seen = (jnp.right_shift(words[...], shifts) & 1) == 1
        predicted = lax.dot_general(
            block, factor[...], (((1,), (1,)), ((), ())), preferred_element_type=jnp.float32
        )
        error = predicted * scale - target[span, :].astype(jnp.float32)
        return jnp.where(seen, error, 0.0).astype(jnp.bfloat16)

    def stepped(error, block, factor):
        move = jnp.dot(error, factor[...], preferred_element_type=jnp.float32)
        return (block.astype(jnp.float32) - step_right * scale * move).astype(jnp.bfloat16)

    def tile(k, s, source, target, guest=False, count=1):
        span = chunk(k, count)
        block = source[span, :]
        if guest:
            factor, words, wanted = left_g, codes_g, obs_g
        else:
            factor, words, wanted = left, codes, obs.at[natural.index(s)]
        error = error_of(span, s, block, factor, words, wanted)
        errs[s, span, :] = error
        target[span, :] = stepped(error, block, factor)

    last = steps - 1

    def last_visit(k, count=1):
        cross_over(k, count).wait_recv()
        tile(k, last, turn_in, final, count=count)

    def last_pair(p):
        last_visit(2 * p, 2)

    def outer(error, block):
        return lax.dot_general(error, block, (((0,), (0,)), ((), ())), preferred_element_type=jnp.float32)

    def open_table():
        loads[0].wait()
        turn(0, shift)

    pl.semaphore_wait(barrier, greeters)
    pl.when(odd == 1)(lambda: answer(0, blk=partner))
    pl.when((odd == 0) & inner_blk)(lambda: answer(1, blk=behind))
    pl.when(inner_blk)(lambda: answer(2, blk=behind2))
    for m, peer in enumerate(peers):
        pl.when(peer < lane)(functools.partial(answer, 3 + others - 1 - m, lane=peer))

    @pl.when(odd == 0)
    def _():
        open_table()
        await_answer(0)

    for u in range(SUBS):
        lend(u).start()
    for copy in tables:
        copy.start()
    for p in range(PAIRS):
        give(p, max(0, p + 3 - PAIRS)).start()
    pl.when(odd == 1)(open_table)
    for copy in loads[1:5]:
        copy.wait()
    for copy in loads[5:]:
        copy.start()

    def relay():
        for m, peer in enumerate(peers):
            pl.when(peer > lane)(functools.partial(await_answer, 3 + m))
        for u in range(SUBS):
            lend(u).wait_recv()
            for m in range(others):
                lend_peer(m, u).start()
            lend_pair(0, u).start()

    def gather():
        for u in range(SUBS):
            for m in range(others):
                lend_peer(m, u).wait_recv()
                lend_pair(1 + m, u).start()
        for copy in tables:
            copy.wait_recv()
        turn(GUEST, shift_g)
        for m in range(1 + others):
            for u in range(SUBS):
                lend_pair(m, u).wait_recv()

    back = remote(back_out, back_in, back_send.at[0], back_recv.at[0], lane=pair)

    def send_back():
        back_out[...] = grad_g[pl.ds(other, half), :].astype(jnp.bfloat16)
        back.start()

    def fold(m):
        span = pl.ds(pl.multiple_of((peers[m] // 2) * own, own), own)
        return remote(ret_sum.at[span], ret_part.at[m], fold_send.at[m], fold_recv.at[m], lane=peers[m])

    def give_back(q):
        span = pl.ds(q * part, part)
        return remote(ret_out.at[span], ret_in.at[span], ret_send.at[0], ret_recv.at[q], blk=partner)

    def send_fold():
        back.wait_recv()
        ret_sum[...] = (grad_g[pl.ds(mine, half), :] + back_in[...].astype(jnp.float32)).astype(jnp.bfloat16)
        for m in range(others):
            fold(m).start()

    def send_return():
        total = ret_sum[pl.ds(pl.multiple_of(chip * own, own), own), :].astype(jnp.float32)
        for m in range(others):
            fold(m).wait_recv()
            total = total + ret_part[m].astype(jnp.float32)
        ret_out[...] = total.astype(jnp.bfloat16)
        for q in range(quota):
            give_back(q).start()

    @pl.when(odd == 0)
    def _():
        pl.loop(0, PAIRS)(lambda p: tile(2 * p, 0, first, inner, count=2))
        relay()
        grad[...] = outer(errs[0], first[...])
        turn(2, shift)
        turn(3, shift)
        gather()

        pl.when(~wraps)(lambda: await_answer(2))

        def guest_pair(p):
            give(p).wait_recv()
            tile(2 * p, GUEST, inner, hop_out, guest=True, count=2)
            for step in range(2):
                hop(2 * p + step).start()

        def home_visit(k):
            hop(k).wait_recv()
            tile(k, 2, hop_in, turn_out)
            cross_over(k).start()

        loads[5].wait()
        pl.loop(0, PAIRS - 1)(guest_pair)
        give_sent(0).wait_send()
        pl.semaphore_signal(clear_sem, inc=1, device_id={"lane": pair}, device_id_type=MESH)
        pl.semaphore_wait(clear_sem, 1)
        pl.loop(0, PAIRS - 1)(home_visit)
        guest_pair(PAIRS - 1)
        grad_g[...] = outer(errs[GUEST], inner[...])
        send_back()
        pl.loop(PAIRS - 1, PAIRS + 1)(home_visit)
        send_fold()

        pl.loop(PAIRS + 1, CHUNKS - 2)(home_visit)
        last_pair(0)
        home_visit(CHUNKS - 2)
        last_pair(1)
        home_visit(CHUNKS - 1)
        grad[...] += outer(errs[2], hop_in[...])
        give_sent(1).wait_send()
        give_sent(2).wait_send()

    @pl.when(odd == 1)
    def _():
        def start_pair(p):
            tile(2 * p, 0, first, hop_out, count=2)

        def hop_pair(p):
            for step in range(2):
                hop(2 * p + step).start()

        start_pair(0)
        pl.when(~wraps)(lambda: await_answer(2))
        hop_pair(0)

        @pl.loop(1, PAIRS)
        def _(p):
            start_pair(p)
            hop_pair(p)

        relay()
        grad[...] = outer(errs[0], first[...])
        turn(2, shift)
        turn(3, shift)
        gather()
        loads[5].wait()

        def visit_pair(p):
            give(p).wait_recv()
            for step in range(2):
                hop(2 * p + step).wait_recv()
            tile(2 * p, GUEST, hop_in, inner, guest=True, count=2)
            tile(2 * p, 2, inner, turn_out, count=2)

        def send_pair(p):
            for step in range(2):
                cross_over(2 * p + step).start()

        def release(*groups):
            for group in groups:
                give_sent(group).wait_send()
            pl.semaphore_signal(clear_sem, inc=1, device_id={"lane": pair}, device_id_type=MESH)
            pl.semaphore_wait(clear_sem, 1)
            pl.semaphore_signal(go_sem, inc=1, device_id={"blk": behind2}, device_id_type=MESH)

        def go():
            pl.semaphore_wait(go_sem, 1)
            pl.when(~ends)(lambda: await_answer(1))
            send_pair(0)

        visit_pair(0)

        @pl.when(blk == 1)
        def _():
            release(0)
            go()
            give_sent(1).wait_send()

        @pl.when((blk > 1) & ~wraps)
        def _():
            release(0, 1)
            go()

        @pl.when((blk > 1) & wraps)
        def _():
            go()
            release(0, 1)

        @pl.loop(1, PAIRS)
        def _(p):
            visit_pair(p)
            send_pair(p)

        grad_g[...] = outer(errs[GUEST], hop_in[...])
        send_back()
        grad[...] += outer(errs[2], inner[...])
        give_sent(2).wait_send()
        send_fold()

    pl.loop(2 - 2 * odd, CHUNKS // 2 - 1)(last_pair)
    send_return()
    grad[...] += outer(errs[last, pl.ds(0, cols - 4 * size)], turn_in[pl.ds(0, cols - 4 * size)])
    last_visit(CHUNKS - 2)

    rest = pl.ds(cols - 4 * size, 3 * size)
    grad[...] += outer(errs[last, rest], turn_in[rest])
    tail = pl.ds(early, size)
    cross_over(CHUNKS - 1).wait_recv()
    errs[last, tail, :] = error_of(tail, last, turn_in[tail, :], left, codes, obs.at[natural.index(last)])

    def finish(start):
        span = pl.ds(pl.multiple_of(start, width), width)
        return grad[span, :] + outer(errs[last, tail, span], turn_in[tail, :])

    def swap(start):
        span = pl.ds(pl.multiple_of(start, width), width)
        return remote(pair_out.at[span], pair_in.at[span], swap_send.at[0], swap_recv.at[start // width], lane=pair)

    def cross(m, n):
        span = pl.ds(pl.multiple_of(n * part, part), part)
        return remote(peer_out.at[span], peer_in.at[m, span], cross_send.at[m], cross_recv.at[m, n], lane=peers[m])

    def share(n):
        span = pl.ds(pl.multiple_of(mine + n * part, part), part)
        return remote(result.at[span], result.at[span], last_send.at[0], last_recv.at[0], lane=pair)

    starts = [lax.rem((chip + 1) * own + step, half) for step in range(0, half, width)]
    for start in starts:
        pair_out[pl.ds(pl.multiple_of(start, width), width), :] = finish(other + start).astype(jnp.bfloat16)
        swap(start).start()
    for start in starts:
        grad[pl.ds(pl.multiple_of(mine + start, width), width), :] = finish(mine + start)
    for q in range(PIECES):
        n = lax.rem((chip + 1) * quota + q, PIECES)
        span = pl.ds(pl.multiple_of(n * part, part), part)
        if q % (width // part) == 0:
            swap(n * part).wait_recv()
        total = (
            grad[pl.ds(pl.multiple_of(mine + n * part, part), part), :]
            + pair_in[span, :].astype(jnp.float32)
        )
        if q >= PIECES - quota:
            r = q - (PIECES - quota)
            give_back(r).wait_recv()
            total = total + ret_in[pl.ds(r * part, part), :].astype(jnp.float32)
        peer_out[span, :] = total.astype(jnp.bfloat16)
        for m in range(len(peers)):
            cross(m, n).start()

    final[tail, :] = stepped(errs[last, tail, :], turn_in[tail, :], left)

    lent = pl.ds(pl.multiple_of(lane * own, own), own)
    remote(left_hbm.at[lent], left_g.at[lent], share_send.at[0], share_recv.at[0], blk=partner).wait_send()
    for m in range(others):
        remote(left_g.at[lent], left_g.at[lent], peer_share_send.at[m], peer_share_recv.at[m, 0], lane=peers[m]).wait_send()
    for m in range(1 + others):
        remote(left_g.at[lent], left_g.at[lent], pair_share_send.at[m], pair_share_recv.at[m, 0], lane=pair).wait_send()
    for copy in tables:
        copy.wait_send()
    remote(hop_out, hop_in, hop_send.at[0], hop_recv.at[0], blk=ahead2).wait_send()
    remote(turn_out, turn_in, turn_send.at[0], turn_recv.at[0], blk=ahead).wait_send()
    back.wait_send()
    for m in range(others):
        fold(m).wait_send()

    for q in range(PIECES):
        n = lax.rem(chip * quota + q, PIECES)
        span = pl.ds(pl.multiple_of(n * part, part), part)
        here = pl.ds(pl.multiple_of(mine + n * part, part), part)
        total = peer_out[span, :].astype(jnp.float32)
        for m in range(len(peers)):
            cross(m, n).wait_recv()
            total = total + peer_in[m, span, :].astype(jnp.float32)
        result[here, :] = (left[here, :].astype(jnp.float32) - step_left * scale * total).astype(jnp.bfloat16)
        share(n).start()
    shared = result.at[pl.ds(mine, half)]
    remote(shared, shared, last_send.at[0], last_recv.at[0], lane=pair).wait_recv()
    remote(ret_out, ret_in, ret_send.at[0], ret_recv.at[0], blk=partner).wait_send()
    remote(pair_out, pair_in, swap_send.at[0], swap_recv.at[0], lane=pair).wait_send()
    for m in range(len(peers)):
        remote(peer_out, peer_in.at[m], cross_send.at[m], cross_recv.at[m, 0], lane=peers[m]).wait_send()
    remote(shared, shared, last_send.at[0], last_recv.at[0], lane=pair).wait_send()


def place(left_from, right_from, left_to, right_to, sem):
    moves = [
        pltpu.make_async_copy(left_from, left_to, sem.at[0]),
        pltpu.make_async_copy(right_from, right_to, sem.at[1]),
    ]
    for move in moves:
        move.start()
    for move in moves:
        move.wait()


def solution(mesh):
    blocks = mesh.shape["blk"]
    lanes = mesh.shape["lane"]

    def local(left_factor, right_factor, observed, row_codes, shift_codes):
        rows, rank = left_factor.shape
        _, steps, cols, _ = observed.shape
        bf16, f32, i32 = jnp.bfloat16, jnp.float32, jnp.int32
        dma = pltpu.SemaphoreType.DMA
        vmem = pltpu.VMEM
        hbm = pl.BlockSpec(memory_space=pltpu.HBM)
        here = pl.BlockSpec(memory_space=pltpu.VMEM)
        room = VMEM_BYTES - 2 * (rows + cols) * rank
        others = lanes // 2 - 1
        half = rows // 2
        shapes = (
            jax.ShapeDtypeStruct((rows, rank), bf16),
            jax.ShapeDtypeStruct((1, cols, rank), bf16),
        )
        results = pl.pallas_call(
            functools.partial(kernel, blocks, lanes),
            out_shape=(vmem((rows, rank), bf16), vmem((1, cols, rank), bf16)),
            in_specs=[hbm] * 5,
            out_specs=(here, here),
            scratch_shapes=[
                vmem((rows, rank), bf16),
                vmem((rows, rank), bf16),
                *[vmem((cols, rank), bf16)] * 6,
                vmem((steps - 1, cols, rows), bf16),
                vmem((cols, rows), bf16),
                vmem((1, rows), i32),
                vmem((1, rows), i32),
                vmem((1, steps, cols), i32),
                vmem((1, steps, cols), i32),
                vmem((steps, cols, WIDTH), i32),
                vmem((steps, cols, rows), bf16),
                vmem((rows, rank), f32),
                vmem((rows, rank), f32),
                *[vmem((half, rank), bf16)] * 3,
                vmem((others, rows // lanes, rank), bf16),
                *[vmem((rows // lanes, rank), bf16)] * 2,
                *[vmem((half, rank), bf16)] * 3,
                vmem((others, half, rank), bf16),
                dma((6,)),
                dma((3,)), dma((PAIRS,)),
                dma((2,)), dma((2,)),
                dma((1,)), dma((SUBS,)),
                dma((others,)), dma((others, SUBS)),
                dma((1 + others,)), dma((1 + others, SUBS)),
                dma((1,)), dma((CHUNKS,)),
                dma((1,)), dma((PAIRS + 1,)),
                dma((1,)), dma((1,)),
                dma((others,)), dma((others,)),
                dma((1,)), dma((PIECES * 2 // lanes,)),
                dma((1,)), dma((half // WIDTH,)),
                dma((others,)), dma((others, PIECES)),
                dma((1,)), dma((1,)),
                pltpu.SemaphoreType.REGULAR,
                pltpu.SemaphoreType.REGULAR,
                pltpu.SemaphoreType.REGULAR((3 + others,)),
            ],
            compiler_params=pltpu.CompilerParams(
                collective_id=0, has_side_effects=True, vmem_limit_bytes=room
            ),
        )(
            left_factor, right_factor, observed,
            row_codes.reshape(1, rows), shift_codes,
        )
        return pl.pallas_call(
            place,
            out_shape=shapes,
            in_specs=[here] * 2,
            out_specs=(hbm, hbm),
            scratch_shapes=[dma((2,))],
            compiler_params=pltpu.CompilerParams(vmem_limit_bytes=room),
        )(*[pltpu.with_memory_space_constraint(value, pltpu.VMEM) for value in results])

    in_specs = (
        P("blk", None),
        P("lane", "blk", None),
        P("lane", None, None, "blk"),
        P("blk"),
        P("lane", None, "blk"),
    )
    out_specs = (P("blk", None), P("lane", "blk", None))
    return jax.shard_map(local, mesh=mesh, in_specs=in_specs, out_specs=out_specs, check_vma=False)
```

```python
import functools
import math

import jax
import jax.numpy as jnp
from jax import lax
from jax.experimental import pallas as pl
from jax.experimental.pallas import tpu as pltpu
from jax.sharding import PartitionSpec as P

step_right = 0.25
step_left = 0.1

CHUNKS = 8
PAIRS = CHUNKS // 2
WIDTH = 128
PIECES = 4
SUBS = 4
GUEST = 1
VMEM_BYTES = 67043328
MESH = pl.DeviceIdType.MESH


def kernel(
    blocks, lanes,
    left_hbm, right_hbm, obs_hbm, codes_hbm, shift_hbm,
    result, final_out,
    left, left_g, first, inner, hop_out, hop_in, turn_out, turn_in,
    obs, obs_g, codes, codes_g, shift, shift_g, turned, errs,
    grad, grad_g, back_out, back_in, ret_sum, ret_part, ret_out, ret_in, pair_out, pair_in, peer_out, peer_in,
    load_sem, tile_send, tile_recv, table_send, table_recv, share_send, share_recv,
    peer_share_send, peer_share_recv, pair_share_send, pair_share_recv,
    hop_send, hop_recv, turn_send, turn_recv, back_send, back_recv, fold_send, fold_recv, ret_send, ret_recv,
    swap_send, swap_recv, cross_send, cross_recv, last_send, last_recv, clear_sem, go_sem, ready_sem,
):
    steps, cols, rows = errs.shape
    final = final_out.at[0]
    rank = left.shape[1]
    scale = 1.0 / math.sqrt(rank)
    size = cols // CHUNKS
    early = cols - size
    half = rows // 2
    part = half // PIECES
    own = rows // lanes
    sub = own // SUBS
    width = turned.shape[2]
    others = lanes // 2 - 1
    quota = own // part
    blk = lax.axis_index("blk")
    lane = lax.axis_index("lane")
    odd = lax.rem(blk, 2)
    partner = blk + 1 - 2 * odd
    ahead = lax.rem(blk + 1, blocks)
    behind = lax.rem(blk + blocks - 1, blocks)
    ahead2 = lax.rem(blk + 2, blocks)
    behind2 = lax.rem(blk + blocks - 2, blocks)
    side = lax.rem(lane, 2)
    chip = lane // 2
    pair = lane + 1 - 2 * side
    peers = [lax.rem(lane + 2 * hop, lanes) for hop in range(1, lanes // 2)]
    sources = [lax.rem(lane + lanes - 2 * hop, lanes) for hop in range(1, lanes // 2)]
    mine = pl.multiple_of(side * half, half)
    other = pl.multiple_of((1 - side) * half, half)

    barrier = pltpu.get_barrier_semaphore()

    def greet(**place):
        pl.semaphore_signal(barrier, inc=1, device_id=place, device_id_type=MESH)

    def answer(which, **place):
        pl.semaphore_signal(ready_sem.at[which], inc=1, device_id=place, device_id_type=MESH)

    def await_answer(which):
        pl.semaphore_wait(ready_sem.at[which], 1)

    inner_blk = blk >= 2
    wraps = blk >= blocks - 2
    ends = blk == blocks - 1
    greet(lane=pair)
    pl.when(odd == 0)(lambda: greet(blk=partner))
    pl.when((odd == 1) & ~ends)(lambda: greet(blk=ahead))
    pl.when(~wraps)(lambda: greet(blk=ahead2))
    pl.when(~inner_blk)(lambda: greet(blk=behind2))
    pl.when(blk == 0)(lambda: greet(blk=behind))
    greeters = 1 + odd + ((odd == 0) & inner_blk).astype(jnp.int32) + inner_blk.astype(jnp.int32)
    greeters += wraps.astype(jnp.int32) + ends.astype(jnp.int32)
    for peer in peers:
        pl.when(peer > lane)(functools.partial(greet, lane=peer))
        greeters += (peer < lane).astype(jnp.int32)

    def remote(source, target, send, recv, **place):
        return pltpu.make_async_remote_copy(
            src_ref=source, dst_ref=target, send_sem=send, recv_sem=recv,
            device_id=place, device_id_type=MESH,
        )

    def chunk(k, count=1):
        return pl.ds(pl.multiple_of(k * size, size), count * size)

    natural = [s for s in range(steps) if s != GUEST]
    loads = [
        pltpu.make_async_copy(shift_hbm, shift, load_sem.at[0]),
        pltpu.make_async_copy(codes_hbm, codes, load_sem.at[1]),
        pltpu.make_async_copy(right_hbm.at[0], first, load_sem.at[2]),
        pltpu.make_async_copy(left_hbm, left, load_sem.at[3]),
    ]
    later = pl.ds(GUEST + 1, steps - 1 - GUEST)
    loads.append(pltpu.make_async_copy(obs_hbm.at[0, 0], obs.at[0], load_sem.at[4]))
    loads.append(pltpu.make_async_copy(obs_hbm.at[0, later], obs.at[pl.ds(1, steps - 2)], load_sem.at[5]))
    for copy in loads[:5]:
        copy.start()

    def piece(owner, u):
        return pl.ds(pl.multiple_of(owner * own + u * sub, sub), sub)

    def lend(u):
        span = piece(lane, u)
        return remote(left_hbm.at[span], left_g.at[span], share_send.at[0], share_recv.at[u], blk=partner)

    def lend_peer(m, u):
        span = piece(lane, u)
        return remote(left_g.at[span], left_g.at[span], peer_share_send.at[m], peer_share_recv.at[m, u], lane=peers[m])

    def lend_pair(m, u):
        span = piece(lane if m == 0 else sources[m - 1], u)
        return remote(left_g.at[span], left_g.at[span], pair_share_send.at[0], pair_share_recv.at[0], lane=pair)

    def give(p, group=0):
        span = chunk(2 * p, 2)
        return remote(obs_hbm.at[0, GUEST, span], obs_g.at[span], tile_send.at[group], tile_recv.at[p], blk=partner)

    def give_sent(group):
        first_col = (0, cols - 4 * size, cols - 2 * size)[group]
        span = pl.ds(first_col, cols - 4 * size if group == 0 else 2 * size)
        return remote(obs_hbm.at[0, GUEST, span], obs_g.at[span], tile_send.at[group], tile_recv.at[0], blk=partner)

    tables = [
        remote(codes_hbm, codes_g, table_send.at[0], table_recv.at[0], blk=partner),
        remote(shift_hbm, shift_g, table_send.at[1], table_recv.at[1], blk=partner),
    ]

    def hop(k):
        span = chunk(k)
        return remote(hop_out.at[span], hop_in.at[span], hop_send.at[0], hop_recv.at[k], blk=ahead2)

    def cross_over(k, count=1):
        span = chunk(k, count)
        return remote(turn_out.at[span], turn_in.at[span], turn_send.at[0], turn_recv.at[k // 2 + k // (CHUNKS - 1)], blk=ahead)

    def turn(s, table):
        for start in range(0, cols, width):
            span = pl.ds(start, width)
            turned[s, span, :] = jnp.transpose(jnp.broadcast_to(table[0, pl.ds(s, 1), span], (width, width)))

    def error_of(span, s, block, factor, words, target):
        shifts = jnp.concatenate([turned[s, span, :]] * (rows // width), axis=1)
        seen = (jnp.right_shift(words[...], shifts) & 1) == 1
        predicted = lax.dot_general(
            block, factor[...], (((1,), (1,)), ((), ())), preferred_element_type=jnp.float32
        )
        error = predicted * scale - target[span, :].astype(jnp.float32)
        return jnp.where(seen, error, 0.0).astype(jnp.bfloat16)

    def stepped(error, block, factor):
        move = jnp.dot(error, factor[...], preferred_element_type=jnp.float32)
        return (block.astype(jnp.float32) - step_right * scale * move).astype(jnp.bfloat16)

    def tile(k, s, source, target, guest=False, count=1):
        span = chunk(k, count)
        block = source[span, :]
        if guest:
            factor, words, wanted = left_g, codes_g, obs_g
        else:
            factor, words, wanted = left, codes, obs.at[natural.index(s)]
        error = error_of(span, s, block, factor, words, wanted)
        errs[s, span, :] = error
        target[span, :] = stepped(error, block, factor)

    last = steps - 1

    def last_visit(k, count=1):
        cross_over(k, count).wait_recv()
        tile(k, last, turn_in, final, count=count)

    def last_pair(p):
        last_visit(2 * p, 2)

    def outer(error, block):
        return lax.dot_general(error, block, (((0,), (0,)), ((), ())), preferred_element_type=jnp.float32)

    def open_table():
        loads[0].wait()
        turn(0, shift)

    pl.semaphore_wait(barrier, greeters)
    pl.when(odd == 1)(lambda: answer(0, blk=partner))
    pl.when((odd == 0) & inner_blk)(lambda: answer(1, blk=behind))
    pl.when(inner_blk)(lambda: answer(2, blk=behind2))
    for m, peer in enumerate(peers):
        pl.when(peer < lane)(functools.partial(answer, 3 + others - 1 - m, lane=peer))

    @pl.when(odd == 0)
    def _():
        open_table()
        await_answer(0)

    for u in range(SUBS):
        lend(u).start()
    for copy in tables:
        copy.start()
    for p in range(PAIRS):
        give(p, max(0, p + 3 - PAIRS)).start()
    pl.when(odd == 1)(open_table)
    for copy in loads[1:5]:
        copy.wait()
    for copy in loads[5:]:
        copy.start()

    def relay():
        for m, peer in enumerate(peers):
            pl.when(peer > lane)(functools.partial(await_answer, 3 + m))
        for u in range(SUBS):
            lend(u).wait_recv()
            for m in range(others):
                lend_peer(m, u).start()
            lend_pair(0, u).start()

    passed = left_g.at[pl.ds(0, (1 + others) * own)]
    lent_pair = remote(passed, passed, pair_share_send.at[0], pair_share_recv.at[0], lane=pair)

    def gather():
        for u in range(SUBS):
            for m in range(others):
                lend_peer(m, u).wait_recv()
                lend_pair(1 + m, u).start()
        for copy in tables:
            copy.wait_recv()
        turn(GUEST, shift_g)
        lent_pair.wait_recv()

    back = remote(back_out, back_in, back_send.at[0], back_recv.at[0], lane=pair)

    def send_back():
        back_out[...] = grad_g[pl.ds(other, half), :].astype(jnp.bfloat16)
        back.start()

    def fold(m):
        span = pl.ds(pl.multiple_of((peers[m] // 2) * own, own), own)
        return remote(ret_sum.at[span], ret_part.at[m], fold_send.at[m], fold_recv.at[m], lane=peers[m])

    def give_back(q):
        span = pl.ds(q * part, part)
        return remote(ret_out.at[span], ret_in.at[span], ret_send.at[0], ret_recv.at[q], blk=partner)

    def send_fold():
        back.wait_recv()
        ret_sum[...] = (grad_g[pl.ds(mine, half), :] + back_in[...].astype(jnp.float32)).astype(jnp.bfloat16)
        for m in range(others):
            fold(m).start()

    def send_return():
        total = ret_sum[pl.ds(pl.multiple_of(chip * own, own), own), :].astype(jnp.float32)
        for m in range(others):
            fold(m).wait_recv()
            total = total + ret_part[m].astype(jnp.float32)
        ret_out[...] = total.astype(jnp.bfloat16)
        for q in range(quota):
            give_back(q).start()

    @pl.when(odd == 0)
    def _():
        pl.loop(0, PAIRS)(lambda p: tile(2 * p, 0, first, inner, count=2))
        relay()
        grad[...] = outer(errs[0], first[...])
        turn(2, shift)
        turn(3, shift)
        gather()

        pl.when(~wraps)(lambda: await_answer(2))

        def guest_pair(p):
            give(p).wait_recv()
            tile(2 * p, GUEST, inner, hop_out, guest=True, count=2)
            for step in range(2):
                hop(2 * p + step).start()

        def home_visit(k):
            hop(k).wait_recv()
            tile(k, 2, hop_in, turn_out)
            cross_over(k).start()

        loads[5].wait()
        pl.loop(0, PAIRS - 1)(guest_pair)
        give_sent(0).wait_send()
        give_sent(1).wait_send()
        pl.semaphore_signal(clear_sem, inc=1, device_id={"lane": pair}, device_id_type=MESH)
        pl.semaphore_wait(clear_sem, 1)
        pl.loop(0, PAIRS - 1)(home_visit)
        guest_pair(PAIRS - 1)
        grad_g[...] = outer(errs[GUEST], inner[...])
        send_back()
        pl.loop(PAIRS - 1, PAIRS + 1)(home_visit)
        send_fold()

        pl.loop(PAIRS + 1, CHUNKS - 2)(home_visit)
        last_pair(0)
        home_visit(CHUNKS - 2)
        last_pair(1)
        home_visit(CHUNKS - 1)
        grad[...] += outer(errs[2], hop_in[...])
        give_sent(2).wait_send()

    @pl.when(odd == 1)
    def _():
        def start_pair(p):
            tile(2 * p, 0, first, hop_out, count=2)

        def hop_pair(p):
            for step in range(2):
                hop(2 * p + step).start()

        start_pair(0)
        pl.when(~wraps)(lambda: await_answer(2))
        hop_pair(0)

        @pl.loop(1, PAIRS)
        def _(p):
            start_pair(p)
            hop_pair(p)

        relay()
        grad[...] = outer(errs[0], first[...])
        turn(2, shift)
        turn(3, shift)
        gather()
        loads[5].wait()

        def visit_pair(p):
            give(p).wait_recv()
            for step in range(2):
                hop(2 * p + step).wait_recv()
            tile(2 * p, GUEST, hop_in, inner, guest=True, count=2)
            tile(2 * p, 2, inner, turn_out, count=2)

        def send_pair(p):
            for step in range(2):
                cross_over(2 * p + step).start()

        def release(*groups):
            for group in groups:
                give_sent(group).wait_send()
            pl.semaphore_signal(clear_sem, inc=1, device_id={"lane": pair}, device_id_type=MESH)
            pl.semaphore_wait(clear_sem, 1)
            pl.semaphore_signal(go_sem, inc=1, device_id={"blk": behind2}, device_id_type=MESH)

        def go():
            pl.semaphore_wait(go_sem, 1)
            pl.when(~ends)(lambda: await_answer(1))
            send_pair(0)

        visit_pair(0)

        @pl.when(blk == 1)
        def _():
            release(0)
            go()
            give_sent(1).wait_send()

        @pl.when((blk > 1) & ~wraps)
        def _():
            release(0, 1)
            go()

        @pl.when((blk > 1) & wraps)
        def _():
            go()
            release(0, 1)

        @pl.loop(1, PAIRS)
        def _(p):
            visit_pair(p)
            send_pair(p)

        grad_g[...] = outer(errs[GUEST], hop_in[...])
        send_back()
        grad[...] += outer(errs[2], inner[...])
        give_sent(2).wait_send()
        send_fold()

    pl.loop(2 - 2 * odd, CHUNKS // 2 - 1)(last_pair)
    send_return()
    grad[...] += outer(errs[last, pl.ds(0, cols - 4 * size)], turn_in[pl.ds(0, cols - 4 * size)])
    last_visit(CHUNKS - 2)

    rest = pl.ds(cols - 4 * size, 3 * size)
    grad[...] += outer(errs[last, rest], turn_in[rest])
    tail = pl.ds(early, size)
    cross_over(CHUNKS - 1).wait_recv()
    errs[last, tail, :] = error_of(tail, last, turn_in[tail, :], left, codes, obs.at[natural.index(last)])

    def finish(start):
        span = pl.ds(pl.multiple_of(start, width), width)
        return grad[span, :] + outer(errs[last, tail, span], turn_in[tail, :])

    def swap(start):
        span = pl.ds(pl.multiple_of(start, width), width)
        return remote(pair_out.at[span], pair_in.at[span], swap_send.at[0], swap_recv.at[start // width], lane=pair)

    def cross(m, n):
        span = pl.ds(pl.multiple_of(n * part, part), part)
        return remote(peer_out.at[span], peer_in.at[m, span], cross_send.at[m], cross_recv.at[m, n], lane=peers[m])

    def share(n):
        span = pl.ds(pl.multiple_of(mine + n * part, part), part)
        return remote(result.at[span], result.at[span], last_send.at[0], last_recv.at[0], lane=pair)

    starts = [lax.rem((chip + 1) * own + step, half) for step in range(0, half, width)]
    for start in starts:
        pair_out[pl.ds(pl.multiple_of(start, width), width), :] = finish(other + start).astype(jnp.bfloat16)
        swap(start).start()
    for start in starts:
        grad[pl.ds(pl.multiple_of(mine + start, width), width), :] = finish(mine + start)
    for q in range(PIECES):
        n = lax.rem((chip + 1) * quota + q, PIECES)
        span = pl.ds(pl.multiple_of(n * part, part), part)
        if q % (width // part) == 0:
            swap(n * part).wait_recv()
        total = (
            grad[pl.ds(pl.multiple_of(mine + n * part, part), part), :]
            + pair_in[span, :].astype(jnp.float32)
        )
        if q >= PIECES - quota:
            r = q - (PIECES - quota)
            give_back(r).wait_recv()
            total = total + ret_in[pl.ds(r * part, part), :].astype(jnp.float32)
        peer_out[span, :] = total.astype(jnp.bfloat16)
        for m in range(len(peers)):
            cross(m, n).start()

    final[tail, :] = stepped(errs[last, tail, :], turn_in[tail, :], left)

    lent = pl.ds(pl.multiple_of(lane * own, own), own)
    remote(left_hbm.at[lent], left_g.at[lent], share_send.at[0], share_recv.at[0], blk=partner).wait_send()
    for m in range(others):
        remote(left_g.at[lent], left_g.at[lent], peer_share_send.at[m], peer_share_recv.at[m, 0], lane=peers[m]).wait_send()
    lent_pair.wait_send()
    for copy in tables:
        copy.wait_send()
    remote(hop_out, hop_in, hop_send.at[0], hop_recv.at[0], blk=ahead2).wait_send()
    remote(turn_out, turn_in, turn_send.at[0], turn_recv.at[0], blk=ahead).wait_send()
    back.wait_send()
    for m in range(others):
        fold(m).wait_send()

    for q in range(PIECES):
        n = lax.rem(chip * quota + q, PIECES)
        span = pl.ds(pl.multiple_of(n * part, part), part)
        here = pl.ds(pl.multiple_of(mine + n * part, part), part)
        total = peer_out[span, :].astype(jnp.float32)
        for m in range(len(peers)):
            cross(m, n).wait_recv()
            total = total + peer_in[m, span, :].astype(jnp.float32)
        result[here, :] = (left[here, :].astype(jnp.float32) - step_left * scale * total).astype(jnp.bfloat16)
        share(n).start()
    shared = result.at[pl.ds(mine, half)]
    remote(shared, shared, last_send.at[0], last_recv.at[0], lane=pair).wait_recv()
    remote(ret_out, ret_in, ret_send.at[0], ret_recv.at[0], blk=partner).wait_send()
    remote(pair_out, pair_in, swap_send.at[0], swap_recv.at[0], lane=pair).wait_send()
    for m in range(len(peers)):
        remote(peer_out, peer_in.at[m], cross_send.at[m], cross_recv.at[m, 0], lane=peers[m]).wait_send()
    remote(shared, shared, last_send.at[0], last_recv.at[0], lane=pair).wait_send()


def place(left_from, right_from, left_to, right_to, sem):
    moves = [
        pltpu.make_async_copy(left_from, left_to, sem.at[0]),
        pltpu.make_async_copy(right_from, right_to, sem.at[1]),
    ]
    for move in moves:
        move.start()
    for move in moves:
        move.wait()


def solution(mesh):
    blocks = mesh.shape["blk"]
    lanes = mesh.shape["lane"]

    def local(left_factor, right_factor, observed, row_codes, shift_codes):
        rows, rank = left_factor.shape
        _, steps, cols, _ = observed.shape
        bf16, f32, i32 = jnp.bfloat16, jnp.float32, jnp.int32
        dma = pltpu.SemaphoreType.DMA
        vmem = pltpu.VMEM
        hbm = pl.BlockSpec(memory_space=pltpu.HBM)
        here = pl.BlockSpec(memory_space=pltpu.VMEM)
        room = VMEM_BYTES - 2 * (rows + cols) * rank
        others = lanes // 2 - 1
        half = rows // 2
        shapes = (
            jax.ShapeDtypeStruct((rows, rank), bf16),
            jax.ShapeDtypeStruct((1, cols, rank), bf16),
        )
        results = pl.pallas_call(
            functools.partial(kernel, blocks, lanes),
            out_shape=(vmem((rows, rank), bf16), vmem((1, cols, rank), bf16)),
            in_specs=[hbm] * 5,
            out_specs=(here, here),
            scratch_shapes=[
                vmem((rows, rank), bf16),
                vmem((rows, rank), bf16),
                *[vmem((cols, rank), bf16)] * 6,
                vmem((steps - 1, cols, rows), bf16),
                vmem((cols, rows), bf16),
                vmem((1, rows), i32),
                vmem((1, rows), i32),
                vmem((1, steps, cols), i32),
                vmem((1, steps, cols), i32),
                vmem((steps, cols, WIDTH), i32),
                vmem((steps, cols, rows), bf16),
                vmem((rows, rank), f32),
                vmem((rows, rank), f32),
                *[vmem((half, rank), bf16)] * 3,
                vmem((others, rows // lanes, rank), bf16),
                *[vmem((rows // lanes, rank), bf16)] * 2,
                *[vmem((half, rank), bf16)] * 3,
                vmem((others, half, rank), bf16),
                dma((6,)),
                dma((3,)), dma((PAIRS,)),
                dma((2,)), dma((2,)),
                dma((1,)), dma((SUBS,)),
                dma((others,)), dma((others, SUBS)),
                dma((1,)), dma((1,)),
                dma((1,)), dma((CHUNKS,)),
                dma((1,)), dma((PAIRS + 1,)),
                dma((1,)), dma((1,)),
                dma((others,)), dma((others,)),
                dma((1,)), dma((PIECES * 2 // lanes,)),
                dma((1,)), dma((half // WIDTH,)),
                dma((others,)), dma((others, PIECES)),
                dma((1,)), dma((1,)),
                pltpu.SemaphoreType.REGULAR,
                pltpu.SemaphoreType.REGULAR,
                pltpu.SemaphoreType.REGULAR((3 + others,)),
            ],
            compiler_params=pltpu.CompilerParams(
                collective_id=0, has_side_effects=True, vmem_limit_bytes=room
            ),
        )(
            left_factor, right_factor, observed,
            row_codes.reshape(1, rows), shift_codes,
        )
        return pl.pallas_call(
            place,
            out_shape=shapes,
            in_specs=[here] * 2,
            out_specs=(hbm, hbm),
            scratch_shapes=[dma((2,))],
            compiler_params=pltpu.CompilerParams(vmem_limit_bytes=room),
        )(*[pltpu.with_memory_space_constraint(value, pltpu.VMEM) for value in results])

    in_specs = (
        P("blk", None),
        P("lane", "blk", None),
        P("lane", None, None, "blk"),
        P("blk"),
        P("lane", None, "blk"),
    )
    out_specs = (P("blk", None), P("lane", "blk", None))
    return jax.shard_map(local, mesh=mesh, in_specs=in_specs, out_specs=out_specs, check_vma=False)
```

```python
import functools
import math

import jax
import jax.numpy as jnp
from jax import lax
from jax.experimental import pallas as pl
from jax.experimental.pallas import tpu as pltpu
from jax.sharding import PartitionSpec as P

step_right = 0.25
step_left = 0.1

CHUNKS = 8
PAIRS = CHUNKS // 2
WIDTH = 128
PIECES = 4
SUBS = 4
GUEST = 1
VMEM_BYTES = 67043328
MESH = pl.DeviceIdType.MESH


def kernel(
    blocks, lanes,
    left_hbm, right_hbm, obs_hbm, codes_hbm, shift_hbm,
    result, final_out,
    left, left_g, first, inner, hop_out, hop_in, turn_out, turn_in,
    obs, obs_g, codes, codes_g, shift, shift_g, turned, errs,
    grad, grad_g, back_out, back_in, ret_sum, ret_part, ret_out, ret_in, pair_out, pair_in, peer_out, peer_in,
    load_sem, tile_send, tile_recv, table_send, table_recv, share_send, share_recv,
    peer_share_send, peer_share_recv, pair_share_send, pair_share_recv,
    hop_send, hop_recv, turn_send, turn_recv, back_send, back_recv, fold_send, fold_recv, ret_send, ret_recv,
    swap_send, swap_recv, cross_send, cross_recv, last_send, last_recv, clear_sem, go_sem, ready_sem,
):
    steps, cols, rows = errs.shape
    final = final_out.at[0]
    rank = left.shape[1]
    scale = 1.0 / math.sqrt(rank)
    size = cols // CHUNKS
    early = cols - size
    half = rows // 2
    part = half // PIECES
    own = rows // lanes
    sub = own // SUBS
    width = turned.shape[2]
    others = lanes // 2 - 1
    quota = own // part
    blk = lax.axis_index("blk")
    lane = lax.axis_index("lane")
    odd = lax.rem(blk, 2)
    partner = blk + 1 - 2 * odd
    ahead = lax.rem(blk + 1, blocks)
    behind = lax.rem(blk + blocks - 1, blocks)
    ahead2 = lax.rem(blk + 2, blocks)
    behind2 = lax.rem(blk + blocks - 2, blocks)
    side = lax.rem(lane, 2)
    chip = lane // 2
    pair = lane + 1 - 2 * side
    peers = [lax.rem(lane + 2 * hop, lanes) for hop in range(1, lanes // 2)]
    sources = [lax.rem(lane + lanes - 2 * hop, lanes) for hop in range(1, lanes // 2)]
    mine = pl.multiple_of(side * half, half)
    other = pl.multiple_of((1 - side) * half, half)

    barrier = pltpu.get_barrier_semaphore()

    def greet(**place):
        pl.semaphore_signal(barrier, inc=1, device_id=place, device_id_type=MESH)

    def answer(which, **place):
        pl.semaphore_signal(ready_sem.at[which], inc=1, device_id=place, device_id_type=MESH)

    def await_answer(which):
        pl.semaphore_wait(ready_sem.at[which], 1)

    inner_blk = blk >= 2
    wraps = blk >= blocks - 2
    ends = blk == blocks - 1
    greet(lane=pair)
    pl.when(odd == 0)(lambda: greet(blk=partner))
    pl.when((odd == 1) & ~ends)(lambda: greet(blk=ahead))
    pl.when(~wraps)(lambda: greet(blk=ahead2))
    pl.when(~inner_blk)(lambda: greet(blk=behind2))
    pl.when(blk == 0)(lambda: greet(blk=behind))
    greeters = 1 + odd + ((odd == 0) & inner_blk).astype(jnp.int32) + inner_blk.astype(jnp.int32)
    greeters += wraps.astype(jnp.int32) + ends.astype(jnp.int32)
    for peer in peers:
        pl.when(peer > lane)(functools.partial(greet, lane=peer))
        greeters += (peer < lane).astype(jnp.int32)

    def remote(source, target, send, recv, **place):
        return pltpu.make_async_remote_copy(
            src_ref=source, dst_ref=target, send_sem=send, recv_sem=recv,
            device_id=place, device_id_type=MESH,
        )

    def chunk(k, count=1):
        return pl.ds(pl.multiple_of(k * size, size), count * size)

    natural = [s for s in range(steps) if s != GUEST]
    loads = [
        pltpu.make_async_copy(shift_hbm, shift, load_sem.at[0]),
        pltpu.make_async_copy(codes_hbm, codes, load_sem.at[1]),
        pltpu.make_async_copy(right_hbm.at[0], first, load_sem.at[2]),
        pltpu.make_async_copy(left_hbm, left, load_sem.at[3]),
    ]
    later = pl.ds(GUEST + 1, steps - 1 - GUEST)
    loads.append(pltpu.make_async_copy(obs_hbm.at[0, 0], obs.at[0], load_sem.at[4]))
    loads.append(pltpu.make_async_copy(obs_hbm.at[0, later], obs.at[pl.ds(1, steps - 2)], load_sem.at[5]))
    for copy in loads[:5]:
        copy.start()

    def piece(owner, u):
        return pl.ds(pl.multiple_of(owner * own + u * sub, sub), sub)

    def lend(u):
        span = piece(lane, u)
        return remote(left_hbm.at[span], left_g.at[span], share_send.at[0], share_recv.at[u], blk=partner)

    def lend_peer(m, u):
        span = piece(lane, u)
        return remote(left_g.at[span], left_g.at[span], peer_share_send.at[m], peer_share_recv.at[m, u], lane=peers[m])

    def lend_pair(m, u):
        span = piece(lane if m == 0 else sources[m - 1], u)
        return remote(left_g.at[span], left_g.at[span], pair_share_send.at[0], pair_share_recv.at[0], lane=pair)

    def give(p, group=0):
        span = chunk(2 * p, 2)
        return remote(obs_hbm.at[0, GUEST, span], obs_g.at[span], tile_send.at[group], tile_recv.at[p], blk=partner)

    def give_sent(group):
        first_col = (0, cols - 4 * size, cols - 2 * size)[group]
        span = pl.ds(first_col, cols - 4 * size if group == 0 else 2 * size)
        return remote(obs_hbm.at[0, GUEST, span], obs_g.at[span], tile_send.at[group], tile_recv.at[0], blk=partner)

    tables = [
        remote(codes_hbm, codes_g, table_send.at[0], table_recv.at[0], blk=partner),
        remote(shift_hbm, shift_g, table_send.at[1], table_recv.at[1], blk=partner),
    ]

    def hop(k):
        span = chunk(k)
        return remote(hop_out.at[span], hop_in.at[span], hop_send.at[0], hop_recv.at[k], blk=ahead2)

    def cross_over(k, count=1):
        span = chunk(k, count)
        return remote(turn_out.at[span], turn_in.at[span], turn_send.at[0], turn_recv.at[k // 2 + k // (CHUNKS - 1)], blk=ahead)

    def turn(s, table):
        for start in range(0, cols, width):
            span = pl.ds(start, width)
            turned[s, span, :] = jnp.transpose(jnp.broadcast_to(table[0, pl.ds(s, 1), span], (width, width)))

    def error_of(span, s, block, factor, words, target):
        shifts = jnp.concatenate([turned[s, span, :]] * (rows // width), axis=1)
        seen = (jnp.right_shift(words[...], shifts) & 1) == 1
        predicted = lax.dot_general(
            block, factor[...], (((1,), (1,)), ((), ())), preferred_element_type=jnp.float32
        )
        error = predicted * scale - target[span, :].astype(jnp.float32)
        return jnp.where(seen, error, 0.0).astype(jnp.bfloat16)

    def stepped(error, block, factor):
        move = jnp.dot(error, factor[...], preferred_element_type=jnp.float32)
        return (block.astype(jnp.float32) - step_right * scale * move).astype(jnp.bfloat16)

    def tile(k, s, source, target, guest=False, count=1):
        span = chunk(k, count)
        block = source[span, :]
        if guest:
            factor, words, wanted = left_g, codes_g, obs_g
        else:
            factor, words, wanted = left, codes, obs.at[natural.index(s)]
        error = error_of(span, s, block, factor, words, wanted)
        errs[s, span, :] = error
        target[span, :] = stepped(error, block, factor)

    last = steps - 1

    def last_visit(k, count=1):
        cross_over(k, count).wait_recv()
        tile(k, last, turn_in, final, count=count)

    def last_pair(p):
        last_visit(2 * p, 2)

    def outer(error, block):
        return lax.dot_general(error, block, (((0,), (0,)), ((), ())), preferred_element_type=jnp.float32)

    def open_table():
        loads[0].wait()
        turn(0, shift)

    pl.semaphore_wait(barrier, greeters)
    pl.when(odd == 1)(lambda: answer(0, blk=partner))
    pl.when((odd == 0) & inner_blk)(lambda: answer(1, blk=behind))
    pl.when(inner_blk)(lambda: answer(2, blk=behind2))
    for m, peer in enumerate(peers):
        pl.when(peer < lane)(functools.partial(answer, 3 + others - 1 - m, lane=peer))

    @pl.when(odd == 0)
    def _():
        open_table()
        await_answer(0)

    for u in range(SUBS):
        lend(u).start()
    for copy in tables:
        copy.start()
    for p in range(PAIRS):
        give(p, max(0, p + 3 - PAIRS)).start()
    pl.when(odd == 1)(open_table)
    for copy in loads[1:5]:
        copy.wait()
    for copy in loads[5:]:
        copy.start()

    def relay():
        for m, peer in enumerate(peers):
            pl.when(peer > lane)(functools.partial(await_answer, 3 + m))
        for u in range(SUBS):
            lend(u).wait_recv()
            for m in range(others):
                lend_peer(m, u).start()
            lend_pair(0, u).start()

    passed = left_g.at[pl.ds(0, (1 + others) * own)]
    lent_pair = remote(passed, passed, pair_share_send.at[0], pair_share_recv.at[0], lane=pair)

    def gather():
        for u in range(SUBS):
            for m in range(others):
                lend_peer(m, u).wait_recv()
                lend_pair(1 + m, u).start()
        for copy in tables:
            copy.wait_recv()
        turn(GUEST, shift_g)
        lent_pair.wait_recv()

    back = remote(back_out, back_in, back_send.at[0], back_recv.at[0], lane=pair)

    def send_back():
        back_out[...] = grad_g[pl.ds(other, half), :].astype(jnp.bfloat16)
        back.start()

    def fold(m):
        span = pl.ds(pl.multiple_of((peers[m] // 2) * own, own), own)
        return remote(ret_sum.at[span], ret_part.at[m], fold_send.at[m], fold_recv.at[m], lane=peers[m])

    def give_back(q):
        span = pl.ds(q * part, part)
        return remote(ret_out.at[span], ret_in.at[span], ret_send.at[0], ret_recv.at[q], blk=partner)

    def send_fold():
        back.wait_recv()
        ret_sum[...] = (grad_g[pl.ds(mine, half), :] + back_in[...].astype(jnp.float32)).astype(jnp.bfloat16)
        for m in range(others):
            fold(m).start()

    def send_return():
        total = ret_sum[pl.ds(pl.multiple_of(chip * own, own), own), :].astype(jnp.float32)
        for m in range(others):
            fold(m).wait_recv()
            total = total + ret_part[m].astype(jnp.float32)
        ret_out[...] = total.astype(jnp.bfloat16)
        for q in range(quota):
            give_back(q).start()

    @pl.when(odd == 0)
    def _():
        pl.loop(0, PAIRS)(lambda p: tile(2 * p, 0, first, inner, count=2))
        relay()
        grad[...] = outer(errs[0], first[...])
        turn(2, shift)
        turn(3, shift)
        gather()

        pl.when(~wraps)(lambda: await_answer(2))

        def guest_pair(p):
            give(p).wait_recv()
            tile(2 * p, GUEST, inner, hop_out, guest=True, count=2)
            for step in range(2):
                hop(2 * p + step).start()

        def home_visit(k):
            hop(k).wait_recv()
            tile(k, 2, hop_in, turn_out)
            cross_over(k).start()

        loads[5].wait()
        pl.loop(0, PAIRS - 1)(guest_pair)
        give_sent(0).wait_send()
        pl.semaphore_signal(clear_sem, inc=1, device_id={"lane": pair}, device_id_type=MESH)
        pl.semaphore_wait(clear_sem, 1)
        pl.loop(0, PAIRS - 1)(home_visit)
        guest_pair(PAIRS - 1)
        grad_g[...] = outer(errs[GUEST], inner[...])
        send_back()
        pl.loop(PAIRS - 1, PAIRS + 1)(home_visit)
        send_fold()

        pl.loop(PAIRS + 1, CHUNKS - 2)(home_visit)
        last_pair(0)
        home_visit(CHUNKS - 2)
        last_pair(1)
        home_visit(CHUNKS - 1)
        grad[...] += outer(errs[2], hop_in[...])
        give_sent(1).wait_send()
        give_sent(2).wait_send()

    @pl.when(odd == 1)
    def _():
        def start_pair(p):
            tile(2 * p, 0, first, hop_out, count=2)

        def hop_pair(p):
            for step in range(2):
                hop(2 * p + step).start()

        start_pair(0)
        pl.when(~wraps)(lambda: await_answer(2))
        hop_pair(0)

        @pl.loop(1, PAIRS)
        def _(p):
            start_pair(p)
            hop_pair(p)

        relay()
        grad[...] = outer(errs[0], first[...])
        turn(2, shift)
        turn(3, shift)
        gather()
        loads[5].wait()

        def visit_pair(p):
            give(p).wait_recv()
            for step in range(2):
                hop(2 * p + step).wait_recv()
            tile(2 * p, GUEST, hop_in, inner, guest=True, count=2)
            tile(2 * p, 2, inner, turn_out, count=2)

        def send_pair(p):
            for step in range(2):
                cross_over(2 * p + step).start()

        def release(*groups):
            for group in groups:
                give_sent(group).wait_send()
            pl.semaphore_signal(clear_sem, inc=1, device_id={"lane": pair}, device_id_type=MESH)
            pl.semaphore_wait(clear_sem, 1)
            pl.semaphore_signal(go_sem, inc=1, device_id={"blk": behind2}, device_id_type=MESH)

        def go():
            pl.semaphore_wait(go_sem, 1)
            pl.when(~ends)(lambda: await_answer(1))
            send_pair(0)

        visit_pair(0)

        @pl.when(blk == 1)
        def _():
            release(0)
            go()
            give_sent(1).wait_send()

        @pl.when((blk > 1) & ~wraps)
        def _():
            release(0, 1)
            go()

        @pl.when((blk > 1) & wraps)
        def _():
            go()
            release(0, 1)

        @pl.loop(1, PAIRS)
        def _(p):
            visit_pair(p)
            send_pair(p)

        grad_g[...] = outer(errs[GUEST], hop_in[...])
        send_back()
        grad[...] += outer(errs[2], inner[...])
        give_sent(2).wait_send()
        send_fold()

    pl.loop(2 - 2 * odd, CHUNKS // 2 - 1)(last_pair)
    send_return()
    grad[...] += outer(errs[last, pl.ds(0, cols - 4 * size)], turn_in[pl.ds(0, cols - 4 * size)])
    last_visit(CHUNKS - 2)

    rest = pl.ds(cols - 4 * size, 3 * size)
    grad[...] += outer(errs[last, rest], turn_in[rest])
    tail = pl.ds(early, size)
    cross_over(CHUNKS - 1).wait_recv()
    errs[last, tail, :] = error_of(tail, last, turn_in[tail, :], left, codes, obs.at[natural.index(last)])

    def finish(start):
        span = pl.ds(pl.multiple_of(start, width), width)
        return grad[span, :] + outer(errs[last, tail, span], turn_in[tail, :])

    def swap(start):
        span = pl.ds(pl.multiple_of(start, width), width)
        return remote(pair_out.at[span], pair_in.at[span], swap_send.at[0], swap_recv.at[start // width], lane=pair)

    def cross(m, n):
        span = pl.ds(pl.multiple_of(n * part, part), part)
        return remote(peer_out.at[span], peer_in.at[m, span], cross_send.at[m], cross_recv.at[m, n], lane=peers[m])

    def share(n):
        span = pl.ds(pl.multiple_of(mine + n * part, part), part)
        return remote(result.at[span], result.at[span], last_send.at[0], last_recv.at[0], lane=pair)

    starts = [lax.rem((chip + 1) * own + step, half) for step in range(0, half, width)]
    for start in starts:
        pair_out[pl.ds(pl.multiple_of(start, width), width), :] = finish(other + start).astype(jnp.bfloat16)
        swap(start).start()
    for start in starts:
        grad[pl.ds(pl.multiple_of(mine + start, width), width), :] = finish(mine + start)
    for q in range(PIECES):
        n = lax.rem((chip + 1) * quota + q, PIECES)
        span = pl.ds(pl.multiple_of(n * part, part), part)
        if q % (width // part) == 0:
            swap(n * part).wait_recv()
        total = (
            grad[pl.ds(pl.multiple_of(mine + n * part, part), part), :]
            + pair_in[span, :].astype(jnp.float32)
        )
        if q >= PIECES - quota:
            r = q - (PIECES - quota)
            give_back(r).wait_recv()
            total = total + ret_in[pl.ds(r * part, part), :].astype(jnp.float32)
        peer_out[span, :] = total.astype(jnp.bfloat16)
        for m in range(len(peers)):
            cross(m, n).start()

    final[tail, :] = stepped(errs[last, tail, :], turn_in[tail, :], left)

    lent = pl.ds(pl.multiple_of(lane * own, own), own)
    remote(left_hbm.at[lent], left_g.at[lent], share_send.at[0], share_recv.at[0], blk=partner).wait_send()
    for m in range(others):
        remote(left_g.at[lent], left_g.at[lent], peer_share_send.at[m], peer_share_recv.at[m, 0], lane=peers[m]).wait_send()
    lent_pair.wait_send()
    for copy in tables:
        copy.wait_send()
    remote(hop_out, hop_in, hop_send.at[0], hop_recv.at[0], blk=ahead2).wait_send()
    remote(turn_out, turn_in, turn_send.at[0], turn_recv.at[0], blk=ahead).wait_send()
    back.wait_send()
    for m in range(others):
        fold(m).wait_send()

    for q in range(PIECES):
        n = lax.rem(chip * quota + q, PIECES)
        span = pl.ds(pl.multiple_of(n * part, part), part)
        here = pl.ds(pl.multiple_of(mine + n * part, part), part)
        total = peer_out[span, :].astype(jnp.float32)
        for m in range(len(peers)):
            cross(m, n).wait_recv()
            total = total + peer_in[m, span, :].astype(jnp.float32)
        result[here, :] = (left[here, :].astype(jnp.float32) - step_left * scale * total).astype(jnp.bfloat16)
        share(n).start()
    shared = result.at[pl.ds(mine, half)]
    remote(shared, shared, last_send.at[0], last_recv.at[0], lane=pair).wait_recv()
    remote(ret_out, ret_in, ret_send.at[0], ret_recv.at[0], blk=partner).wait_send()
    remote(pair_out, pair_in, swap_send.at[0], swap_recv.at[0], lane=pair).wait_send()
    for m in range(len(peers)):
        remote(peer_out, peer_in.at[m], cross_send.at[m], cross_recv.at[m, 0], lane=peers[m]).wait_send()
    remote(shared, shared, last_send.at[0], last_recv.at[0], lane=pair).wait_send()


def place(left_from, right_from, left_to, right_to, sem):
    moves = [
        pltpu.make_async_copy(left_from, left_to, sem.at[0]),
        pltpu.make_async_copy(right_from, right_to, sem.at[1]),
    ]
    for move in moves:
        move.start()
    for move in moves:
        move.wait()


def solution(mesh):
    blocks = mesh.shape["blk"]
    lanes = mesh.shape["lane"]

    def local(left_factor, right_factor, observed, row_codes, shift_codes):
        rows, rank = left_factor.shape
        _, steps, cols, _ = observed.shape
        bf16, f32, i32 = jnp.bfloat16, jnp.float32, jnp.int32
        dma = pltpu.SemaphoreType.DMA
        vmem = pltpu.VMEM
        hbm = pl.BlockSpec(memory_space=pltpu.HBM)
        here = pl.BlockSpec(memory_space=pltpu.VMEM)
        room = VMEM_BYTES - 2 * (rows + cols) * rank
        others = lanes // 2 - 1
        half = rows // 2
        shapes = (
            jax.ShapeDtypeStruct((rows, rank), bf16),
            jax.ShapeDtypeStruct((1, cols, rank), bf16),
        )
        results = pl.pallas_call(
            functools.partial(kernel, blocks, lanes),
            out_shape=(vmem((rows, rank), bf16), vmem((1, cols, rank), bf16)),
            in_specs=[hbm] * 5,
            out_specs=(here, here),
            scratch_shapes=[
                vmem((rows, rank), bf16),
                vmem((rows, rank), bf16),
                *[vmem((cols, rank), bf16)] * 6,
                vmem((steps - 1, cols, rows), bf16),
                vmem((cols, rows), bf16),
                vmem((1, rows), i32),
                vmem((1, rows), i32),
                vmem((1, steps, cols), i32),
                vmem((1, steps, cols), i32),
                vmem((steps, cols, WIDTH), i32),
                vmem((steps, cols, rows), bf16),
                vmem((rows, rank), f32),
                vmem((rows, rank), f32),
                *[vmem((half, rank), bf16)] * 3,
                vmem((others, rows // lanes, rank), bf16),
                *[vmem((rows // lanes, rank), bf16)] * 2,
                *[vmem((half, rank), bf16)] * 3,
                vmem((others, half, rank), bf16),
                dma((6,)),
                dma((3,)), dma((PAIRS,)),
                dma((2,)), dma((2,)),
                dma((1,)), dma((SUBS,)),
                dma((others,)), dma((others, SUBS)),
                dma((1,)), dma((1,)),
                dma((1,)), dma((CHUNKS,)),
                dma((1,)), dma((PAIRS + 1,)),
                dma((1,)), dma((1,)),
                dma((others,)), dma((others,)),
                dma((1,)), dma((PIECES * 2 // lanes,)),
                dma((1,)), dma((half // WIDTH,)),
                dma((others,)), dma((others, PIECES)),
                dma((1,)), dma((1,)),
                pltpu.SemaphoreType.REGULAR,
                pltpu.SemaphoreType.REGULAR,
                pltpu.SemaphoreType.REGULAR((3 + others,)),
            ],
            compiler_params=pltpu.CompilerParams(
                collective_id=0, has_side_effects=True, vmem_limit_bytes=room
            ),
        )(
            left_factor, right_factor, observed,
            row_codes.reshape(1, rows), shift_codes,
        )
        return pl.pallas_call(
            place,
            out_shape=shapes,
            in_specs=[here] * 2,
            out_specs=(hbm, hbm),
            scratch_shapes=[dma((2,))],
            compiler_params=pltpu.CompilerParams(vmem_limit_bytes=room),
        )(*[pltpu.with_memory_space_constraint(value, pltpu.VMEM) for value in results])

    in_specs = (
        P("blk", None),
        P("lane", "blk", None),
        P("lane", None, None, "blk"),
        P("blk"),
        P("lane", None, "blk"),
    )
    out_specs = (P("blk", None), P("lane", "blk", None))
    return jax.shard_map(local, mesh=mesh, in_specs=in_specs, out_specs=out_specs, check_vma=False)
```
